128 devices in a mesh: tile: 32 (over z, y, core), sub: 4 (over x).
Axes of the slice: x: 4, y: 4, z: 4, core: 2. Of those that a mesh axis runs over, the one named last changes fastest.
Arguments:
- offsets: float32 [3, 32, 64, 1024], P(None, None, 'tile', 'sub'), may hold values from 0 to 1
- velocity: float32 [3, 32, 64, 1024], P(None, None, 'tile', 'sub'), may hold values from -1.5 to 1.5
- mass: float32 [32, 64, 1024], P(None, 'tile', 'sub'), may hold values from 0.015625 to 0.0625
- entropy: float32 [32, 64, 1024], P(None, 'tile', 'sub'), may hold values from 0.5 to 2
- active_counts: int32 [3, 64, 1024], P(None, 'tile', 'sub'), may hold values from 0 to 32, as said below
- targets: int32 [32, 64, 1024], P(None, 'tile', 'sub'), may hold values from 0 to 3, as said below
Outputs:
- arrived: float32 [8, 3145728], P(None, ('tile', 'sub'))
The draws below stay inside these ranges and needn't reach their ends.
Inputs may be any that keep to these rules, and one draw needn't show every extreme that they name: active_counts[0] is a cell's number of occupied slots, from 16 to 32; counts never rise from one level to the next; active_counts[1] is at most 16 and active_counts[2] at most 8, and these bounds and 32 are each reached in some cell. Active particles of a substep are the cell's first slots. `targets`: among one device's 16384 particles, no destination is named by more than 6144 of them, and one destination is named by exactly 6144.
All inputs are finite; a program needn't handle non-finite values.
Results may differ from the reference program's by a relative error of at most 0.0001.
Values sent between devices are 32-bit elements; how exact they have to be, the bound alone decides.
A program may use at most 128 MiB of HBM per device.

```python
import math
import jax
import jax.numpy as jnp
from jax import lax

S = 32
LEVELS = 3
TX = 2
SY = 256
GX = 64
GY = 1024
CAP = 6144


def draw_active_counts(key, part):
    tile_count = GX // TX
    subkeys = jax.random.split(jax.random.fold_in(key, 11), 3)
    occupied = jax.random.randint(subkeys[0], (GX, GY), S // 2, S + 1)
    level_draw = jax.random.randint(subkeys[1], (tile_count,), 0, 4)
    tile_weight = jnp.where(level_draw == 3, 8, 1)
    row_weight = jnp.repeat(tile_weight, TX)[:, None]
    middle = jnp.minimum(occupied * row_weight // 16, S // 2)
    finest = jnp.minimum(middle * row_weight // 16, S // 4)
    chosen_cell = jax.random.randint(subkeys[2], (), 0, GX * GY)
    cell_ids = jnp.arange(GX * GY).reshape(GX, GY)
    picked = cell_ids == chosen_cell
    occupied = jnp.where(picked, S, occupied)
    middle = jnp.where(picked, S // 2, middle)
    finest = jnp.where(picked, S // 4, finest)
    return jnp.stack([occupied, middle, finest]).astype(jnp.int32)


def draw_targets(key, part):
    tile_count = GX // TX
    sub_count = GY // SY
    per_device = S * TX * SY
    capacity = 3 * per_device // 8

    def device_labels(device):
        device_key = jax.random.fold_in(jax.random.fold_in(key, 7), device)
        subkeys = jax.random.split(device_key, 4)
        ordering = jax.random.permutation(subkeys[0], sub_count)
        second_load = jax.random.randint(subkeys[1], (), per_device // 4, capacity + 1)
        coin_flip = jax.random.randint(subkeys[2], (per_device,), 0, 2)
        position = jnp.arange(per_device)
        labels = jnp.where(position < capacity, ordering[0], jnp.where(position < capacity + second_load, ordering[1], jnp.where(coin_flip == 0, ordering[2], ordering[3])))
        return jax.random.permutation(subkeys[3], labels)
    blocks = jax.vmap(device_labels)(jnp.arange(tile_count * sub_count))
    blocks = blocks.reshape(tile_count, sub_count, S, TX, SY)
    return jnp.transpose(blocks, (2, 0, 3, 1, 4)).reshape(S, GX, GY).astype(jnp.int32)


def levels(own_key, shape, cuts, least, top_value):
    factor_of, own = 1.0, jax.random.fold_in(own_key, 6)
    for axis_at, blocks in cuts:
        draws = jnp.exp(jax.random.uniform(jax.random.fold_in(own, axis_at), (blocks,), jnp.float32, least / len(cuts), top_value / len(cuts)))
        factor_of = factor_of * jnp.repeat(draws, shape[axis_at] // blocks).reshape([-1 if axis == axis_at else 1 for axis in range(len(shape))])
    return factor_of


def normal_values(stream_key, shape, deviation, reach, cuts=(), kind=jnp.bfloat16):
    factor_of = levels(stream_key, shape, cuts, -0.22, 0.18) if cuts else 1.0
    entries = jax.random.normal(stream_key, shape, jnp.float32) * deviation * factor_of
    return jnp.minimum(jnp.maximum(entries, -reach), reach).astype(kind)


def setup_inputs(seed: int = 0) -> dict:
    key_of = jax.random.split(jax.random.key(seed), 7)
    return {
        "offsets": jnp.clip(1.0 * jax.random.uniform(key_of[0], (3, S, GX, GY), jnp.float32) ** levels(key_of[0], (3, S, GX, GY), ((2, 32), (3, 4)), -0.2, 0.2), 0.0, 1.0),
        "velocity": normal_values(key_of[1], (3, S, GX, GY), 0.3, 1.5, ((2, 32), (3, 4)), jnp.float32),
        "mass": jnp.clip(jnp.exp(math.log(0.0625) - 1.3862944 * jax.random.uniform(key_of[2], (S, GX, GY), jnp.float32) ** levels(key_of[2], (S, GX, GY), ((1, 32), (2, 4)), -0.2, 0.2)), 0.015625, 0.0625),
        "entropy": jnp.clip(jnp.exp(math.log(2.0) - 1.3862944 * jax.random.uniform(key_of[3], (S, GX, GY), jnp.float32) ** levels(key_of[3], (S, GX, GY), ((1, 32), (2, 4)), -0.2, 0.2)), 0.5, 2.0),
        "active_counts": draw_active_counts(jax.random.fold_in(key_of[6], 71), 0),
        "targets": draw_targets(jax.random.fold_in(key_of[6], 71), 0),
    }


KERNEL_NORM = 21.0 / (2.0 * math.pi)
GAMMA = 5.0 / 3.0
VISC_ALPHA = 1.0
VISC_BETA = 2.0
TIME_STEP = 0.05
SOFTEN = 0.01

def separation(local_part, theirs, shift_x, shift_y):
    delta_x = local_part[0][:, None] - theirs[0][None, :] - shift_x
    delta_y = local_part[1][:, None] - theirs[1][None, :] - shift_y
    delta_z = local_part[2][:, None] - theirs[2][None, :]
    return (delta_x, delta_y, delta_z)

def density_pair(local_part, theirs, shift_x, shift_y):
    delta_x, delta_y, delta_z = separation(local_part, theirs, shift_x, shift_y)
    squared = delta_x * delta_x + delta_y * delta_y + delta_z * delta_z
    radius = jnp.sqrt(squared)
    remain = jnp.maximum(1.0 - radius, 0.0)
    weight = KERNEL_NORM * remain ** 4 * (1.0 + 4.0 * radius)
    return lax.optimization_barrier(jnp.sum(theirs[6][None, :] * weight, axis=1))

def force_pair(local_part, theirs, own_pressure, their_pressure, shift_x, shift_y):
    delta_x, delta_y, delta_z = separation(local_part, theirs, shift_x, shift_y)
    squared = delta_x * delta_x + delta_y * delta_y + delta_z * delta_z
    radius = jnp.sqrt(squared)
    remain = jnp.maximum(1.0 - radius, 0.0)
    relative_x = local_part[3][:, None] - theirs[3][None, :]
    relative_y = local_part[4][:, None] - theirs[4][None, :]
    relative_z = local_part[5][:, None] - theirs[5][None, :]
    approach = delta_x * relative_x + delta_y * relative_y + delta_z * relative_z
    closing = jnp.minimum(approach, 0.0) / (squared + SOFTEN)
    sound_mean = 0.5 * (own_pressure[1][:, None] + their_pressure[1][None, :])
    mean_density = 0.5 * (own_pressure[2][:, None] + their_pressure[2][None, :])
    viscous = (-VISC_ALPHA * sound_mean * closing + VISC_BETA * closing * closing) / mean_density
    strength = theirs[6][None, :] * (own_pressure[0][:, None] + their_pressure[0][None, :] + viscous)
    strength = strength * (20.0 * KERNEL_NORM) * remain ** 3
    return jnp.stack([lax.optimization_barrier(jnp.sum(strength * delta_x, axis=1)), lax.optimization_barrier(jnp.sum(strength * delta_y, axis=1)), lax.optimization_barrier(jnp.sum(strength * delta_z, axis=1))])

def pressure_terms(density, entropy, occupied):
    density_used = jnp.where(occupied, density, 1.0)
    return jnp.stack([entropy * density_used ** (GAMMA - 2.0), jnp.sqrt(GAMMA * entropy * density_used ** (GAMMA - 1.0)), density_used])

def wrap_rows(field):
    return jnp.concatenate([field[:, :, -1:], field, field[:, :, :1]], axis=2)

def density_all(motion):
    padded = wrap_rows(motion)

    def one_row(row_index):
        window = lax.dynamic_slice_in_dim(padded, row_index, 3, 2)
        local_part = window[:, :, 1]
        summed = jnp.zeros(local_part.shape[1:], jnp.float32)
        for shift_x in (-1, 0, 1):
            for shift_y in (-1, 0, 1):
                theirs = jnp.roll(window[:, :, 1 + shift_x], -shift_y, axis=2)
                summed = summed + density_pair(local_part, theirs, float(shift_x), float(shift_y))
        return summed
    rows = lax.map(one_row, jnp.arange(GX, dtype=jnp.int32))
    return jnp.transpose(rows, (1, 0, 2))

def force_all(motion, pressure):
    padded = wrap_rows(motion)
    padded_pressure = wrap_rows(pressure)

    def one_row(row_index):
        window = lax.dynamic_slice_in_dim(padded, row_index, 3, 2)
        window_pressure = lax.dynamic_slice_in_dim(padded_pressure, row_index, 3, 2)
        local_part = window[:, :, 1]
        own_pressure = window_pressure[:, :, 1]
        summed = jnp.zeros((3,) + local_part.shape[1:], jnp.float32)
        for shift_x in (-1, 0, 1):
            for shift_y in (-1, 0, 1):
                theirs = jnp.roll(window[:, :, 1 + shift_x], -shift_y, axis=2)
                their_pressure = jnp.roll(window_pressure[:, :, 1 + shift_x], -shift_y, axis=2)
                summed = summed + force_pair(local_part, theirs, own_pressure, their_pressure, float(shift_x), float(shift_y))
        return summed
    rows = lax.map(one_row, jnp.arange(GX, dtype=jnp.int32))
    return jnp.transpose(rows, (1, 2, 0, 3))

def reference(offsets, velocity, mass, entropy, active_counts, targets):
    slot_index = lax.broadcasted_iota(jnp.int32, (S, GX, GY), 0)
    occupied = slot_index < active_counts[0][None]
    mass_live = jnp.where(occupied, mass, 0.0)
    places = offsets
    speeds = velocity
    density = jnp.ones((S, GX, GY), jnp.float32)
    for substep in range(LEVELS):
        active = slot_index < active_counts[substep][None]
        motion = jnp.concatenate([places, speeds, mass_live[None]], axis=0)
        fresh_density = density_all(motion)
        density = jnp.where(active, fresh_density, density)
        pressure = pressure_terms(density, entropy, occupied)
        acceleration = force_all(motion, pressure)
        speeds = jnp.where(active[None], speeds + TIME_STEP * acceleration, speeds)
        places = jnp.where(active[None], places + TIME_STEP * speeds, places)
    particle_state = jnp.concatenate([places, speeds, density[None], mass_live[None]], axis=0)
    tile_count = GX // TX
    sub_count = GY // SY
    per_device = S * TX * SY
    particle_state = particle_state.reshape(8, S, tile_count, TX, sub_count, SY)
    particle_state = jnp.transpose(particle_state, (0, 2, 4, 1, 3, 5)).reshape(8, tile_count, sub_count, per_device)
    destination = targets.reshape(S, tile_count, TX, sub_count, SY)
    destination = jnp.transpose(destination, (1, 3, 0, 2, 4)).reshape(tile_count, sub_count, per_device)
    choices_of = jnp.arange(sub_count, dtype=jnp.int32)
    onehot = (destination[:, :, None, :] == choices_of[None, None, :, None]).astype(jnp.int32)
    rank_in = lax.optimization_barrier(jnp.sum((jnp.cumsum(onehot, axis=3) - 1) * onehot, axis=2))
    tile_ids = jnp.arange(tile_count, dtype=jnp.int32)[:, None, None]
    source_ids = jnp.arange(sub_count, dtype=jnp.int32)[None, :, None]
    flat_slot = ((tile_ids * sub_count + destination) * sub_count + source_ids) * CAP + rank_in
    arrived = jnp.zeros((8, tile_count * sub_count * sub_count * CAP), jnp.float32)
    arrived = arrived.at[:, flat_slot.reshape(-1)].set(particle_state.reshape(8, -1))
    return arrived
```

```python
import functools
import math

import jax
import jax.numpy as jnp
from jax import lax
from jax.experimental import pallas as pl
from jax.experimental.pallas import tpu as pltpu
from jax.sharding import PartitionSpec as P

MESH = pl.DeviceIdType.MESH

S = 32
LN = 128
KERNEL_NORM = 21.0 / (2.0 * math.pi)
NACT = (32, 16, 8)
NMOVED = (32, 32, 16)

X, Y, Z, VX, VY, VZ, MS, Q, C, R = range(10)
NF = 10


def field(row, comp, b, h):
    return ((row * NF + comp) * 3 + b) * 2 + h


def lane_iota():
    return lax.broadcasted_iota(jnp.int32, (8, LN), 1)


def stage_ids(stage, c):
    if stage == 0:
        return c // 2, 1 + c % 2, 1
    if stage == 1:
        return c // 4, 1 + (c // 2) % 2, 2 * (c % 2)
    return c // 3, 3 * (c // 3), c % 3


STAGE_SIZE = (4, 8, 6)
STAGE_BASE = (0, 4, 12)


def substeps_kernel(
    tiles, subs, off, vel, mass, ent, cnt, out, fld, st, pr, dens, acc, sq, ysend, xin, pin, yin,
    cache_w, cache_a, send_sem, recv_sem
):
    t, u = lax.axis_index("tile"), lax.axis_index("sub")
    up, down = lax.rem(t + 1, tiles), lax.rem(t + tiles - 1, tiles)
    right, left = lax.rem(u + 1, subs), lax.rem(u + subs - 1, subs)
    tile_of = (down, t, up)

    barrier = pltpu.get_barrier_semaphore()
    for dev in ((down, u), (up, u), (down, left), (t, left), (up, left), (down, right), (t, right), (up, right)):
        pl.semaphore_signal(barrier, inc=1, device_id=dev, device_id_type=MESH)

    for row in range(2):
        for h in range(2):
            count = jnp.broadcast_to(cnt[0, pl.ds(h * 2 + row, 1), :], (8, LN))
            for g in range(4):
                rows = pl.ds(g * 32 + h * 2 + row, 8, stride=4)
                dst = (row, h, pl.ds(g * 8, 8))
                for c in range(3):
                    st[(c,) + dst] = off[c, rows, :] * 4.0
                    st[(3 + c,) + dst] = vel[c, rows, :] * 16.0
                slot = lax.broadcasted_iota(jnp.int32, (8, LN), 0) + g * 8
                st[(6,) + dst] = jnp.where(slot < count, mass[rows, :] * (KERNEL_NORM / 64.0), 0.0)
                e = ent[rows, :]
                sq[(0,) + dst] = e
                sq[(1,) + dst] = jnp.sqrt(e * (5.0 / 3.0))
                pr[(2,) + dst] = jnp.full((8, LN), 4.0, jnp.float32)
    pl.semaphore_wait(barrier, 8)

    lane = lane_iota()

    def start_round(rnd, src, ncomp, n, inbox):
        for side in range(2):
            for g in range(n // 8):
                packed = jnp.zeros((8, LN), jnp.float32)
                for c in range(ncomp):
                    for row in range(2):
                        code = c * 2 + row
                        v = src[c, row, side, pl.ds(g * 8, 8), :]
                        from_lane = 127 if side == 1 else 0
                        v = pltpu.roll(v, (code - from_lane) % LN, 1)
                        packed = jnp.where(lane == code, v, packed)
                ysend[rnd, side, pl.ds(g * 8, 8), :] = packed
        copies = []
        for row, dst_t, slot in ((0, down, 1), (1, up, 0)):
            f = row
            copies.append(
                pltpu.make_async_remote_copy(
                    src_ref=src.at[pl.ds(0, ncomp), row, :, pl.ds(0, n)],
                    dst_ref=inbox.at[rnd // 2, slot, pl.ds(0, ncomp), :, pl.ds(0, n)],
                    send_sem=send_sem.at[rnd, f],
                    recv_sem=recv_sem.at[rnd, f],
                    device_id=(dst_t, u),
                    device_id_type=MESH,
                )
            )
        for dt in range(3):
            for side in range(2):
                f = 2 + dt * 2 + side
                copies.append(
                    pltpu.make_async_remote_copy(
                        src_ref=ysend.at[rnd, side, pl.ds(0, n)],
                        dst_ref=yin.at[rnd, 2 - dt, 1 - side, pl.ds(0, n)],
                        send_sem=send_sem.at[rnd, f],
                        recv_sem=recv_sem.at[rnd, f],
                        device_id=(tile_of[dt], right if side == 1 else left),
                        device_id_type=MESH,
                    )
                )
        for f in (4, 5, 0, 1, 2, 3, 6, 7):
            copies[f].start()
        return copies

    def shift_of(comp, r):
        return 4.0 * (r - 1) if comp == X else 0.0

    def centre(load, comps, r, n):
        for c, comp in enumerate(comps):
            for h in range(2):
                v = load(c, h, pl.ds(0, n))
                if comp == X and r != 1:
                    v = v + 4.0 * (r - 1)
                fld[field(r, comp, 1, h), pl.ds(0, n), :] = v

    def sides(load, comps, r, n, rnd, dt, sender_row):
        for c, comp in enumerate(comps):
            code = c * 2 + sender_row
            dx = 4.0 * (r - 1) if comp == X else 0.0
            for g in range(n // 8):
                rows = pl.ds(g * 8, 8)
                a0, a1 = load(c, 0, rows), load(c, 1, rows)
                lo = pltpu.roll(yin[rnd, dt, 0, rows, :], (0 - code) % LN, 1)
                hi = pltpu.roll(yin[rnd, dt, 1, rows, :], (127 - code) % LN, 1)
                r0, r1 = pltpu.roll(a0, 1, 1), pltpu.roll(a1, 1, 1)
                l0, l1 = pltpu.roll(a0, 127, 1), pltpu.roll(a1, 127, 1)
                first, last = lane == 0, lane == 127
                minus = [jnp.where(first, lo, r0), jnp.where(first, r0, r1)]
                plus = [jnp.where(last, l1, l0), jnp.where(last, hi, l1)]
                for h in range(2):
                    m, p = minus[h], plus[h]
                    if comp == Y:
                        m, p = m - 4.0, p + 4.0
                    elif comp == X and r != 1:
                        m, p = m + dx, p + dx
                    fld[field(r, comp, 0, h), rows, :] = m
                    fld[field(r, comp, 2, h), rows, :] = p

    def other(r, comp, b, h, j):
        return fld[field(r, comp, b, h), pl.ds(j, 8, stride=0), :]

    def own(row, comp, h, g, n):
        return fld[field(row + 1, comp, 1, h), pl.ds(g * 8, n * 8), :].reshape(n, 8, LN)

    def density_stage(stage, k):
        per = NACT[k] // 8
        unroll = (16, 16, 16)[k]
        base = STAGE_BASE[stage]

        def combo(ch, _):
            c, h = ch // 2, ch % 2
            row, r, b = stage_ids(stage, c)
            xi, yi, zi = (own(row, comp, h, 0, per) for comp in (X, Y, Z))
            slot = (base + c) * 2 + h
            total0 = dens[row, h, pl.ds(0, per * 8), :].reshape(per, 8, LN)

            def block(jb, total):
                for jj in range(unroll):
                    j = jb * unroll + jj
                    dx = xi - other(r, X, b, h, j)
                    dy = yi - other(r, Y, b, h, j)
                    dz = zi - other(r, Z, b, h, j)
                    r2 = dx * dx + dy * dy + dz * dz
                    rad = r2 * lax.rsqrt(jnp.maximum(r2, 1e-30))
                    s = jnp.maximum(4.0 - rad, 0.0)
                    w3 = (s * other(r, MS, b, h, j)) * (s * s)
                    total = total + w3 * (s * (5.0 - s))
                    at = slot * S + j
                    cache_w[at, pl.ds(0, per)] = w3
                    cache_a[at, pl.ds(0, per)] = r2 + 0.16
                return total

            total = lax.fori_loop(0, S // unroll, block, total0)
            dens[row, h, pl.ds(0, per * 8), :] = total.reshape(per * 8, LN)
            return 0

        lax.fori_loop(0, STAGE_SIZE[stage] * 2, combo, 0)

    def force_stage(stage, k):
        groups = NACT[k] // 8
        per = min(groups, 2)
        sets = groups // per
        unroll = (8, 8, 16)[k]
        base = STAGE_BASE[stage]

        def combo(chg, _):
            ch, g = chg // sets, (chg % sets) * per
            c, h = ch // 2, ch % 2
            row, r, b = stage_ids(stage, c)
            xi, yi, zi, vxi, vyi, vzi, qi, ci, ri = (
                own(row, comp, h, g, per) for comp in (X, Y, Z, VX, VY, VZ, Q, C, R)
            )
            slot = (base + c) * 2 + h
            total0 = tuple(acc[d, row, h, pl.ds(g * 8, per * 8), :].reshape(per, 8, LN) for d in range(3))

            def block(jb, total):
                ax, ay, az = total
                for jj in range(unroll):
                    j = jb * unroll + jj
                    at = slot * S + j
                    dx = xi - other(r, X, b, h, j)
                    dy = yi - other(r, Y, b, h, j)
                    dz = zi - other(r, Z, b, h, j)
                    n = (
                        dx * (vxi - other(r, VX, b, h, j))
                        + dy * (vyi - other(r, VY, b, h, j))
                        + dz * (vzi - other(r, VZ, b, h, j))
                    )
                    n = jnp.minimum(n, 0.0)
                    soft = cache_a[at, pl.ds(g, per)]
                    sound = ci + other(r, C, b, h, j)
                    rho = ri + other(r, R, b, h, j)
                    visc = (n * (n - sound * soft)) / ((soft * soft) * rho)
                    f = cache_w[at, pl.ds(g, per)] * (qi + other(r, Q, b, h, j) + visc)
                    ax, ay, az = ax + f * dx, ay + f * dy, az + f * dz
                return ax, ay, az

            total = lax.fori_loop(0, S // unroll, block, total0)
            for d in range(3):
                acc[d, row, h, pl.ds(g * 8, per * 8), :] = total[d].reshape(per * 8, LN)
            return 0

        lax.fori_loop(0, STAGE_SIZE[stage] * 2 * sets, combo, 0)

    def exchange_and_sum(rnd, src, inbox, comps, n, stage_fn, k):
        copies = start_round(rnd, src, len(comps), n, inbox)
        loads = [None] * 4
        for r in (1, 2):
            loads[r] = functools.partial(lambda row, c, h, rows: src[c, row, h, rows, :], r - 1)
        loads[0] = lambda c, h, rows: inbox[rnd // 2, 0, c, h, rows, :]
        loads[3] = lambda c, h, rows: inbox[rnd // 2, 1, c, h, rows, :]
        for r in (1, 2):
            centre(loads[r], comps, r, n)
        stage_fn(0, k)
        copies[4].wait_recv()
        copies[5].wait_recv()
        for r in (1, 2):
            sides(loads[r], comps, r, n, rnd, 1, r - 1)
        stage_fn(1, k)
        for f in (0, 1, 2, 3, 6, 7):
            copies[f].wait_recv()
        for r, dt, sender_row in ((0, 0, 1), (3, 2, 0)):
            centre(loads[r], comps, r, n)
            sides(loads[r], comps, r, n, rnd, dt, sender_row)
        stage_fn(2, k)
        return copies

    for k in range(3):
        n = NACT[k]
        dens[...] = jnp.zeros_like(dens)
        comps = (X, Y, Z, VX, VY, VZ) + ((MS,) if k == 0 else ())
        moved = exchange_and_sum(2 * k, st, xin, comps, NMOVED[k], density_stage, k)
        for row in range(2):
            for h in range(2):
                count = jnp.broadcast_to(cnt[k, pl.ds(h * 2 + row, 1), :], (8, LN))
                for g in range(n // 8):
                    rows = pl.ds(g * 8, 8)
                    slot = lax.broadcasted_iota(jnp.int32, (8, LN), 0) + g * 8
                    rho4 = jnp.where(slot < count, dens[row, h, rows, :], pr[2, row, h, rows, :])
                    root = jnp.exp(jnp.log(rho4 * 0.25) * (1.0 / 3.0))
                    pr[0, row, h, rows, :] = sq[0, row, h, rows, :] / root
                    pr[1, row, h, rows, :] = sq[1, row, h, rows, :] * root
                    pr[2, row, h, rows, :] = rho4
        acc[...] = jnp.zeros_like(acc)
        pressed = exchange_and_sum(2 * k + 1, pr, pin, (Q, C, R), n, force_stage, k)
        for copy in moved + pressed:
            copy.wait_send()
        for row in range(2):
            for h in range(2):
                count = jnp.broadcast_to(cnt[k, pl.ds(h * 2 + row, 1), :], (8, LN))
                for g in range(n // 8):
                    rows = pl.ds(g * 8, 8)
                    slot = lax.broadcasted_iota(jnp.int32, (8, LN), 0) + g * 8
                    active = slot < count
                    for d in range(3):
                        v = st[3 + d, row, h, rows, :]
                        x = st[d, row, h, rows, :]
                        v_new = v + 4.0 * acc[d, row, h, rows, :]
                        st[3 + d, row, h, rows, :] = jnp.where(active, v_new, v)
                        st[d, row, h, rows, :] = jnp.where(active, x + 0.0125 * v_new, x)

    for row in range(2):
        for h in range(2):
            count = jnp.broadcast_to(cnt[0, pl.ds(h * 2 + row, 1), :], (8, LN))
            for g in range(4):
                rows = pl.ds(g * 8, 8)
                slot = lax.broadcasted_iota(jnp.int32, (8, LN), 0) + g * 8
                in_rows = pl.ds(g * 32 + h * 2 + row, 8, stride=4)
                values = [st[d, row, h, rows, :] * 0.25 for d in range(3)]
                values += [st[3 + d, row, h, rows, :] * 0.0625 for d in range(3)]
                values += [pr[2, row, h, rows, :] * 0.25]
                values += [jnp.where(slot < count, mass[in_rows, :], 0.0)]
                for i, v in enumerate(values):
                    out[pl.ds(((g * 8) * 4 + row * 2 + h) * 8 + i, 8, stride=32), :] = v


def plan_kernel(targets, pos, table):
    tri_r = lax.broadcasted_iota(jnp.int32, (LN, LN), 0)
    tri_c = lax.broadcasted_iota(jnp.int32, (LN, LN), 1)
    before = (tri_r < tri_c).astype(jnp.bfloat16)
    ones = jnp.ones((LN, LN), jnp.bfloat16)
    order_r = (tri_r // 4) * 4 + (tri_r % 2) * 2 + (tri_r // 2) % 2
    order_c = (tri_c // 4) * 4 + (tri_c % 2) * 2 + (tri_c // 2) % 2
    earlier = (order_c < order_r).astype(jnp.bfloat16)
    dest = targets[...]
    start = jnp.zeros((LN, LN), jnp.float32)
    place = jnp.zeros((LN, LN), jnp.float32)
    info = jnp.zeros((LN, LN), jnp.float32)
    for d in range(4):
        mine = dest == d
        hot = jnp.where(mine, 1.0, 0.0).astype(jnp.bfloat16)
        inside = jnp.dot(hot, before, preferred_element_type=jnp.float32)
        counts = jnp.dot(hot, ones, preferred_element_type=jnp.float32)
        base = jnp.dot(earlier, counts.astype(jnp.bfloat16), preferred_element_type=jnp.float32)
        place = jnp.where(mine, start + inside, place)
        info = jnp.where(tri_c == d, base, info)
        info = jnp.where(tri_c == 4 + d, start, info)
        info = jnp.where(tri_c == 8 + d, counts, info)
        start = start + counts
    pos[...] = place.astype(jnp.int32)
    table[...] = info.astype(jnp.int32)


TILES = 48


def route_kernel(table, pos, state, out, order):
    row_q = lax.broadcasted_iota(jnp.int32, (LN, LN), 0)
    lane = lane_iota()
    unroll = 8

    def sort(i, _):
        for jj in range(unroll):
            ch = i * unroll + jj
            src = (ch // 4) * 4 + (ch % 2) * 2 + (ch // 2) % 2
            hot = jnp.where(row_q == jnp.broadcast_to(pos[pl.ds(src, 1), :], (LN, LN)), 1.0, 0.0).astype(jnp.bfloat16)
            v = state[pl.ds(ch * 8, 8), :]
            hi = v.astype(jnp.bfloat16)
            rest = v - hi.astype(jnp.float32)
            mid = rest.astype(jnp.bfloat16)
            low = (rest - mid.astype(jnp.float32)).astype(jnp.bfloat16)
            pieces = jnp.concatenate([hi, mid, low], axis=0)
            moved = lax.dot_general(pieces, hot, (((1,), (1,)), ((), ())), preferred_element_type=jnp.float32)
            order[ch] = (moved[0:8] + moved[8:16]) + moved[16:24]
        return 0

    out[...] = jnp.zeros_like(out)
    lax.fori_loop(0, LN // unroll, sort, 0)

    def lay(ch, _):
        src = (ch // 4) * 4 + (ch % 2) * 2 + (ch // 2) % 2
        v = order[ch]
        for d in range(4):
            base = table[src, d]
            start = table[src, 4 + d]
            count = table[src, 8 + d]
            w = base // LN
            skip = base - w * LN
            turned = pltpu.roll(v, lax.rem(skip - start + 2 * LN, LN), 1)
            keep = (lane >= skip) & (lane < skip + count)
            out[d, w] = jnp.where(keep, turned, out[d, w])
            out[d, w + 1] = jnp.where(lane < skip + count - LN, turned, out[d, w + 1])
        return 0

    lax.fori_loop(0, LN, lay, 0, unroll=2)


def exchange_kernel(subs, buf, out, local_sem, send_sem, recv_sem):
    t, u = lax.axis_index("tile"), lax.axis_index("sub")
    barrier = pltpu.get_barrier_semaphore()
    for k in range(1, subs):
        pl.semaphore_signal(barrier, inc=1, device_id=(t, lax.rem(u + k, subs)), device_id_type=MESH)
    pl.semaphore_wait(barrier, subs - 1)
    copies = []
    for k in (2, 1, 3):
        dst = lax.rem(u + k, subs)
        copy = pltpu.make_async_remote_copy(
            src_ref=buf.at[dst, pl.ds(0, TILES)],
            dst_ref=out.at[pl.ds(u * TILES, TILES)],
            send_sem=send_sem.at[k],
            recv_sem=recv_sem.at[k],
            device_id=(t, dst),
            device_id_type=MESH,
        )
        copy.start()
        copies.append(copy)
    mine = pltpu.make_async_copy(buf.at[u, pl.ds(0, TILES)], out.at[pl.ds(u * TILES, TILES)], local_sem)
    mine.start()
    mine.wait()
    for copy in copies:
        copy.wait_send()
    for copy in copies:
        copy.wait_recv()


def rows_of(a):
    lead = a.shape[:-2]
    a = a.reshape(lead + (2, 2, LN))
    a = jnp.swapaxes(a, -3, -2)
    return a


def shards(tiles, subs, offsets, velocity, mass, entropy, active_counts, targets):
    off = rows_of(offsets).reshape(3, LN, LN)
    vel = rows_of(velocity).reshape(3, LN, LN)
    mas = rows_of(mass).reshape(LN, LN)
    ent = rows_of(entropy).reshape(LN, LN)
    cnt = rows_of(active_counts).reshape(3, 4, LN)
    tgt = rows_of(targets).reshape(LN, LN)
    vmem = pl.BlockSpec(memory_space=pltpu.VMEM)
    f32 = jnp.float32
    pos, table = pl.pallas_call(
        plan_kernel,
        out_shape=[jax.ShapeDtypeStruct((LN, LN), jnp.int32)] * 2,
        in_specs=[vmem],
        out_specs=[vmem] * 2,
        name="plan",
    )(tgt)
    state = pl.pallas_call(
        functools.partial(substeps_kernel, tiles, subs),
        out_shape=jax.ShapeDtypeStruct((8 * LN, LN), f32),
        in_specs=[vmem] * 5,
        out_specs=vmem,
        scratch_shapes=[
            pltpu.VMEM((4 * NF * 6, S, LN), f32),
            pltpu.VMEM((7, 2, 2, S, LN), f32),
            pltpu.VMEM((3, 2, 2, S, LN), f32),
            pltpu.VMEM((2, 2, S, LN), f32),
            pltpu.VMEM((3, 2, 2, S, LN), f32),
            pltpu.VMEM((2, 2, 2, S, LN), f32),
            pltpu.VMEM((6, 2, S, LN), f32),
            pltpu.VMEM((3, 2, 7, 2, S, LN), f32),
            pltpu.VMEM((3, 2, 3, 2, S, LN), f32),
            pltpu.VMEM((6, 3, 2, S, LN), f32),
            pltpu.VMEM((18 * 2 * S, 4, 8, LN), f32),
            pltpu.VMEM((18 * 2 * S, 4, 8, LN), f32),
            pltpu.SemaphoreType.DMA((6, 8)),
            pltpu.SemaphoreType.DMA((6, 8)),
        ],
        compiler_params=pltpu.CompilerParams(collective_id=0, has_side_effects=True, vmem_limit_bytes=62 * 1024 * 1024),
        name="substeps",
    )(off, vel, mas, ent, cnt)
    buf = pl.pallas_call(
        route_kernel,
        out_shape=jax.ShapeDtypeStruct((subs, TILES + 2, 8, LN), f32),
        in_specs=[pl.BlockSpec(memory_space=pltpu.SMEM), vmem, vmem],
        out_specs=vmem,
        scratch_shapes=[pltpu.VMEM((LN, 8, LN), f32)],
        name="route",
    )(table, pos, state)
    arrived = pl.pallas_call(
        functools.partial(exchange_kernel, subs),
        out_shape=jax.ShapeDtypeStruct((subs * TILES, 8, LN), f32),
        in_specs=[vmem],
        out_specs=vmem,
        scratch_shapes=[pltpu.SemaphoreType.DMA, pltpu.SemaphoreType.DMA((4,)), pltpu.SemaphoreType.DMA((4,))],
        compiler_params=pltpu.CompilerParams(collective_id=1, has_side_effects=True),
        name="exchange",
    )(buf)
    return jnp.transpose(arrived, (1, 0, 2)).reshape(8, subs * TILES * LN)


def solution(mesh):
    tiles, subs = mesh.shape["tile"], mesh.shape["sub"]
    placed = (
        P(None, None, "tile", "sub"),
        P(None, None, "tile", "sub"),
        P(None, "tile", "sub"),
        P(None, "tile", "sub"),
        P(None, "tile", "sub"),
        P(None, "tile", "sub"),
    )
    return jax.shard_map(
        functools.partial(shards, tiles, subs),
        mesh=mesh,
        in_specs=placed,
        out_specs=P(None, ("tile", "sub")),
        check_vma=False,
    )
```

```python
import functools
import math

import jax
import jax.numpy as jnp
from jax import lax
from jax.experimental import pallas as pl
from jax.experimental.pallas import tpu as pltpu
from jax.sharding import PartitionSpec as P

MESH = pl.DeviceIdType.MESH

S = 32
LN = 128
KERNEL_NORM = 21.0 / (2.0 * math.pi)
NACT = (32, 16, 8)
NMOVED = (32, 32, 16)

X, Y, Z, VX, VY, VZ, MS, Q, C, R = range(10)
NF = 10


def field(row, comp, b, h):
    return ((row * NF + comp) * 3 + b) * 2 + h


def lane_iota():
    return lax.broadcasted_iota(jnp.int32, (8, LN), 1)


def stage_ids(stage, c):
    if stage == 0:
        return c // 2, 1 + c % 2, 1
    if stage == 1:
        return c // 4, 1 + (c // 2) % 2, 2 * (c % 2)
    return c // 3, 3 * (c // 3), c % 3


STAGE_SIZE = (4, 8, 6)
STAGE_BASE = (0, 4, 12)


def substeps_kernel(
    tiles, subs, off, vel, mass, ent, cnt, out, fld, st, pr, dens, acc, sq, ysend, xin, pin, yin,
    cache_w, cache_a, send_sem, recv_sem
):
    t, u = lax.axis_index("tile"), lax.axis_index("sub")
    up, down = lax.rem(t + 1, tiles), lax.rem(t + tiles - 1, tiles)
    right, left = lax.rem(u + 1, subs), lax.rem(u + subs - 1, subs)
    tile_of = (down, t, up)

    barrier = pltpu.get_barrier_semaphore()
    for dev in ((down, u), (up, u), (down, left), (t, left), (up, left), (down, right), (t, right), (up, right)):
        pl.semaphore_signal(barrier, inc=1, device_id=dev, device_id_type=MESH)

    for row in range(2):
        for h in range(2):
            count = jnp.broadcast_to(cnt[0, pl.ds(h * 2 + row, 1), :], (8, LN))
            for g in range(4):
                rows = pl.ds(g * 32 + h * 2 + row, 8, stride=4)
                dst = (row, h, pl.ds(g * 8, 8))
                for c in range(3):
                    st[(c,) + dst] = off[c, rows, :] * 4.0
                    st[(3 + c,) + dst] = vel[c, rows, :] * 16.0
                slot = lax.broadcasted_iota(jnp.int32, (8, LN), 0) + g * 8
                st[(6,) + dst] = jnp.where(slot < count, mass[rows, :] * (KERNEL_NORM / 64.0), 0.0)
                e = ent[rows, :]
                sq[(0,) + dst] = e
                sq[(1,) + dst] = jnp.sqrt(e * (5.0 / 3.0))
                pr[(2,) + dst] = jnp.full((8, LN), 4.0, jnp.float32)
    pl.semaphore_wait(barrier, 8)

    lane = lane_iota()

    def start_round(rnd, src, ncomp, n, inbox):
        for side in range(2):
            for g in range(n // 8):
                packed = jnp.zeros((8, LN), jnp.float32)
                for c in range(ncomp):
                    for row in range(2):
                        code = c * 2 + row
                        v = src[c, row, side, pl.ds(g * 8, 8), :]
                        from_lane = 127 if side == 1 else 0
                        v = pltpu.roll(v, (code - from_lane) % LN, 1)
                        packed = jnp.where(lane == code, v, packed)
                ysend[rnd, side, pl.ds(g * 8, 8), :] = packed
        copies = []
        for row, dst_t, slot in ((0, down, 1), (1, up, 0)):
            f = row
            copies.append(
                pltpu.make_async_remote_copy(
                    src_ref=src.at[pl.ds(0, ncomp), row, :, pl.ds(0, n)],
                    dst_ref=inbox.at[rnd // 2, slot, pl.ds(0, ncomp), :, pl.ds(0, n)],
                    send_sem=send_sem.at[rnd, f],
                    recv_sem=recv_sem.at[rnd, f],
                    device_id=(dst_t, u),
                    device_id_type=MESH,
                )
            )
        for dt in range(3):
            for side in range(2):
                f = 2 + dt * 2 + side
                copies.append(
                    pltpu.make_async_remote_copy(
                        src_ref=ysend.at[rnd, side, pl.ds(0, n)],
                        dst_ref=yin.at[rnd, 2 - dt, 1 - side, pl.ds(0, n)],
                        send_sem=send_sem.at[rnd, f],
                        recv_sem=recv_sem.at[rnd, f],
                        device_id=(tile_of[dt], right if side == 1 else left),
                        device_id_type=MESH,
                    )
                )
        for f in (4, 5, 0, 1, 2, 3, 6, 7):
            copies[f].start()
        return copies

    def shift_of(comp, r):
        return 4.0 * (r - 1) if comp == X else 0.0

    def centre(load, comps, r, n):
        for c, comp in enumerate(comps):
            for h in range(2):
                v = load(c, h, pl.ds(0, n))
                if comp == X and r != 1:
                    v = v + 4.0 * (r - 1)
                fld[field(r, comp, 1, h), pl.ds(0, n), :] = v

    def sides(load, comps, r, n, rnd, dt, sender_row):
        for c, comp in enumerate(comps):
            code = c * 2 + sender_row
            dx = 4.0 * (r - 1) if comp == X else 0.0
            for g in range(n // 8):
                rows = pl.ds(g * 8, 8)
                a0, a1 = load(c, 0, rows), load(c, 1, rows)
                lo = pltpu.roll(yin[rnd, dt, 0, rows, :], (0 - code) % LN, 1)
                hi = pltpu.roll(yin[rnd, dt, 1, rows, :], (127 - code) % LN, 1)
                r0, r1 = pltpu.roll(a0, 1, 1), pltpu.roll(a1, 1, 1)
                l0, l1 = pltpu.roll(a0, 127, 1), pltpu.roll(a1, 127, 1)
                first, last = lane == 0, lane == 127
                minus = [jnp.where(first, lo, r0), jnp.where(first, r0, r1)]
                plus = [jnp.where(last, l1, l0), jnp.where(last, hi, l1)]
                for h in range(2):
                    m, p = minus[h], plus[h]
                    if comp == Y:
                        m, p = m - 4.0, p + 4.0
                    elif comp == X and r != 1:
                        m, p = m + dx, p + dx
                    fld[field(r, comp, 0, h), rows, :] = m
                    fld[field(r, comp, 2, h), rows, :] = p

    def other(r, comp, b, h, j):
        return fld[field(r, comp, b, h), pl.ds(j, 8, stride=0), :]

    def own(row, comp, h, g, n):
        return fld[field(row + 1, comp, 1, h), pl.ds(g * 8, n * 8), :].reshape(n, 8, LN)

    def density_stage(stage, k):
        per = NACT[k] // 8
        halves = 2 if per == 1 else 1
        base = STAGE_BASE[stage]

        def pairs(c, h):
            row, r, b = stage_ids(stage, c)
            xi, yi, zi = (own(row, comp, h, 0, per) for comp in (X, Y, Z))
            slot = (base + c) * 2 + h
            total = dens[row, h, pl.ds(0, per * 8), :].reshape(per, 8, LN)
            for j in range(S):
                dx = xi - other(r, X, b, h, j)
                dy = yi - other(r, Y, b, h, j)
                dz = zi - other(r, Z, b, h, j)
                r2 = dx * dx + dy * dy + dz * dz
                rad = r2 * lax.rsqrt(jnp.maximum(r2, 1e-30))
                s = jnp.maximum(4.0 - rad, 0.0)
                w3 = (s * other(r, MS, b, h, j)) * (s * s)
                total = total + w3 * (s * (5.0 - s))
                cache_w[slot * S + j, pl.ds(0, per)] = w3
                cache_a[slot * S + j, pl.ds(0, per)] = 1.0 / (r2 + 0.16)
            dens[row, h, pl.ds(0, per * 8), :] = total.reshape(per * 8, LN)

        def combo(i, _):
            if halves == 2:
                pairs(i, 0)
                pairs(i, 1)
            else:
                pairs(i // 2, i % 2)
            return 0

        lax.fori_loop(0, STAGE_SIZE[stage] * 2 // halves, combo, 0)

    def force_stage(stage, k):
        groups = NACT[k] // 8
        per = min(groups, 2)
        sets = groups // per
        halves = 2 if per == 1 else 1
        base = STAGE_BASE[stage]

        def pairs(c, h, g):
            row, r, b = stage_ids(stage, c)
            xi, yi, zi, vxi, vyi, vzi, qi, ci, ri = (
                own(row, comp, h, g, per) for comp in (X, Y, Z, VX, VY, VZ, Q, C, R)
            )
            slot = (base + c) * 2 + h
            ax, ay, az = (acc[d, row, h, pl.ds(g * 8, per * 8), :].reshape(per, 8, LN) for d in range(3))
            for j in range(S):
                dx = xi - other(r, X, b, h, j)
                dy = yi - other(r, Y, b, h, j)
                dz = zi - other(r, Z, b, h, j)
                n = (
                    dx * (vxi - other(r, VX, b, h, j))
                    + dy * (vyi - other(r, VY, b, h, j))
                    + dz * (vzi - other(r, VZ, b, h, j))
                )
                mu = jnp.minimum(n, 0.0) * cache_a[slot * S + j, pl.ds(g, per)]
                sound = ci + other(r, C, b, h, j)
                visc = (mu * (mu - sound)) / (ri + other(r, R, b, h, j))
                f = cache_w[slot * S + j, pl.ds(g, per)] * (qi + other(r, Q, b, h, j) + visc)
                ax, ay, az = ax + f * dx, ay + f * dy, az + f * dz
            for d, total in enumerate((ax, ay, az)):
                acc[d, row, h, pl.ds(g * 8, per * 8), :] = total.reshape(per * 8, LN)

        def combo(i, _):
            if halves == 2:
                pairs(i, 0, 0)
                pairs(i, 1, 0)
            else:
                ch, g = i // sets, (i % sets) * per
                pairs(ch // 2, ch % 2, g)
            return 0

        lax.fori_loop(0, STAGE_SIZE[stage] * 2 * sets // halves, combo, 0)

    def exchange_and_sum(rnd, src, inbox, comps, n, stage_fn, k):
        copies = start_round(rnd, src, len(comps), n, inbox)
        loads = [None] * 4
        for r in (1, 2):
            loads[r] = functools.partial(lambda row, c, h, rows: src[c, row, h, rows, :], r - 1)
        loads[0] = lambda c, h, rows: inbox[rnd // 2, 0, c, h, rows, :]
        loads[3] = lambda c, h, rows: inbox[rnd // 2, 1, c, h, rows, :]
        for r in (1, 2):
            centre(loads[r], comps, r, n)
        stage_fn(0, k)
        copies[4].wait_recv()
        copies[5].wait_recv()
        for r in (1, 2):
            sides(loads[r], comps, r, n, rnd, 1, r - 1)
        stage_fn(1, k)
        for f in (0, 1, 2, 3, 6, 7):
            copies[f].wait_recv()
        for r, dt, sender_row in ((0, 0, 1), (3, 2, 0)):
            centre(loads[r], comps, r, n)
            sides(loads[r], comps, r, n, rnd, dt, sender_row)
        stage_fn(2, k)
        return copies

    for k in range(3):
        n = NACT[k]
        dens[...] = jnp.zeros_like(dens)
        comps = (X, Y, Z, VX, VY, VZ) + ((MS,) if k == 0 else ())
        moved = exchange_and_sum(2 * k, st, xin, comps, NMOVED[k], density_stage, k)
        for row in range(2):
            for h in range(2):
                count = jnp.broadcast_to(cnt[k, pl.ds(h * 2 + row, 1), :], (8, LN))
                for g in range(n // 8):
                    rows = pl.ds(g * 8, 8)
                    slot = lax.broadcasted_iota(jnp.int32, (8, LN), 0) + g * 8
                    rho4 = jnp.where(slot < count, dens[row, h, rows, :], pr[2, row, h, rows, :])
                    root = jnp.exp(jnp.log(rho4 * 0.25) * (1.0 / 3.0))
                    pr[0, row, h, rows, :] = sq[0, row, h, rows, :] / root
                    pr[1, row, h, rows, :] = sq[1, row, h, rows, :] * root
                    pr[2, row, h, rows, :] = rho4
        acc[...] = jnp.zeros_like(acc)
        pressed = exchange_and_sum(2 * k + 1, pr, pin, (Q, C, R), n, force_stage, k)
        for copy in moved + pressed:
            copy.wait_send()
        for row in range(2):
            for h in range(2):
                count = jnp.broadcast_to(cnt[k, pl.ds(h * 2 + row, 1), :], (8, LN))
                for g in range(n // 8):
                    rows = pl.ds(g * 8, 8)
                    slot = lax.broadcasted_iota(jnp.int32, (8, LN), 0) + g * 8
                    active = slot < count
                    for d in range(3):
                        v = st[3 + d, row, h, rows, :]
                        x = st[d, row, h, rows, :]
                        v_new = v + 4.0 * acc[d, row, h, rows, :]
                        st[3 + d, row, h, rows, :] = jnp.where(active, v_new, v)
                        st[d, row, h, rows, :] = jnp.where(active, x + 0.0125 * v_new, x)

    for row in range(2):
        for h in range(2):
            count = jnp.broadcast_to(cnt[0, pl.ds(h * 2 + row, 1), :], (8, LN))
            for g in range(4):
                rows = pl.ds(g * 8, 8)
                slot = lax.broadcasted_iota(jnp.int32, (8, LN), 0) + g * 8
                in_rows = pl.ds(g * 32 + h * 2 + row, 8, stride=4)
                values = [st[d, row, h, rows, :] * 0.25 for d in range(3)]
                values += [st[3 + d, row, h, rows, :] * 0.0625 for d in range(3)]
                values += [pr[2, row, h, rows, :] * 0.25]
                values += [jnp.where(slot < count, mass[in_rows, :], 0.0)]
                for i, v in enumerate(values):
                    out[pl.ds(((g * 8) * 4 + row * 2 + h) * 8 + i, 8, stride=32), :] = v


def plan_kernel(targets, pos, table):
    tri_r = lax.broadcasted_iota(jnp.int32, (LN, LN), 0)
    tri_c = lax.broadcasted_iota(jnp.int32, (LN, LN), 1)
    before = (tri_r < tri_c).astype(jnp.bfloat16)
    ones = jnp.ones((LN, LN), jnp.bfloat16)
    order_r = (tri_r // 4) * 4 + (tri_r % 2) * 2 + (tri_r // 2) % 2
    order_c = (tri_c // 4) * 4 + (tri_c % 2) * 2 + (tri_c // 2) % 2
    earlier = (order_c < order_r).astype(jnp.bfloat16)
    dest = targets[...]
    start = jnp.zeros((LN, LN), jnp.float32)
    place = jnp.zeros((LN, LN), jnp.float32)
    info = jnp.zeros((LN, LN), jnp.float32)
    for d in range(4):
        mine = dest == d
        hot = jnp.where(mine, 1.0, 0.0).astype(jnp.bfloat16)
        inside = jnp.dot(hot, before, preferred_element_type=jnp.float32)
        counts = jnp.dot(hot, ones, preferred_element_type=jnp.float32)
        base = jnp.dot(earlier, counts.astype(jnp.bfloat16), preferred_element_type=jnp.float32)
        place = jnp.where(mine, start + inside, place)
        info = jnp.where(tri_c == d, base, info)
        info = jnp.where(tri_c == 4 + d, start, info)
        info = jnp.where(tri_c == 8 + d, counts, info)
        start = start + counts
    pos[...] = place.astype(jnp.int32)
    table[...] = info.astype(jnp.int32)


TILES = 48


def route_kernel(table, pos, state, out, order):
    row_q = lax.broadcasted_iota(jnp.int32, (LN, LN), 0)
    lane = lane_iota()
    unroll = 8

    def sort(i, _):
        for jj in range(unroll):
            ch = i * unroll + jj
            src = (ch // 4) * 4 + (ch % 2) * 2 + (ch // 2) % 2
            hot = jnp.where(row_q == jnp.broadcast_to(pos[pl.ds(src, 1), :], (LN, LN)), 1.0, 0.0).astype(jnp.bfloat16)
            v = state[pl.ds(ch * 8, 8), :]
            hi = v.astype(jnp.bfloat16)
            rest = v - hi.astype(jnp.float32)
            mid = rest.astype(jnp.bfloat16)
            low = (rest - mid.astype(jnp.float32)).astype(jnp.bfloat16)
            pieces = jnp.concatenate([hi, mid, low], axis=0)
            moved = lax.dot_general(pieces, hot, (((1,), (1,)), ((), ())), preferred_element_type=jnp.float32)
            order[ch] = (moved[0:8] + moved[8:16]) + moved[16:24]
        return 0

    out[...] = jnp.zeros_like(out)
    lax.fori_loop(0, LN // unroll, sort, 0)

    def lay(ch, _):
        src = (ch // 4) * 4 + (ch % 2) * 2 + (ch // 2) % 2
        v = order[ch]
        for d in range(4):
            base = table[src, d]
            start = table[src, 4 + d]
            count = table[src, 8 + d]
            w = base // LN
            skip = base - w * LN
            turned = pltpu.roll(v, lax.rem(skip - start + 2 * LN, LN), 1)
            keep = (lane >= skip) & (lane < skip + count)
            out[d, w] = jnp.where(keep, turned, out[d, w])
            out[d, w + 1] = jnp.where(lane < skip + count - LN, turned, out[d, w + 1])
        return 0

    lax.fori_loop(0, LN, lay, 0, unroll=2)


def exchange_kernel(subs, buf, out, local_sem, send_sem, recv_sem):
    t, u = lax.axis_index("tile"), lax.axis_index("sub")
    barrier = pltpu.get_barrier_semaphore()
    for k in range(1, subs):
        pl.semaphore_signal(barrier, inc=1, device_id=(t, lax.rem(u + k, subs)), device_id_type=MESH)
    pl.semaphore_wait(barrier, subs - 1)
    copies = []
    for k in (2, 1, 3):
        dst = lax.rem(u + k, subs)
        copy = pltpu.make_async_remote_copy(
            src_ref=buf.at[dst, pl.ds(0, TILES)],
            dst_ref=out.at[pl.ds(u * TILES, TILES)],
            send_sem=send_sem.at[k],
            recv_sem=recv_sem.at[k],
            device_id=(t, dst),
            device_id_type=MESH,
        )
        copy.start()
        copies.append(copy)
    mine = pltpu.make_async_copy(buf.at[u, pl.ds(0, TILES)], out.at[pl.ds(u * TILES, TILES)], local_sem)
    mine.start()
    mine.wait()
    for copy in copies:
        copy.wait_send()
    for copy in copies:
        copy.wait_recv()


def rows_of(a):
    lead = a.shape[:-2]
    a = a.reshape(lead + (2, 2, LN))
    a = jnp.swapaxes(a, -3, -2)
    return a


def shards(tiles, subs, offsets, velocity, mass, entropy, active_counts, targets):
    off = rows_of(offsets).reshape(3, LN, LN)
    vel = rows_of(velocity).reshape(3, LN, LN)
    mas = rows_of(mass).reshape(LN, LN)
    ent = rows_of(entropy).reshape(LN, LN)
    cnt = rows_of(active_counts).reshape(3, 4, LN)
    tgt = rows_of(targets).reshape(LN, LN)
    vmem = pl.BlockSpec(memory_space=pltpu.VMEM)
    f32 = jnp.float32
    pos, table = pl.pallas_call(
        plan_kernel,
        out_shape=[jax.ShapeDtypeStruct((LN, LN), jnp.int32)] * 2,
        in_specs=[vmem],
        out_specs=[vmem] * 2,
        name="plan",
    )(tgt)
    state = pl.pallas_call(
        functools.partial(substeps_kernel, tiles, subs),
        out_shape=jax.ShapeDtypeStruct((8 * LN, LN), f32),
        in_specs=[vmem] * 5,
        out_specs=vmem,
        scratch_shapes=[
            pltpu.VMEM((4 * NF * 6, S, LN), f32),
            pltpu.VMEM((7, 2, 2, S, LN), f32),
            pltpu.VMEM((3, 2, 2, S, LN), f32),
            pltpu.VMEM((2, 2, S, LN), f32),
            pltpu.VMEM((3, 2, 2, S, LN), f32),
            pltpu.VMEM((2, 2, 2, S, LN), f32),
            pltpu.VMEM((6, 2, S, LN), f32),
            pltpu.VMEM((3, 2, 7, 2, S, LN), f32),
            pltpu.VMEM((3, 2, 3, 2, S, LN), f32),
            pltpu.VMEM((6, 3, 2, S, LN), f32),
            pltpu.VMEM((18 * 2 * S, 4, 8, LN), f32),
            pltpu.VMEM((18 * 2 * S, 4, 8, LN), f32),
            pltpu.SemaphoreType.DMA((6, 8)),
            pltpu.SemaphoreType.DMA((6, 8)),
        ],
        compiler_params=pltpu.CompilerParams(collective_id=0, has_side_effects=True, vmem_limit_bytes=62 * 1024 * 1024),
        name="substeps",
    )(off, vel, mas, ent, cnt)
    buf = pl.pallas_call(
        route_kernel,
        out_shape=jax.ShapeDtypeStruct((subs, TILES + 2, 8, LN), f32),
        in_specs=[pl.BlockSpec(memory_space=pltpu.SMEM), vmem, vmem],
        out_specs=vmem,
        scratch_shapes=[pltpu.VMEM((LN, 8, LN), f32)],
        name="route",
    )(table, pos, state)
    arrived = pl.pallas_call(
        functools.partial(exchange_kernel, subs),
        out_shape=jax.ShapeDtypeStruct((subs * TILES, 8, LN), f32),
        in_specs=[vmem],
        out_specs=vmem,
        scratch_shapes=[pltpu.SemaphoreType.DMA, pltpu.SemaphoreType.DMA((4,)), pltpu.SemaphoreType.DMA((4,))],
        compiler_params=pltpu.CompilerParams(collective_id=1, has_side_effects=True),
        name="exchange",
    )(buf)
    return jnp.transpose(arrived, (1, 0, 2)).reshape(8, subs * TILES * LN)


def solution(mesh):
    tiles, subs = mesh.shape["tile"], mesh.shape["sub"]
    placed = (
        P(None, None, "tile", "sub"),
        P(None, None, "tile", "sub"),
        P(None, "tile", "sub"),
        P(None, "tile", "sub"),
        P(None, "tile", "sub"),
        P(None, "tile", "sub"),
    )
    return jax.shard_map(
        functools.partial(shards, tiles, subs),
        mesh=mesh,
        in_specs=placed,
        out_specs=P(None, ("tile", "sub")),
        check_vma=False,
    )
```

```python
import functools
import math

import jax
import jax.numpy as jnp
from jax import lax
from jax.experimental import pallas as pl
from jax.experimental.pallas import tpu as pltpu
from jax.sharding import PartitionSpec as P

MESH = pl.DeviceIdType.MESH

S = 32
LN = 128
KERNEL_NORM = 21.0 / (2.0 * math.pi)
NACT = (32, 16, 8)
NMOVED = (32, 32, 16)

X, Y, Z, VX, VY, VZ, MS, Q, C, R = range(10)
NF = 10


def field(row, comp, b, h):
    return ((row * NF + comp) * 3 + b) * 2 + h


def lane_iota():
    return lax.broadcasted_iota(jnp.int32, (8, LN), 1)


def stage_ids(stage, c):
    if stage == 0:
        return c // 2, 1 + c % 2, 1
    if stage == 1:
        return c // 4, 1 + (c // 2) % 2, 2 * (c % 2)
    return c // 3, 3 * (c // 3), c % 3


STAGE_SIZE = (4, 8, 6)
STAGE_BASE = (0, 4, 12)


def substeps_kernel(
    tiles, subs, off, vel, mass, ent, cnt, tgt, gathered, runs, fld, st, pr, dens, acc, sq, ysend, xin, pin, yin,
    cache_w, cache_a, raw, pos, tab, send_sem, recv_sem, tab_send, tab_recv, piece_send, piece_recv
):
    t, u = lax.axis_index("tile"), lax.axis_index("sub")
    up, down = lax.rem(t + 1, tiles), lax.rem(t + tiles - 1, tiles)
    right, left = lax.rem(u + 1, subs), lax.rem(u + subs - 1, subs)
    tile_of = (down, t, up)

    barrier = pltpu.get_barrier_semaphore()
    across = lax.rem(u + 2, subs)
    near = ((down, u), (up, u), (down, left), (t, left), (up, left), (down, right), (t, right), (up, right))
    for dev in near + ((t, across),):
        pl.semaphore_signal(barrier, inc=1, device_id=dev, device_id_type=MESH)

    for row in range(2):
        for h in range(2):
            count = jnp.broadcast_to(cnt[0, pl.ds(h * 2 + row, 1), :], (8, LN))
            for g in range(4):
                rows = pl.ds(g * 32 + h * 2 + row, 8, stride=4)
                dst = (row, h, pl.ds(g * 8, 8))
                for c in range(3):
                    st[(c,) + dst] = off[c, rows, :] * 4.0
                    st[(3 + c,) + dst] = vel[c, rows, :] * 16.0
                slot = lax.broadcasted_iota(jnp.int32, (8, LN), 0) + g * 8
                st[(6,) + dst] = jnp.where(slot < count, mass[rows, :] * (KERNEL_NORM / 64.0), 0.0)
                e = ent[rows, :]
                sq[(0,) + dst] = e
                sq[(1,) + dst] = jnp.sqrt(e * (5.0 / 3.0))
                pr[(2,) + dst] = jnp.full((8, LN), 4.0, jnp.float32)
    pl.semaphore_wait(barrier, 9)

    lane = lane_iota()

    def start_round(rnd, src, ncomp, n, inbox):
        for side in range(2):
            for g in range(n // 8):
                packed = jnp.zeros((8, LN), jnp.float32)
                for c in range(ncomp):
                    for row in range(2):
                        code = c * 2 + row
                        v = src[c, row, side, pl.ds(g * 8, 8), :]
                        from_lane = 127 if side == 1 else 0
                        v = pltpu.roll(v, (code - from_lane) % LN, 1)
                        packed = jnp.where(lane == code, v, packed)
                ysend[rnd, side, pl.ds(g * 8, 8), :] = packed
        copies = []
        for row, dst_t, slot in ((0, down, 1), (1, up, 0)):
            f = row
            copies.append(
                pltpu.make_async_remote_copy(
                    src_ref=src.at[pl.ds(0, ncomp), row, :, pl.ds(0, n)],
                    dst_ref=inbox.at[rnd // 2, slot, pl.ds(0, ncomp), :, pl.ds(0, n)],
                    send_sem=send_sem.at[rnd, f],
                    recv_sem=recv_sem.at[rnd, f],
                    device_id=(dst_t, u),
                    device_id_type=MESH,
                )
            )
        for dt in range(3):
            for side in range(2):
                f = 2 + dt * 2 + side
                copies.append(
                    pltpu.make_async_remote_copy(
                        src_ref=ysend.at[rnd, side, pl.ds(0, n)],
                        dst_ref=yin.at[rnd, 2 - dt, 1 - side, pl.ds(0, n)],
                        send_sem=send_sem.at[rnd, f],
                        recv_sem=recv_sem.at[rnd, f],
                        device_id=(tile_of[dt], right if side == 1 else left),
                        device_id_type=MESH,
                    )
                )
        for f in (4, 5, 0, 1, 2, 3, 6, 7):
            copies[f].start()
        return copies

    def shift_of(comp, r):
        return 4.0 * (r - 1) if comp == X else 0.0

    def centre(load, comps, r, n):
        for c, comp in enumerate(comps):
            for h in range(2):
                v = load(c, h, pl.ds(0, n))
                if comp == X and r != 1:
                    v = v + 4.0 * (r - 1)
                fld[field(r, comp, 1, h), pl.ds(0, n), :] = v

    def sides(load, comps, r, n, rnd, dt, sender_row):
        for c, comp in enumerate(comps):
            code = c * 2 + sender_row
            dx = 4.0 * (r - 1) if comp == X else 0.0
            for g in range(n // 8):
                rows = pl.ds(g * 8, 8)
                a0, a1 = load(c, 0, rows), load(c, 1, rows)
                lo = pltpu.roll(yin[rnd, dt, 0, rows, :], (0 - code) % LN, 1)
                hi = pltpu.roll(yin[rnd, dt, 1, rows, :], (127 - code) % LN, 1)
                r0, r1 = pltpu.roll(a0, 1, 1), pltpu.roll(a1, 1, 1)
                l0, l1 = pltpu.roll(a0, 127, 1), pltpu.roll(a1, 127, 1)
                first, last = lane == 0, lane == 127
                minus = [jnp.where(first, lo, r0), jnp.where(first, r0, r1)]
                plus = [jnp.where(last, l1, l0), jnp.where(last, hi, l1)]
                for h in range(2):
                    m, p = minus[h], plus[h]
                    if comp == Y:
                        m, p = m - 4.0, p + 4.0
                    elif comp == X and r != 1:
                        m, p = m + dx, p + dx
                    fld[field(r, comp, 0, h), rows, :] = m
                    fld[field(r, comp, 2, h), rows, :] = p

    def other(r, comp, b, h, j):
        return fld[field(r, comp, b, h), pl.ds(j, 8, stride=0), :]

    def own(row, comp, h, g, n):
        return fld[field(row + 1, comp, 1, h), pl.ds(g * 8, n * 8), :].reshape(n, 8, LN)

    def density_stage(stage, k):
        per = NACT[k] // 8
        halves = 2 if per == 1 else 1
        base = STAGE_BASE[stage]

        def pairs(c, h):
            row, r, b = stage_ids(stage, c)
            xi, yi, zi = (own(row, comp, h, 0, per) for comp in (X, Y, Z))
            slot = (base + c) * 2 + h
            total = dens[row, h, pl.ds(0, per * 8), :].reshape(per, 8, LN)
            for j in range(S):
                dx = xi - other(r, X, b, h, j)
                dy = yi - other(r, Y, b, h, j)
                dz = zi - other(r, Z, b, h, j)
                r2 = dx * dx + dy * dy + dz * dz
                rad = r2 * lax.rsqrt(jnp.maximum(r2, 1e-30))
                s = jnp.maximum(4.0 - rad, 0.0)
                w3 = (s * other(r, MS, b, h, j)) * (s * s)
                total = total + w3 * (s * (5.0 - s))
                cache_w[slot * S + j, pl.ds(0, per)] = w3
                cache_a[slot * S + j, pl.ds(0, per)] = 1.0 / (r2 + 0.16)
            dens[row, h, pl.ds(0, per * 8), :] = total.reshape(per * 8, LN)

        def combo(i, _):
            if halves == 2:
                pairs(i, 0)
                pairs(i, 1)
            else:
                pairs(i // 2, i % 2)
            return 0

        lax.fori_loop(0, STAGE_SIZE[stage] * 2 // halves, combo, 0)

    def force_stage(stage, k):
        groups = NACT[k] // 8
        per = min(groups, 2)
        sets = groups // per
        halves = 2 if per == 1 else 1
        base = STAGE_BASE[stage]

        def pairs(c, h, g):
            row, r, b = stage_ids(stage, c)
            xi, yi, zi, vxi, vyi, vzi, qi, ci, ri = (
                own(row, comp, h, g, per) for comp in (X, Y, Z, VX, VY, VZ, Q, C, R)
            )
            slot = (base + c) * 2 + h
            ax, ay, az = (acc[d, row, h, pl.ds(g * 8, per * 8), :].reshape(per, 8, LN) for d in range(3))
            for j in range(S):
                dx = xi - other(r, X, b, h, j)
                dy = yi - other(r, Y, b, h, j)
                dz = zi - other(r, Z, b, h, j)
                n = (
                    dx * (vxi - other(r, VX, b, h, j))
                    + dy * (vyi - other(r, VY, b, h, j))
                    + dz * (vzi - other(r, VZ, b, h, j))
                )
                mu = jnp.minimum(n, 0.0) * cache_a[slot * S + j, pl.ds(g, per)]
                sound = ci + other(r, C, b, h, j)
                visc = (mu * (mu - sound)) / (ri + other(r, R, b, h, j))
                f = cache_w[slot * S + j, pl.ds(g, per)] * (qi + other(r, Q, b, h, j) + visc)
                ax, ay, az = ax + f * dx, ay + f * dy, az + f * dz
            for d, total in enumerate((ax, ay, az)):
                acc[d, row, h, pl.ds(g * 8, per * 8), :] = total.reshape(per * 8, LN)

        def combo(i, _):
            if halves == 2:
                pairs(i, 0, 0)
                pairs(i, 1, 0)
            else:
                ch, g = i // sets, (i % sets) * per
                pairs(ch // 2, ch % 2, g)
            return 0

        lax.fori_loop(0, STAGE_SIZE[stage] * 2 * sets // halves, combo, 0)

    def plan():
        row_i = lax.broadcasted_iota(jnp.int32, (LN, LN), 0)
        col_i = lax.broadcasted_iota(jnp.int32, (LN, LN), 1)
        before = jnp.where(row_i < col_i, 1.0, 0.0).astype(jnp.bfloat16)
        ones = jnp.ones((LN, LN), jnp.bfloat16)
        row8 = lax.broadcasted_iota(jnp.int32, (8, LN), 0)
        dest = tgt[...]
        start = jnp.zeros((LN, LN), jnp.float32)
        place = jnp.zeros((LN, LN), jnp.float32)
        start_t = jnp.zeros((8, LN), jnp.float32)
        info = jnp.zeros((8, LN), jnp.float32)
        for d in range(subs):
            mine = dest == d
            hot = jnp.where(mine, 1.0, 0.0).astype(jnp.bfloat16)
            inside = jnp.dot(hot, before, preferred_element_type=jnp.float32)
            place = jnp.where(mine, start + inside, place)
            start = start + jnp.dot(hot, ones, preferred_element_type=jnp.float32)
            count_t = lax.dot_general(
                ones[0:8], hot, (((1,), (1,)), ((), ())), preferred_element_type=jnp.float32
            )
            info = jnp.where(row8 == d, start_t, info)
            info = jnp.where(row8 == subs + d, count_t, info)
            start_t = start_t + count_t
        pos[...] = place.astype(jnp.int32)
        tab[u] = info
        sends = []
        for k in range(1, subs):
            copy = pltpu.make_async_remote_copy(
                src_ref=tab.at[u],
                dst_ref=tab.at[u],
                send_sem=tab_send.at[k],
                recv_sem=tab_recv.at[k],
                device_id=(t, lax.rem(u + k, subs)),
                device_id_type=MESH,
            )
            copy.start()
            sends.append(copy)
        return sends

    def emit(g):
        row_q = lax.broadcasted_iota(jnp.int32, (LN, LN), 0)
        for row in range(2):
            for h in range(2):
                count = jnp.broadcast_to(cnt[0, pl.ds(h * 2 + row, 1), :], (8, LN))
                rows = pl.ds(g * 8, 8)
                slot = lax.broadcasted_iota(jnp.int32, (8, LN), 0) + g * 8
                in_rows = pl.ds(g * 32 + h * 2 + row, 8, stride=4)
                values = [st[d, row, h, rows, :] * 0.25 for d in range(3)]
                values += [st[3 + d, row, h, rows, :] * 0.0625 for d in range(3)]
                values += [pr[2, row, h, rows, :] * 0.25]
                values += [jnp.where(slot < count, mass[in_rows, :], 0.0)]
                for i, v in enumerate(values):
                    raw[g, pl.ds((h * 2 + row) * 64 + i, 8, stride=8), :] = v

        def sort(hr, _):
            for i in range(8):
                at = (g * 8 + i) * 4 + hr
                hot = jnp.where(row_q == jnp.broadcast_to(pos[pl.ds(at, 1), :], (LN, LN)), 1.0, 0.0)
                v = raw[g, pl.ds(hr * 64 + i * 8, 8), :]
                hi = v.astype(jnp.bfloat16)
                rest = v - hi.astype(jnp.float32)
                mid = rest.astype(jnp.bfloat16)
                low = (rest - mid.astype(jnp.float32)).astype(jnp.bfloat16)
                pieces = jnp.concatenate([hi, mid, low], axis=0)
                moved = lax.dot_general(
                    pieces, hot.astype(jnp.bfloat16), (((1,), (1,)), ((), ())), preferred_element_type=jnp.float32
                )
                gathered[u, at] = (moved[0:8] + moved[8:16]) + moved[16:24]
            return 0

        lax.fori_loop(0, 4, sort, 0)

    PIECES = ((64, 64), (32, 32), (0, 32))

    def piece_copy(p, flow, owner, first, rows, dst):
        return pltpu.make_async_remote_copy(
            src_ref=gathered.at[owner, pl.ds(first, rows)],
            dst_ref=gathered.at[owner, pl.ds(first, rows)],
            send_sem=piece_send.at[p, flow],
            recv_sem=piece_recv.at[p, flow],
            device_id=(t, dst),
            device_id_type=MESH,
        )

    def start_piece(p):
        first, rows = PIECES[p]
        for g in range(first // 32, (first + rows) // 32):
            emit(g)
        half = rows // 2
        copies = [
            piece_copy(p, 0, u, first, half, right),
            piece_copy(p, 1, u, first + half, half, right),
            piece_copy(p, 2, u, first + half, half, left),
            piece_copy(p, 3, u, first, half, left),
        ]
        for f in (0, 2, 1, 3):
            copies[f].start()
        return copies

    def forward_piece(p):
        first, rows = PIECES[p]
        half = rows // 2
        copies = [
            piece_copy(p, 4, left, first, half, right),
            piece_copy(p, 5, right, first + half, half, left),
        ]
        for copy in copies:
            copy.start()
        return copies

    def exchange_and_sum(rnd, src, inbox, comps, n, stage_fn, k, meanwhile):
        copies = start_round(rnd, src, len(comps), n, inbox)
        meanwhile()
        loads = [None] * 4
        for r in (1, 2):
            loads[r] = functools.partial(lambda row, c, h, rows: src[c, row, h, rows, :], r - 1)
        loads[0] = lambda c, h, rows: inbox[rnd // 2, 0, c, h, rows, :]
        loads[3] = lambda c, h, rows: inbox[rnd // 2, 1, c, h, rows, :]
        for r in (1, 2):
            centre(loads[r], comps, r, n)
        stage_fn(0, k)
        copies[4].wait_recv()
        copies[5].wait_recv()
        for r in (1, 2):
            sides(loads[r], comps, r, n, rnd, 1, r - 1)
        stage_fn(1, k)
        for f in (0, 1, 2, 3, 6, 7):
            copies[f].wait_recv()
        for r, dt, sender_row in ((0, 0, 1), (3, 2, 0)):
            centre(loads[r], comps, r, n)
            sides(loads[r], comps, r, n, rnd, dt, sender_row)
        stage_fn(2, k)
        return copies

    pending = []
    arriving = {}

    def during(rnd):
        if rnd == 0:
            arriving["tab"] = plan()
        elif rnd in (2, 4):
            arriving[rnd] = start_piece(rnd // 2 - 1)
        elif rnd in (3, 5):
            p = rnd // 2 - 1
            copies = arriving[rnd - 1]
            copies[0].wait_recv()
            copies[2].wait_recv()
            arriving[rnd] = forward_piece(p)

    for k in range(3):
        n = NACT[k]
        dens[...] = jnp.zeros_like(dens)
        comps = (X, Y, Z, VX, VY, VZ) + ((MS,) if k == 0 else ())
        moved = exchange_and_sum(2 * k, st, xin, comps, NMOVED[k], density_stage, k, lambda: during(2 * k))
        for row in range(2):
            for h in range(2):
                count = jnp.broadcast_to(cnt[k, pl.ds(h * 2 + row, 1), :], (8, LN))
                for g in range(n // 8):
                    rows = pl.ds(g * 8, 8)
                    slot = lax.broadcasted_iota(jnp.int32, (8, LN), 0) + g * 8
                    rho4 = jnp.where(slot < count, dens[row, h, rows, :], pr[2, row, h, rows, :])
                    root = jnp.exp(jnp.log(rho4 * 0.25) * (1.0 / 3.0))
                    pr[0, row, h, rows, :] = sq[0, row, h, rows, :] / root
                    pr[1, row, h, rows, :] = sq[1, row, h, rows, :] * root
                    pr[2, row, h, rows, :] = rho4
        acc[...] = jnp.zeros_like(acc)
        pressed = exchange_and_sum(2 * k + 1, pr, pin, (Q, C, R), n, force_stage, k, lambda: during(2 * k + 1))
        for copy in moved + pressed:
            copy.wait_send()
        for row in range(2):
            for h in range(2):
                count = jnp.broadcast_to(cnt[k, pl.ds(h * 2 + row, 1), :], (8, LN))
                for g in range(n // 8):
                    rows = pl.ds(g * 8, 8)
                    slot = lax.broadcasted_iota(jnp.int32, (8, LN), 0) + g * 8
                    active = slot < count
                    for d in range(3):
                        v = st[3 + d, row, h, rows, :]
                        x = st[d, row, h, rows, :]
                        v_new = v + 4.0 * acc[d, row, h, rows, :]
                        st[3 + d, row, h, rows, :] = jnp.where(active, v_new, v)
                        st[d, row, h, rows, :] = jnp.where(active, x + 0.0125 * v_new, x)
    for rnd in (3, 5):
        direct, passed = arriving[rnd - 1], arriving[rnd]
        pending += direct + passed
        for copy in (direct[1], direct[3], passed[0], passed[1]):
            copy.wait_recv()
    pending += arriving["tab"]
    for copy in arriving["tab"]:
        copy.wait_recv()


    copies = start_piece(2)
    copies[0].wait_recv()
    copies[2].wait_recv()
    forward = forward_piece(2)
    pending += copies + forward
    for src in range(subs):
        runs[src : src + 1, :] = tab[src, pl.ds(u, 1), :].astype(jnp.int32)
        runs[subs + src : subs + src + 1, :] = tab[src, pl.ds(subs + u, 1), :].astype(jnp.int32)
    for copy in pending:
        copy.wait_send()
    for copy in (copies[1], copies[3], forward[0], forward[1]):
        copy.wait_recv()


TILES = 48


def lay_kernel(runs, gathered, out, tiles):
    subs = gathered.shape[0]
    lane = lane_iota()
    tiles[...] = jnp.zeros_like(tiles)

    def lay(i, carry):
        bases, currents = carry
        new_bases, new_currents = [], []
        at = (i & ~3) | ((i & 1) << 1) | ((i >> 1) & 1)
        for src in range(subs):
            base, current = bases[src], currents[src]
            start, count = runs[src, at], runs[subs + src, at]
            skip = base & (LN - 1)
            end = skip + count
            turned = pltpu.roll(gathered[src, at], (skip - start) & (LN - 1), 1)
            merged = jnp.where(lane < skip, current, jnp.where(lane < end, turned, 0.0))
            tiles[src, base >> 7] = merged
            wrapped = jnp.where(lane < end - LN, turned, 0.0)
            new_currents.append(jnp.where(end >= LN, wrapped, merged))
            new_bases.append(base + count)
        return tuple(new_bases), tuple(new_currents)

    zero = jnp.zeros((8, LN), jnp.float32)
    bases, currents = lax.fori_loop(
        0, LN, lay, ((jnp.int32(0),) * subs, (zero,) * subs), unroll=2
    )
    for src in range(subs):
        tiles[src, bases[src] >> 7] = currents[src]
    for src in range(subs):
        out[pl.ds(src * TILES, TILES)] = tiles[src, pl.ds(0, TILES)]


def rows_of(a):
    lead = a.shape[:-2]
    a = a.reshape(lead + (2, 2, LN))
    a = jnp.swapaxes(a, -3, -2)
    return a


def shards(tiles, subs, offsets, velocity, mass, entropy, active_counts, targets):
    off = rows_of(offsets).reshape(3, LN, LN)
    vel = rows_of(velocity).reshape(3, LN, LN)
    mas = rows_of(mass).reshape(LN, LN)
    ent = rows_of(entropy).reshape(LN, LN)
    cnt = rows_of(active_counts).reshape(3, 4, LN)
    tgt = rows_of(targets).reshape(LN, LN)
    vmem = pl.BlockSpec(memory_space=pltpu.VMEM)
    f32 = jnp.float32
    gathered, runs = pl.pallas_call(
        functools.partial(substeps_kernel, tiles, subs),
        out_shape=[
            jax.ShapeDtypeStruct((subs, LN, 8, LN), f32),
            jax.ShapeDtypeStruct((2 * subs, LN), jnp.int32),
        ],
        in_specs=[vmem] * 6,
        out_specs=[vmem] * 2,
        scratch_shapes=[
            pltpu.VMEM((4 * NF * 6, S, LN), f32),
            pltpu.VMEM((7, 2, 2, S, LN), f32),
            pltpu.VMEM((3, 2, 2, S, LN), f32),
            pltpu.VMEM((2, 2, S, LN), f32),
            pltpu.VMEM((3, 2, 2, S, LN), f32),
            pltpu.VMEM((2, 2, 2, S, LN), f32),
            pltpu.VMEM((6, 2, S, LN), f32),
            pltpu.VMEM((3, 2, 7, 2, S, LN), f32),
            pltpu.VMEM((3, 2, 3, 2, S, LN), f32),
            pltpu.VMEM((6, 3, 2, S, LN), f32),
            pltpu.VMEM((18 * 2 * S, 4, 8, LN), f32),
            pltpu.VMEM((18 * 2 * S, 4, 8, LN), f32),
            pltpu.VMEM((4, 256, LN), f32),
            pltpu.VMEM((LN, LN), jnp.int32),
            pltpu.VMEM((subs, 2 * subs, LN), f32),
            pltpu.SemaphoreType.DMA((6, 8)),
            pltpu.SemaphoreType.DMA((6, 8)),
            pltpu.SemaphoreType.DMA((4,)),
            pltpu.SemaphoreType.DMA((4,)),
            pltpu.SemaphoreType.DMA((3, 6)),
            pltpu.SemaphoreType.DMA((3, 6)),
        ],
        compiler_params=pltpu.CompilerParams(collective_id=0, has_side_effects=True, vmem_limit_bytes=62 * 1024 * 1024),
        name="substeps",
    )(off, vel, mas, ent, cnt, tgt)
    arrived = pl.pallas_call(
        lay_kernel,
        out_shape=jax.ShapeDtypeStruct((subs * TILES, 8, LN), f32),
        in_specs=[pl.BlockSpec(memory_space=pltpu.SMEM), vmem],
        out_specs=vmem,
        scratch_shapes=[pltpu.VMEM((subs, TILES + 2, 8, LN), f32)],
        name="lay",
    )(runs, gathered)
    return jnp.transpose(arrived, (1, 0, 2)).reshape(8, subs * TILES * LN)


def solution(mesh):
    tiles, subs = mesh.shape["tile"], mesh.shape["sub"]
    placed = (
        P(None, None, "tile", "sub"),
        P(None, None, "tile", "sub"),
        P(None, "tile", "sub"),
        P(None, "tile", "sub"),
        P(None, "tile", "sub"),
        P(None, "tile", "sub"),
    )
    return jax.shard_map(
        functools.partial(shards, tiles, subs),
        mesh=mesh,
        in_specs=placed,
        out_specs=P(None, ("tile", "sub")),
        check_vma=False,
    )
```

```python
import functools
import math

import jax
import jax.numpy as jnp
from jax import lax
from jax.experimental import pallas as pl
from jax.experimental.pallas import tpu as pltpu
from jax.sharding import PartitionSpec as P

MESH = pl.DeviceIdType.MESH

S = 32
LN = 128
KERNEL_NORM = 21.0 / (2.0 * math.pi)
NACT = (32, 16, 8)
NMOVED = (32, 32, 16)

X, Y, Z, VX, VY, VZ, MS, Q, C, R = range(10)
NF = 10


def field(row, comp, b, h):
    return ((row * NF + comp) * 3 + b) * 2 + h


def lane_iota():
    return lax.broadcasted_iota(jnp.int32, (8, LN), 1)


def stage_ids(stage, c):
    if stage == 0:
        return c // 2, 1 + c % 2, 1
    if stage == 1:
        return c // 4, 1 + (c // 2) % 2, 2 * (c % 2)
    return c // 3, 3 * (c // 3), c % 3


STAGE_SIZE = (4, 8, 6)
STAGE_BASE = (0, 4, 12)


def substeps_kernel(
    tiles, subs, off, vel, mass, ent, cnt, tgt, gathered, runs, fld, st, pr, dens, acc, sq, ysend, xin, pin, yin,
    cache_w, cache_a, raw, pos, tab, send_sem, recv_sem, tab_send, tab_recv, piece_send, piece_recv
):
    t, u = lax.axis_index("tile"), lax.axis_index("sub")
    up, down = lax.rem(t + 1, tiles), lax.rem(t + tiles - 1, tiles)
    right, left = lax.rem(u + 1, subs), lax.rem(u + subs - 1, subs)
    tile_of = (down, t, up)

    barrier = pltpu.get_barrier_semaphore()
    across = lax.rem(u + 2, subs)
    near = ((down, u), (up, u), (down, left), (t, left), (up, left), (down, right), (t, right), (up, right))
    for dev in near + ((t, across),):
        pl.semaphore_signal(barrier, inc=1, device_id=dev, device_id_type=MESH)

    for row in range(2):
        for h in range(2):
            count = jnp.broadcast_to(cnt[0, pl.ds(h * 2 + row, 1), :], (8, LN))
            for g in range(4):
                rows = pl.ds(g * 32 + h * 2 + row, 8, stride=4)
                dst = (row, h, pl.ds(g * 8, 8))
                for c in range(3):
                    st[(c,) + dst] = off[c, rows, :] * 4.0
                    st[(3 + c,) + dst] = vel[c, rows, :] * 16.0
                slot = lax.broadcasted_iota(jnp.int32, (8, LN), 0) + g * 8
                st[(6,) + dst] = jnp.where(slot < count, mass[rows, :] * (KERNEL_NORM / 64.0), 0.0)
                e = ent[rows, :]
                sq[(0,) + dst] = e
                sq[(1,) + dst] = jnp.sqrt(e * (5.0 / 3.0))
                pr[(2,) + dst] = jnp.full((8, LN), 4.0, jnp.float32)
    pl.semaphore_wait(barrier, 9)

    lane = lane_iota()

    def start_round(rnd, src, ncomp, n, inbox):
        for side in range(2):
            for g in range(n // 8):
                packed = jnp.zeros((8, LN), jnp.float32)
                for c in range(ncomp):
                    for row in range(2):
                        code = c * 2 + row
                        v = src[c, row, side, pl.ds(g * 8, 8), :]
                        from_lane = 127 if side == 1 else 0
                        v = pltpu.roll(v, (code - from_lane) % LN, 1)
                        packed = jnp.where(lane == code, v, packed)
                ysend[rnd, side, pl.ds(g * 8, 8), :] = packed
        copies = []
        for row, dst_t, slot in ((0, down, 1), (1, up, 0)):
            f = row
            copies.append(
                pltpu.make_async_remote_copy(
                    src_ref=src.at[pl.ds(0, ncomp), row, :, pl.ds(0, n)],
                    dst_ref=inbox.at[rnd // 2, slot, pl.ds(0, ncomp), :, pl.ds(0, n)],
                    send_sem=send_sem.at[rnd % 2, f],
                    recv_sem=recv_sem.at[rnd % 2, f],
                    device_id=(dst_t, u),
                    device_id_type=MESH,
                )
            )
        for dt in range(3):
            for side in range(2):
                f = 2 + dt * 2 + side
                copies.append(
                    pltpu.make_async_remote_copy(
                        src_ref=ysend.at[rnd, side, pl.ds(0, n)],
                        dst_ref=yin.at[rnd, 2 - dt, 1 - side, pl.ds(0, n)],
                        send_sem=send_sem.at[rnd % 2, f],
                        recv_sem=recv_sem.at[rnd % 2, f],
                        device_id=(tile_of[dt], right if side == 1 else left),
                        device_id_type=MESH,
                    )
                )
        for f in (4, 5, 0, 1, 2, 3, 6, 7):
            copies[f].start()
        return copies

    def shift_of(comp, r):
        return 4.0 * (r - 1) if comp == X else 0.0

    def centre(load, comps, r, n):
        for c, comp in enumerate(comps):
            for h in range(2):
                v = load(c, h, pl.ds(0, n))
                if comp == X and r != 1:
                    v = v + 4.0 * (r - 1)
                fld[field(r, comp, 1, h), pl.ds(0, n), :] = v

    def sides(load, comps, r, n, rnd, dt, sender_row):
        for c, comp in enumerate(comps):
            code = c * 2 + sender_row
            dx = 4.0 * (r - 1) if comp == X else 0.0
            for g in range(n // 8):
                rows = pl.ds(g * 8, 8)
                a0, a1 = load(c, 0, rows), load(c, 1, rows)
                lo = pltpu.roll(yin[rnd, dt, 0, rows, :], (0 - code) % LN, 1)
                hi = pltpu.roll(yin[rnd, dt, 1, rows, :], (127 - code) % LN, 1)
                r0, r1 = pltpu.roll(a0, 1, 1), pltpu.roll(a1, 1, 1)
                l0, l1 = pltpu.roll(a0, 127, 1), pltpu.roll(a1, 127, 1)
                first, last = lane == 0, lane == 127
                minus = [jnp.where(first, lo, r0), jnp.where(first, r0, r1)]
                plus = [jnp.where(last, l1, l0), jnp.where(last, hi, l1)]
                for h in range(2):
                    m, p = minus[h], plus[h]
                    if comp == Y:
                        m, p = m - 4.0, p + 4.0
                    elif comp == X and r != 1:
                        m, p = m + dx, p + dx
                    fld[field(r, comp, 0, h), rows, :] = m
                    fld[field(r, comp, 2, h), rows, :] = p

    def other(r, comp, b, h, j):
        return fld[field(r, comp, b, h), pl.ds(j, 8, stride=0), :]

    def own(row, comp, h, g, n):
        return fld[field(row + 1, comp, 1, h), pl.ds(g * 8, n * 8), :].reshape(n, 8, LN)

    def density_stage(stage, k, first=0, last=2):
        per = NACT[k] // 8
        halves = 2 if per == 1 else 1
        base = STAGE_BASE[stage]

        def pairs(c, h):
            row, r, b = stage_ids(stage, c)
            xi, yi, zi = (own(row, comp, h, 0, per) for comp in (X, Y, Z))
            slot = (base + c) * 2 + h
            total = dens[row, h, pl.ds(0, per * 8), :].reshape(per, 8, LN)
            for j in range(S):
                dx = xi - other(r, X, b, h, j)
                dy = yi - other(r, Y, b, h, j)
                dz = zi - other(r, Z, b, h, j)
                r2 = dx * dx + dy * dy + dz * dz
                rad = r2 * lax.rsqrt(jnp.maximum(r2, 1e-30))
                s = jnp.maximum(4.0 - rad, 0.0)
                w3 = (s * other(r, MS, b, h, j)) * (s * s)
                total = total + w3 * (s * (5.0 - s))
                cache_w[slot * S + j, pl.ds(0, per)] = w3
                cache_a[slot * S + j, pl.ds(0, per)] = 1.0 / (r2 + 0.16)
            dens[row, h, pl.ds(0, per * 8), :] = total.reshape(per * 8, LN)

        def combo(i, _):
            if halves == 2:
                pairs(i, 0)
                pairs(i, 1)
            else:
                pairs(i // 2, i % 2)
            return 0

        per_row = STAGE_SIZE[stage] // halves
        lax.fori_loop(first * per_row, last * per_row, combo, 0)

    def force_stage(stage, k, first=0, last=2):
        groups = NACT[k] // 8
        per = min(groups, 2)
        sets = groups // per
        halves = 2 if per == 1 else 1
        base = STAGE_BASE[stage]

        def pairs(c, h, g):
            row, r, b = stage_ids(stage, c)
            xi, yi, zi, vxi, vyi, vzi, qi, ci, ri = (
                own(row, comp, h, g, per) for comp in (X, Y, Z, VX, VY, VZ, Q, C, R)
            )
            slot = (base + c) * 2 + h
            ax, ay, az = (acc[d, row, h, pl.ds(g * 8, per * 8), :].reshape(per, 8, LN) for d in range(3))
            for j in range(S):
                dx = xi - other(r, X, b, h, j)
                dy = yi - other(r, Y, b, h, j)
                dz = zi - other(r, Z, b, h, j)
                n = (
                    dx * (vxi - other(r, VX, b, h, j))
                    + dy * (vyi - other(r, VY, b, h, j))
                    + dz * (vzi - other(r, VZ, b, h, j))
                )
                mu = jnp.minimum(n, 0.0) * cache_a[slot * S + j, pl.ds(g, per)]
                sound = ci + other(r, C, b, h, j)
                visc = (mu * (mu - sound)) / (ri + other(r, R, b, h, j))
                f = cache_w[slot * S + j, pl.ds(g, per)] * (qi + other(r, Q, b, h, j) + visc)
                ax, ay, az = ax + f * dx, ay + f * dy, az + f * dz
            for d, total in enumerate((ax, ay, az)):
                acc[d, row, h, pl.ds(g * 8, per * 8), :] = total.reshape(per * 8, LN)

        def combo(i, _):
            if halves == 2:
                pairs(i, 0, 0)
                pairs(i, 1, 0)
            else:
                ch, g = i // sets, (i % sets) * per
                pairs(ch // 2, ch % 2, g)
            return 0

        per_row = STAGE_SIZE[stage] * sets // halves
        lax.fori_loop(first * per_row, last * per_row, combo, 0)

    def plan():
        row_i = lax.broadcasted_iota(jnp.int32, (LN, LN), 0)
        col_i = lax.broadcasted_iota(jnp.int32, (LN, LN), 1)
        before = jnp.where(row_i < col_i, 1.0, 0.0).astype(jnp.bfloat16)
        ones = jnp.ones((LN, LN), jnp.bfloat16)
        row8 = lax.broadcasted_iota(jnp.int32, (8, LN), 0)
        dest = tgt[...]
        start = jnp.zeros((LN, LN), jnp.float32)
        place = jnp.zeros((LN, LN), jnp.float32)
        start_t = jnp.zeros((8, LN), jnp.float32)
        info = jnp.zeros((8, LN), jnp.float32)
        for d in range(subs):
            mine = dest == d
            hot = jnp.where(mine, 1.0, 0.0).astype(jnp.bfloat16)
            inside = jnp.dot(hot, before, preferred_element_type=jnp.float32)
            place = jnp.where(mine, start + inside, place)
            start = start + jnp.dot(hot, ones, preferred_element_type=jnp.float32)
            count_t = lax.dot_general(
                ones[0:8], hot, (((1,), (1,)), ((), ())), preferred_element_type=jnp.float32
            )
            info = jnp.where(row8 == d, start_t, info)
            info = jnp.where(row8 == subs + d, count_t, info)
            start_t = start_t + count_t
        pos[...] = place.astype(jnp.int32)
        tab[u] = info
        sends = []
        for k in range(1, subs):
            copy = pltpu.make_async_remote_copy(
                src_ref=tab.at[u],
                dst_ref=tab.at[u],
                send_sem=tab_send.at[k],
                recv_sem=tab_recv.at[k],
                device_id=(t, lax.rem(u + k, subs)),
                device_id_type=MESH,
            )
            copy.start()
            sends.append(copy)
        return sends

    def emit(g, own_rows):
        row_q = lax.broadcasted_iota(jnp.int32, (LN, LN), 0)
        for row in own_rows:
            for h in range(2):
                count = jnp.broadcast_to(cnt[0, pl.ds(h * 2 + row, 1), :], (8, LN))
                rows = pl.ds(g * 8, 8)
                slot = lax.broadcasted_iota(jnp.int32, (8, LN), 0) + g * 8
                in_rows = pl.ds(g * 32 + h * 2 + row, 8, stride=4)
                values = [st[d, row, h, rows, :] * 0.25 for d in range(3)]
                values += [st[3 + d, row, h, rows, :] * 0.0625 for d in range(3)]
                values += [pr[2, row, h, rows, :] * 0.25]
                values += [jnp.where(slot < count, mass[in_rows, :], 0.0)]
                for i, v in enumerate(values):
                    raw[g, pl.ds((row * 2 + h) * 64 + i, 8, stride=8), :] = v

        def sort(rh, _):
            row, h = rh // 2, rh % 2
            for i in range(8):
                slot = g * 8 + i
                line = pos[pl.ds(slot * 4 + h * 2 + row, 1), :]
                hot = jnp.where(row_q == jnp.broadcast_to(line, (LN, LN)), 1.0, 0.0)
                v = raw[g, pl.ds(rh * 64 + i * 8, 8), :]
                hi = v.astype(jnp.bfloat16)
                rest = v - hi.astype(jnp.float32)
                mid = rest.astype(jnp.bfloat16)
                low = (rest - mid.astype(jnp.float32)).astype(jnp.bfloat16)
                pieces = jnp.concatenate([hi, mid, low], axis=0)
                moved = lax.dot_general(
                    pieces, hot.astype(jnp.bfloat16), (((1,), (1,)), ((), ())), preferred_element_type=jnp.float32
                )
                gathered[u, slot * 2 + h, row] = (moved[0:8] + moved[8:16]) + moved[16:24]
            return 0

        lax.fori_loop(own_rows[0] * 2, own_rows[-1] * 2 + 2, sort, 0)

    PIECES = ((32, 32, (0, 1)), (16, 16, (0, 1)), (0, 16, (0,)), (0, 16, (1,)))

    def piece_copy(p, flow, owner, second_half, dst):
        first, rows, own_rows = PIECES[p]
        half = rows // 2
        part = pl.ds(first + half * second_half, half)
        which = slice(None) if len(own_rows) == 2 else own_rows[0]
        return pltpu.make_async_remote_copy(
            src_ref=gathered.at[owner, part, which],
            dst_ref=gathered.at[owner, part, which],
            send_sem=piece_send.at[p, flow],
            recv_sem=piece_recv.at[p, flow],
            device_id=(t, dst),
            device_id_type=MESH,
        )

    def start_piece(p):
        first, rows, own_rows = PIECES[p]
        for g in range(first // 16, (first + rows) // 16):
            emit(g, own_rows)
        copies = [
            piece_copy(p, 0, u, 0, right),
            piece_copy(p, 1, u, 1, right),
            piece_copy(p, 2, u, 1, left),
            piece_copy(p, 3, u, 0, left),
        ]
        for f in (0, 2, 1, 3):
            copies[f].start()
        arriving[p] = copies

    def forward_piece(p):
        arriving[p][0].wait_recv()
        arriving[p][2].wait_recv()
        copies = [piece_copy(p, 4, left, 0, right), piece_copy(p, 5, right, 1, left)]
        for copy in copies:
            copy.start()
        arriving[p] += copies

    def finish_piece(p):
        for f in (1, 3, 4, 5):
            arriving[p][f].wait_recv()
        for copy in arriving[p]:
            copy.wait_send()

    def exchange_and_sum(rnd, src, inbox, comps, n, stage_fn, k, meanwhile, row_done=None):
        copies = start_round(rnd, src, len(comps), n, inbox)
        meanwhile()
        loads = [None] * 4
        for r in (1, 2):
            loads[r] = functools.partial(lambda row, c, h, rows: src[c, row, h, rows, :], r - 1)
        loads[0] = lambda c, h, rows: inbox[rnd // 2, 0, c, h, rows, :]
        loads[3] = lambda c, h, rows: inbox[rnd // 2, 1, c, h, rows, :]
        for r in (1, 2):
            centre(loads[r], comps, r, n)
        stage_fn(0, k)
        copies[4].wait_recv()
        copies[5].wait_recv()
        for r in (1, 2):
            sides(loads[r], comps, r, n, rnd, 1, r - 1)
        stage_fn(1, k, 0, 2 if row_done is None else 1)
        for f in (0, 1, 2, 3, 6, 7):
            copies[f].wait_recv()
        for r, dt, sender_row in ((0, 0, 1), (3, 2, 0)):
            centre(loads[r], comps, r, n)
            sides(loads[r], comps, r, n, rnd, dt, sender_row)
        if row_done is None:
            stage_fn(2, k)
            return copies
        for copy in copies:
            copy.wait_send()
        stage_fn(2, k, 0, 1)
        row_done(0)
        stage_fn(1, k, 1, 2)
        row_done(1)
        stage_fn(2, k, 1, 2)
        row_done(2)
        return []

    arriving = {}

    def lay_plan():
        for copy in arriving["tab"]:
            copy.wait_recv()
        row_i = lax.broadcasted_iota(jnp.int32, (LN, LN), 0)
        col_i = lax.broadcasted_iota(jnp.int32, (LN, LN), 1)

        def order(i):
            return (i // 4) * 4 + (i % 2) * 2 + (i // 2) % 2

        earlier = jnp.where(order(row_i) < order(col_i), 1.0, 0.0).astype(jnp.bfloat16)
        starts = jnp.concatenate([tab[src, pl.ds(u, 1), :] for src in range(subs)], axis=0)
        counts = jnp.concatenate([tab[src, pl.ds(subs + u, 1), :] for src in range(subs)], axis=0)
        padded = jnp.concatenate([counts, jnp.zeros_like(counts)], axis=0).astype(jnp.bfloat16)
        base = jnp.dot(padded, earlier, preferred_element_type=jnp.float32)[0:subs]
        base = base.astype(jnp.int32)
        skip = base & (LN - 1)
        runs[0:subs, :] = (skip - starts.astype(jnp.int32)) & (LN - 1)
        runs[subs : 2 * subs, :] = skip
        runs[2 * subs : 3 * subs, :] = skip + counts.astype(jnp.int32)
        runs[3 * subs : 4 * subs, :] = base >> 7

    def during(rnd):
        if rnd == 0:
            arriving["tab"] = plan()
        elif rnd == 1:
            lay_plan()
        elif rnd in (2, 4):
            start_piece(rnd // 2 - 1)
        elif rnd in (3, 5):
            forward_piece(rnd // 2 - 1)

    def move(k, row):
        for h in range(2):
            count = jnp.broadcast_to(cnt[k, pl.ds(h * 2 + row, 1), :], (8, LN))
            for g in range(NACT[k] // 8):
                rows = pl.ds(g * 8, 8)
                slot = lax.broadcasted_iota(jnp.int32, (8, LN), 0) + g * 8
                active = slot < count
                for d in range(3):
                    v = st[3 + d, row, h, rows, :]
                    x = st[d, row, h, rows, :]
                    v_new = v + 4.0 * acc[d, row, h, rows, :]
                    st[3 + d, row, h, rows, :] = jnp.where(active, v_new, v)
                    st[d, row, h, rows, :] = jnp.where(active, x + 0.0125 * v_new, x)

    def last_rows(step):
        if step == 0:
            move(2, 0)
            start_piece(2)
        elif step == 1:
            forward_piece(2)
        else:
            move(2, 1)
            start_piece(3)
            forward_piece(3)

    for k in range(3):
        n = NACT[k]
        dens[...] = jnp.zeros_like(dens)
        comps = (X, Y, Z, VX, VY, VZ) + ((MS,) if k == 0 else ())
        moved = exchange_and_sum(2 * k, st, xin, comps, NMOVED[k], density_stage, k, lambda: during(2 * k))
        for row in range(2):
            for h in range(2):
                count = jnp.broadcast_to(cnt[k, pl.ds(h * 2 + row, 1), :], (8, LN))
                for g in range(n // 8):
                    rows = pl.ds(g * 8, 8)
                    slot = lax.broadcasted_iota(jnp.int32, (8, LN), 0) + g * 8
                    rho4 = jnp.where(slot < count, dens[row, h, rows, :], pr[2, row, h, rows, :])
                    root = jnp.exp(jnp.log(rho4 * 0.25) * (1.0 / 3.0))
                    pr[0, row, h, rows, :] = sq[0, row, h, rows, :] / root
                    pr[1, row, h, rows, :] = sq[1, row, h, rows, :] * root
                    pr[2, row, h, rows, :] = rho4
        acc[...] = jnp.zeros_like(acc)
        if k == 2:
            for copy in moved:
                copy.wait_send()
        pressed = exchange_and_sum(
            2 * k + 1, pr, pin, (Q, C, R), n, force_stage, k, lambda: during(2 * k + 1), last_rows if k == 2 else None
        )
        if k < 2:
            for copy in moved + pressed:
                copy.wait_send()
            for row in range(2):
                move(k, row)
    for copy in arriving["tab"]:
        copy.wait_send()
    for p in range(4):
        finish_piece(p)


TILES = 48


def lay_kernel(runs, gathered, out, tiles):
    subs = gathered.shape[0]
    lane = lane_iota()
    beyond = lane + LN
    tiles[...] = jnp.zeros_like(tiles)

    def lay(slot, currents):
        for row in range(2):
            for h in range(2):
                at = slot * 4 + h * 2 + row
                later = []
                for src in range(subs):
                    end = jnp.full((8, LN), runs[2 * subs + src, at])
                    turned = pltpu.roll(gathered[src, slot * 2 + h, row], runs[src, at], 1)
                    kept = jnp.where(lane < end, turned, 0.0)
                    merged = jnp.where(lane < runs[subs + src, at], currents[src], kept)
                    tiles[src, runs[3 * subs + src, at]] = merged
                    wrapped = jnp.where(beyond < end, turned, 0.0)
                    later.append(jnp.where(end >= LN, wrapped, merged))
                currents = later
        return tuple(currents)

    zero = jnp.zeros((8, LN), jnp.float32)
    currents = lax.fori_loop(0, S, lay, (zero,) * subs)
    for src in range(subs):
        last = runs[2 * subs + src, LN - 1]
        tiles[src, runs[3 * subs + src, LN - 1] + jnp.where(last >= LN, 1, 0)] = currents[src]
    for src in range(subs):
        out[pl.ds(src * TILES, TILES)] = tiles[src, pl.ds(0, TILES)]


def rows_of(a):
    lead = a.shape[:-2]
    a = a.reshape(lead + (2, 2, LN))
    a = jnp.swapaxes(a, -3, -2)
    return a


def shards(tiles, subs, offsets, velocity, mass, entropy, active_counts, targets):
    off = rows_of(offsets).reshape(3, LN, LN)
    vel = rows_of(velocity).reshape(3, LN, LN)
    mas = rows_of(mass).reshape(LN, LN)
    ent = rows_of(entropy).reshape(LN, LN)
    cnt = rows_of(active_counts).reshape(3, 4, LN)
    tgt = rows_of(targets).reshape(LN, LN)
    vmem = pl.BlockSpec(memory_space=pltpu.VMEM)
    f32 = jnp.float32
    gathered, runs = pl.pallas_call(
        functools.partial(substeps_kernel, tiles, subs),
        out_shape=[
            jax.ShapeDtypeStruct((subs, LN // 2, 2, 8, LN), f32),
            jax.ShapeDtypeStruct((4 * subs, LN), jnp.int32),
        ],
        in_specs=[vmem] * 6,
        out_specs=[vmem] * 2,
        scratch_shapes=[
            pltpu.VMEM((4 * NF * 6, S, LN), f32),
            pltpu.VMEM((7, 2, 2, S, LN), f32),
            pltpu.VMEM((3, 2, 2, S, LN), f32),
            pltpu.VMEM((2, 2, S, LN), f32),
            pltpu.VMEM((3, 2, 2, S, LN), f32),
            pltpu.VMEM((2, 2, 2, S, LN), f32),
            pltpu.VMEM((6, 2, S, LN), f32),
            pltpu.VMEM((3, 2, 7, 2, S, LN), f32),
            pltpu.VMEM((3, 2, 3, 2, S, LN), f32),
            pltpu.VMEM((6, 3, 2, S, LN), f32),
            pltpu.VMEM((18 * 2 * S, 4, 8, LN), f32),
            pltpu.VMEM((18 * 2 * S, 4, 8, LN), f32),
            pltpu.VMEM((4, 256, LN), f32),
            pltpu.VMEM((LN, LN), jnp.int32),
            pltpu.VMEM((subs, 2 * subs, LN), f32),
            pltpu.SemaphoreType.DMA((2, 8)),
            pltpu.SemaphoreType.DMA((2, 8)),
            pltpu.SemaphoreType.DMA((4,)),
            pltpu.SemaphoreType.DMA((4,)),
            pltpu.SemaphoreType.DMA((4, 6)),
            pltpu.SemaphoreType.DMA((4, 6)),
        ],
        compiler_params=pltpu.CompilerParams(collective_id=0, has_side_effects=True, vmem_limit_bytes=62 * 1024 * 1024),
        name="substeps",
    )(off, vel, mas, ent, cnt, tgt)
    arrived = pl.pallas_call(
        lay_kernel,
        out_shape=jax.ShapeDtypeStruct((subs * TILES, 8, LN), f32),
        in_specs=[pl.BlockSpec(memory_space=pltpu.SMEM), vmem],
        out_specs=vmem,
        scratch_shapes=[pltpu.VMEM((subs, TILES + 2, 8, LN), f32)],
        name="lay",
    )(runs, gathered)
    return jnp.transpose(arrived, (1, 0, 2)).reshape(8, subs * TILES * LN)


def solution(mesh):
    tiles, subs = mesh.shape["tile"], mesh.shape["sub"]
    placed = (
        P(None, None, "tile", "sub"),
        P(None, None, "tile", "sub"),
        P(None, "tile", "sub"),
        P(None, "tile", "sub"),
        P(None, "tile", "sub"),
        P(None, "tile", "sub"),
    )
    return jax.shard_map(
        functools.partial(shards, tiles, subs),
        mesh=mesh,
        in_specs=placed,
        out_specs=P(None, ("tile", "sub")),
        check_vma=False,
    )
```

```python
import functools
import math

import jax
import jax.numpy as jnp
from jax import lax
from jax.experimental import pallas as pl
from jax.experimental.pallas import tpu as pltpu
from jax.sharding import PartitionSpec as P

MESH = pl.DeviceIdType.MESH

S = 32
LN = 128
KERNEL_NORM = 21.0 / (2.0 * math.pi)
NACT = (32, 16, 8)
NMOVED = (32, 32, 16)

X, Y, Z, VX, VY, VZ, MS, Q, C, R = range(10)
NF = 10


def field(row, comp, b, h):
    return ((row * NF + comp) * 3 + b) * 2 + h


def lane_iota():
    return lax.broadcasted_iota(jnp.int32, (8, LN), 1)


def stage_ids(stage, c):
    if stage == 0:
        return c // 2, 1 + c % 2, 1
    if stage == 1:
        return c // 4, 1 + (c // 2) % 2, 2 * (c % 2)
    return c // 3, 3 * (c // 3), c % 3


STAGE_SIZE = (4, 8, 6)
STAGE_BASE = (0, 4, 12)


def substeps_kernel(
    tiles, subs, off, vel, mass, ent, cnt, tgt, done, runs, gathered, fld, st, pr, dens, acc, sq, ysend, xin, pin, yin,
    cache_w, cache_a, raw, pos, tab, send_sem, recv_sem, tab_send, tab_recv, piece_send, piece_recv, done_sem
):
    t, u = lax.axis_index("tile"), lax.axis_index("sub")
    up, down = lax.rem(t + 1, tiles), lax.rem(t + tiles - 1, tiles)
    right, left = lax.rem(u + 1, subs), lax.rem(u + subs - 1, subs)
    tile_of = (down, t, up)

    barrier = pltpu.get_barrier_semaphore()
    across = lax.rem(u + 2, subs)
    near = ((down, u), (up, u), (down, left), (t, left), (up, left), (down, right), (t, right), (up, right))
    for dev in near + ((t, across),):
        pl.semaphore_signal(barrier, inc=1, device_id=dev, device_id_type=MESH)

    for row in range(2):
        for h in range(2):
            count = jnp.broadcast_to(cnt[0, pl.ds(h * 2 + row, 1), :], (8, LN))
            for g in range(4):
                rows = pl.ds(g * 32 + h * 2 + row, 8, stride=4)
                dst = (row, h, pl.ds(g * 8, 8))
                for c in range(3):
                    st[(c,) + dst] = off[c, rows, :] * 4.0
                    st[(3 + c,) + dst] = vel[c, rows, :] * 16.0
                slot = lax.broadcasted_iota(jnp.int32, (8, LN), 0) + g * 8
                st[(6,) + dst] = jnp.where(slot < count, mass[rows, :] * (KERNEL_NORM / 64.0), 0.0)
                e = ent[rows, :]
                sq[(0,) + dst] = e
                sq[(1,) + dst] = jnp.sqrt(e * (5.0 / 3.0))
                pr[(2,) + dst] = jnp.full((8, LN), 4.0, jnp.float32)
    pl.semaphore_wait(barrier, 9)

    lane = lane_iota()

    def start_round(rnd, src, ncomp, n, inbox):
        for side in range(2):
            for g in range(n // 8):
                packed = jnp.zeros((8, LN), jnp.float32)
                for c in range(ncomp):
                    for row in range(2):
                        code = c * 2 + row
                        v = src[c, row, side, pl.ds(g * 8, 8), :]
                        from_lane = 127 if side == 1 else 0
                        v = pltpu.roll(v, (code - from_lane) % LN, 1)
                        packed = jnp.where(lane == code, v, packed)
                ysend[rnd, side, pl.ds(g * 8, 8), :] = packed
        copies = []
        for row, dst_t, slot in ((0, down, 1), (1, up, 0)):
            f = row
            copies.append(
                pltpu.make_async_remote_copy(
                    src_ref=src.at[pl.ds(0, ncomp), row, :, pl.ds(0, n)],
                    dst_ref=inbox.at[rnd // 2, slot, pl.ds(0, ncomp), :, pl.ds(0, n)],
                    send_sem=send_sem.at[rnd % 2, f],
                    recv_sem=recv_sem.at[rnd % 2, f],
                    device_id=(dst_t, u),
                    device_id_type=MESH,
                )
            )
        for dt in range(3):
            for side in range(2):
                f = 2 + dt * 2 + side
                copies.append(
                    pltpu.make_async_remote_copy(
                        src_ref=ysend.at[rnd, side, pl.ds(0, n)],
                        dst_ref=yin.at[rnd, 2 - dt, 1 - side, pl.ds(0, n)],
                        send_sem=send_sem.at[rnd % 2, f],
                        recv_sem=recv_sem.at[rnd % 2, f],
                        device_id=(tile_of[dt], right if side == 1 else left),
                        device_id_type=MESH,
                    )
                )
        for f in (4, 5, 0, 1, 2, 3, 6, 7):
            copies[f].start()
        return copies

    def shift_of(comp, r):
        return 4.0 * (r - 1) if comp == X else 0.0

    def centre(load, comps, r, n):
        for c, comp in enumerate(comps):
            for h in range(2):
                v = load(c, h, pl.ds(0, n))
                if comp == X and r != 1:
                    v = v + 4.0 * (r - 1)
                fld[field(r, comp, 1, h), pl.ds(0, n), :] = v

    def sides(load, comps, r, n, rnd, dt, sender_row):
        for c, comp in enumerate(comps):
            code = c * 2 + sender_row
            dx = 4.0 * (r - 1) if comp == X else 0.0
            for g in range(n // 8):
                rows = pl.ds(g * 8, 8)
                a0, a1 = load(c, 0, rows), load(c, 1, rows)
                lo = pltpu.roll(yin[rnd, dt, 0, rows, :], (0 - code) % LN, 1)
                hi = pltpu.roll(yin[rnd, dt, 1, rows, :], (127 - code) % LN, 1)
                r0, r1 = pltpu.roll(a0, 1, 1), pltpu.roll(a1, 1, 1)
                l0, l1 = pltpu.roll(a0, 127, 1), pltpu.roll(a1, 127, 1)
                first, last = lane == 0, lane == 127
                minus = [jnp.where(first, lo, r0), jnp.where(first, r0, r1)]
                plus = [jnp.where(last, l1, l0), jnp.where(last, hi, l1)]
                for h in range(2):
                    m, p = minus[h], plus[h]
                    if comp == Y:
                        m, p = m - 4.0, p + 4.0
                    elif comp == X and r != 1:
                        m, p = m + dx, p + dx
                    fld[field(r, comp, 0, h), rows, :] = m
                    fld[field(r, comp, 2, h), rows, :] = p

    def other(r, comp, b, h, j):
        return fld[field(r, comp, b, h), pl.ds(j, 8, stride=0), :]

    def own(row, comp, h, g, n):
        return fld[field(row + 1, comp, 1, h), pl.ds(g * 8, n * 8), :].reshape(n, 8, LN)

    def density_stage(stage, k, first=0, last=2):
        per = NACT[k] // 8
        halves = 2 if per == 1 else 1
        base = STAGE_BASE[stage]

        def pairs(c, h):
            row, r, b = stage_ids(stage, c)
            xi, yi, zi = (own(row, comp, h, 0, per) for comp in (X, Y, Z))
            slot = (base + c) * 2 + h
            total = dens[row, h, pl.ds(0, per * 8), :].reshape(per, 8, LN)
            for j in range(S):
                dx = xi - other(r, X, b, h, j)
                dy = yi - other(r, Y, b, h, j)
                dz = zi - other(r, Z, b, h, j)
                r2 = dx * dx + dy * dy + dz * dz
                rad = r2 * lax.rsqrt(jnp.maximum(r2, 1e-30))
                s = jnp.maximum(4.0 - rad, 0.0)
                w3 = (s * other(r, MS, b, h, j)) * (s * s)
                total = total + w3 * (s * (5.0 - s))
                cache_w[slot * S + j, pl.ds(0, per)] = w3
                cache_a[slot * S + j, pl.ds(0, per)] = 1.0 / (r2 + 0.16)
            dens[row, h, pl.ds(0, per * 8), :] = total.reshape(per * 8, LN)

        def combo(i, _):
            if halves == 2:
                pairs(i, 0)
                pairs(i, 1)
            else:
                pairs(i // 2, i % 2)
            return 0

        per_row = STAGE_SIZE[stage] // halves
        lax.fori_loop(first * per_row, last * per_row, combo, 0)

    def force_stage(stage, k, first=0, last=2):
        groups = NACT[k] // 8
        per = min(groups, 2)
        sets = groups // per
        halves = 2 if per == 1 else 1
        base = STAGE_BASE[stage]

        def pairs(c, h, g):
            row, r, b = stage_ids(stage, c)
            xi, yi, zi, vxi, vyi, vzi, qi, ci, ri = (
                own(row, comp, h, g, per) for comp in (X, Y, Z, VX, VY, VZ, Q, C, R)
            )
            slot = (base + c) * 2 + h
            ax, ay, az = (acc[d, row, h, pl.ds(g * 8, per * 8), :].reshape(per, 8, LN) for d in range(3))
            for j in range(S):
                dx = xi - other(r, X, b, h, j)
                dy = yi - other(r, Y, b, h, j)
                dz = zi - other(r, Z, b, h, j)
                n = (
                    dx * (vxi - other(r, VX, b, h, j))
                    + dy * (vyi - other(r, VY, b, h, j))
                    + dz * (vzi - other(r, VZ, b, h, j))
                )
                mu = jnp.minimum(n, 0.0) * cache_a[slot * S + j, pl.ds(g, per)]
                sound = ci + other(r, C, b, h, j)
                visc = (mu * (mu - sound)) / (ri + other(r, R, b, h, j))
                f = cache_w[slot * S + j, pl.ds(g, per)] * (qi + other(r, Q, b, h, j) + visc)
                ax, ay, az = ax + f * dx, ay + f * dy, az + f * dz
            for d, total in enumerate((ax, ay, az)):
                acc[d, row, h, pl.ds(g * 8, per * 8), :] = total.reshape(per * 8, LN)

        def combo(i, _):
            if halves == 2:
                pairs(i, 0, 0)
                pairs(i, 1, 0)
            else:
                ch, g = i // sets, (i % sets) * per
                pairs(ch // 2, ch % 2, g)
            return 0

        per_row = STAGE_SIZE[stage] * sets // halves
        lax.fori_loop(first * per_row, last * per_row, combo, 0)

    def plan():
        row_i = lax.broadcasted_iota(jnp.int32, (LN, LN), 0)
        col_i = lax.broadcasted_iota(jnp.int32, (LN, LN), 1)
        before = jnp.where(row_i < col_i, 1.0, 0.0).astype(jnp.bfloat16)
        ones = jnp.ones((LN, LN), jnp.bfloat16)
        row8 = lax.broadcasted_iota(jnp.int32, (8, LN), 0)
        dest = tgt[...]
        start = jnp.zeros((LN, LN), jnp.float32)
        place = jnp.zeros((LN, LN), jnp.float32)
        start_t = jnp.zeros((8, LN), jnp.float32)
        info = jnp.zeros((8, LN), jnp.float32)
        for d in range(subs):
            mine = dest == d
            hot = jnp.where(mine, 1.0, 0.0).astype(jnp.bfloat16)
            inside = jnp.dot(hot, before, preferred_element_type=jnp.float32)
            place = jnp.where(mine, start + inside, place)
            start = start + jnp.dot(hot, ones, preferred_element_type=jnp.float32)
            count_t = lax.dot_general(
                ones[0:8], hot, (((1,), (1,)), ((), ())), preferred_element_type=jnp.float32
            )
            info = jnp.where(row8 == d, start_t, info)
            info = jnp.where(row8 == subs + d, count_t, info)
            start_t = start_t + count_t
        pos[...] = place.astype(jnp.int32)
        tab[u] = info
        sends = []
        for k in range(1, subs):
            copy = pltpu.make_async_remote_copy(
                src_ref=tab.at[u],
                dst_ref=tab.at[u],
                send_sem=tab_send.at[k],
                recv_sem=tab_recv.at[k],
                device_id=(t, lax.rem(u + k, subs)),
                device_id_type=MESH,
            )
            copy.start()
            sends.append(copy)
        return sends

    def emit(g, own_rows):
        row_q = lax.broadcasted_iota(jnp.int32, (LN, LN), 0)
        for row in own_rows:
            for h in range(2):
                count = jnp.broadcast_to(cnt[0, pl.ds(h * 2 + row, 1), :], (8, LN))
                rows = pl.ds(g * 8, 8)
                slot = lax.broadcasted_iota(jnp.int32, (8, LN), 0) + g * 8
                in_rows = pl.ds(g * 32 + h * 2 + row, 8, stride=4)
                values = [st[d, row, h, rows, :] * 0.25 for d in range(3)]
                values += [st[3 + d, row, h, rows, :] * 0.0625 for d in range(3)]
                values += [pr[2, row, h, rows, :] * 0.25]
                values += [jnp.where(slot < count, mass[in_rows, :], 0.0)]
                for i, v in enumerate(values):
                    raw[g, pl.ds((row * 2 + h) * 64 + i, 8, stride=8), :] = v

        def sort(rh, _):
            row, h = rh // 2, rh % 2
            for i in range(8):
                slot = g * 8 + i
                line = pos[pl.ds(slot * 4 + h * 2 + row, 1), :]
                hot = jnp.where(row_q == jnp.broadcast_to(line, (LN, LN)), 1.0, 0.0)
                v = raw[g, pl.ds(rh * 64 + i * 8, 8), :]
                hi = v.astype(jnp.bfloat16)
                rest = v - hi.astype(jnp.float32)
                mid = rest.astype(jnp.bfloat16)
                low = (rest - mid.astype(jnp.float32)).astype(jnp.bfloat16)
                pieces = jnp.concatenate([hi, mid, low], axis=0)
                moved = lax.dot_general(
                    pieces, hot.astype(jnp.bfloat16), (((1,), (1,)), ((), ())), preferred_element_type=jnp.float32
                )
                gathered[u, slot * 2 + h, row] = (moved[0:8] + moved[8:16]) + moved[16:24]
            return 0

        lax.fori_loop(own_rows[0] * 2, own_rows[-1] * 2 + 2, sort, 0)

    PIECES = ((32, 32, (0, 1)), (16, 16, (0, 1)), (0, 16, (0,)), (0, 16, (1,)))

    def piece_copy(p, flow, owner, second_half, dst):
        first, rows, own_rows = PIECES[p]
        half = rows // 2
        part = pl.ds(first + half * second_half, half)
        which = slice(None) if len(own_rows) == 2 else own_rows[0]
        return pltpu.make_async_remote_copy(
            src_ref=gathered.at[owner, part, which],
            dst_ref=gathered.at[owner, part, which],
            send_sem=piece_send.at[p, flow],
            recv_sem=piece_recv.at[p, flow],
            device_id=(t, dst),
            device_id_type=MESH,
        )

    def start_piece(p, before_rest=None):
        first, rows, own_rows = PIECES[p]
        for g in range(first // 16, (first + rows) // 16):
            emit(g, own_rows)
        copies = [
            piece_copy(p, 0, u, 0, right),
            piece_copy(p, 1, u, 1, right),
            piece_copy(p, 2, u, 1, left),
            piece_copy(p, 3, u, 0, left),
        ]
        arriving[p] = copies
        copies[0].start()
        copies[2].start()
        if before_rest is not None:
            before_rest()
        copies[1].start()
        copies[3].start()

    def forward_piece(p):
        arriving[p][0].wait_recv()
        arriving[p][2].wait_recv()
        copies = [piece_copy(p, 4, left, 0, right), piece_copy(p, 5, right, 1, left)]
        for copy in copies:
            copy.start()
        arriving[p] += copies

    leaving = []

    def finish_piece(p):
        for f in (1, 3, 4, 5):
            arriving[p][f].wait_recv()
        for copy in arriving[p]:
            copy.wait_send()
        first, rows, own_rows = PIECES[p]
        which = slice(None) if len(own_rows) == 2 else own_rows[0]
        copy = pltpu.make_async_copy(
            gathered.at[:, pl.ds(first, rows), which], done.at[:, pl.ds(first, rows), which], done_sem.at[p]
        )
        copy.start()
        leaving.append(copy)

    def exchange_and_sum(rnd, src, inbox, comps, n, stage_fn, k, meanwhile, row_done=None):
        copies = start_round(rnd, src, len(comps), n, inbox)
        meanwhile()
        loads = [None] * 4
        for r in (1, 2):
            loads[r] = functools.partial(lambda row, c, h, rows: src[c, row, h, rows, :], r - 1)
        loads[0] = lambda c, h, rows: inbox[rnd // 2, 0, c, h, rows, :]
        loads[3] = lambda c, h, rows: inbox[rnd // 2, 1, c, h, rows, :]
        for r in (1, 2):
            centre(loads[r], comps, r, n)
        stage_fn(0, k)
        copies[4].wait_recv()
        copies[5].wait_recv()
        for r in (1, 2):
            sides(loads[r], comps, r, n, rnd, 1, r - 1)
        stage_fn(1, k, 0, 2 if row_done is None else 1)
        for f in (0, 1, 2, 3, 6, 7):
            copies[f].wait_recv()
        for r, dt, sender_row in ((0, 0, 1), (3, 2, 0)):
            centre(loads[r], comps, r, n)
            sides(loads[r], comps, r, n, rnd, dt, sender_row)
        if row_done is None:
            stage_fn(2, k)
            return copies
        for copy in copies:
            copy.wait_send()
        stage_fn(2, k, 0, 1)
        row_done(0)
        stage_fn(1, k, 1, 2)
        row_done(1)
        stage_fn(2, k, 1, 2)
        row_done(2)
        return []

    arriving = {}

    def lay_plan():
        for copy in arriving["tab"]:
            copy.wait_recv()
        row_i = lax.broadcasted_iota(jnp.int32, (LN, LN), 0)
        col_i = lax.broadcasted_iota(jnp.int32, (LN, LN), 1)

        def order(i):
            return (i // 4) * 4 + (i % 2) * 2 + (i // 2) % 2

        earlier = jnp.where(order(row_i) < order(col_i), 1.0, 0.0).astype(jnp.bfloat16)
        starts = jnp.concatenate([tab[src, pl.ds(u, 1), :] for src in range(subs)], axis=0)
        counts = jnp.concatenate([tab[src, pl.ds(subs + u, 1), :] for src in range(subs)], axis=0)
        padded = jnp.concatenate([counts, jnp.zeros_like(counts)], axis=0).astype(jnp.bfloat16)
        base = jnp.dot(padded, earlier, preferred_element_type=jnp.float32)[0:subs]
        base = base.astype(jnp.int32)
        skip = base & (LN - 1)
        runs[0:subs, :] = (skip - starts.astype(jnp.int32)) & (LN - 1)
        runs[subs : 2 * subs, :] = skip
        runs[2 * subs : 3 * subs, :] = skip + counts.astype(jnp.int32)
        runs[3 * subs : 4 * subs, :] = base >> 7

    def during(rnd):
        if rnd == 0:
            arriving["tab"] = plan()
        elif rnd == 1:
            lay_plan()
        elif rnd in (2, 4):
            if rnd == 4:
                finish_piece(0)
            start_piece(rnd // 2 - 1)
        elif rnd in (3, 5):
            forward_piece(rnd // 2 - 1)

    def move(k, row):
        for h in range(2):
            count = jnp.broadcast_to(cnt[k, pl.ds(h * 2 + row, 1), :], (8, LN))
            for g in range(NACT[k] // 8):
                rows = pl.ds(g * 8, 8)
                slot = lax.broadcasted_iota(jnp.int32, (8, LN), 0) + g * 8
                active = slot < count
                for d in range(3):
                    v = st[3 + d, row, h, rows, :]
                    x = st[d, row, h, rows, :]
                    v_new = v + 4.0 * acc[d, row, h, rows, :]
                    st[3 + d, row, h, rows, :] = jnp.where(active, v_new, v)
                    st[d, row, h, rows, :] = jnp.where(active, x + 0.0125 * v_new, x)

    def last_rows(step):
        if step == 0:
            move(2, 0)
            start_piece(2)
        elif step == 2:
            finish_piece(1)
            move(2, 1)
            start_piece(3, lambda: forward_piece(2))
            forward_piece(3)

    for k in range(3):
        n = NACT[k]
        dens[...] = jnp.zeros_like(dens)
        comps = (X, Y, Z, VX, VY, VZ) + ((MS,) if k == 0 else ())
        moved = exchange_and_sum(2 * k, st, xin, comps, NMOVED[k], density_stage, k, lambda: during(2 * k))
        for row in range(2):
            for h in range(2):
                count = jnp.broadcast_to(cnt[k, pl.ds(h * 2 + row, 1), :], (8, LN))
                for g in range(n // 8):
                    rows = pl.ds(g * 8, 8)
                    slot = lax.broadcasted_iota(jnp.int32, (8, LN), 0) + g * 8
                    rho4 = jnp.where(slot < count, dens[row, h, rows, :], pr[2, row, h, rows, :])
                    root = jnp.exp(jnp.log(rho4 * 0.25) * (1.0 / 3.0))
                    pr[0, row, h, rows, :] = sq[0, row, h, rows, :] / root
                    pr[1, row, h, rows, :] = sq[1, row, h, rows, :] * root
                    pr[2, row, h, rows, :] = rho4
        acc[...] = jnp.zeros_like(acc)
        if k == 2:
            for copy in moved:
                copy.wait_send()
        pressed = exchange_and_sum(
            2 * k + 1, pr, pin, (Q, C, R), n, force_stage, k, lambda: during(2 * k + 1), last_rows if k == 2 else None
        )
        if k < 2:
            for copy in moved + pressed:
                copy.wait_send()
            for row in range(2):
                move(k, row)
    for copy in arriving["tab"]:
        copy.wait_send()
    for p in (2, 3):
        finish_piece(p)
    for copy in leaving:
        copy.wait()


TILES = 48


STEPS = 4


def lay_kernel(runs, gathered, out, tiles, edge):
    subs = gathered.shape[0]
    lane = lane_iota()
    beyond = lane + LN
    step = pl.program_id(0)

    @pl.when(step == 0)
    def _():
        tiles[...] = jnp.zeros_like(tiles)
        edge[...] = jnp.zeros_like(edge)

    def lay(slot, currents):
        for row in range(2):
            for h in range(2):
                at = (step * (S // STEPS) + slot) * 4 + h * 2 + row
                later = []
                for src in range(subs):
                    end = jnp.full((8, LN), runs[2 * subs + src, at])
                    turned = pltpu.roll(gathered[src, slot * 2 + h, row], runs[src, at], 1)
                    kept = jnp.where(lane < end, turned, 0.0)
                    merged = jnp.where(lane < runs[subs + src, at], currents[src], kept)
                    tiles[src, runs[3 * subs + src, at]] = merged
                    wrapped = jnp.where(beyond < end, turned, 0.0)
                    later.append(jnp.where(end >= LN, wrapped, merged))
                currents = later
        return tuple(currents)

    currents = lax.fori_loop(0, S // STEPS, lay, tuple(edge[src] for src in range(subs)))
    for src in range(subs):
        edge[src] = currents[src]

    @pl.when(step == STEPS - 1)
    def _():
        for src in range(subs):
            last = runs[2 * subs + src, LN - 1]
            tiles[src, runs[3 * subs + src, LN - 1] + jnp.where(last >= LN, 1, 0)] = currents[src]
        for src in range(subs):
            out[pl.ds(src * TILES, TILES)] = tiles[src, pl.ds(0, TILES)]


def rows_of(a):
    lead = a.shape[:-2]
    a = a.reshape(lead + (2, 2, LN))
    a = jnp.swapaxes(a, -3, -2)
    return a


def shards(tiles, subs, offsets, velocity, mass, entropy, active_counts, targets):
    off = rows_of(offsets).reshape(3, LN, LN)
    vel = rows_of(velocity).reshape(3, LN, LN)
    mas = rows_of(mass).reshape(LN, LN)
    ent = rows_of(entropy).reshape(LN, LN)
    cnt = rows_of(active_counts).reshape(3, 4, LN)
    tgt = rows_of(targets).reshape(LN, LN)
    vmem = pl.BlockSpec(memory_space=pltpu.VMEM)
    f32 = jnp.float32
    gathered, runs = pl.pallas_call(
        functools.partial(substeps_kernel, tiles, subs),
        out_shape=[
            jax.ShapeDtypeStruct((subs, LN // 2, 2, 8, LN), f32),
            jax.ShapeDtypeStruct((4 * subs, LN), jnp.int32),
        ],
        in_specs=[vmem] * 6,
        out_specs=[pl.BlockSpec(memory_space=pl.ANY), vmem],
        scratch_shapes=[
            pltpu.VMEM((subs, LN // 2, 2, 8, LN), f32),
            pltpu.VMEM((4 * NF * 6, S, LN), f32),
            pltpu.VMEM((7, 2, 2, S, LN), f32),
            pltpu.VMEM((3, 2, 2, S, LN), f32),
            pltpu.VMEM((2, 2, S, LN), f32),
            pltpu.VMEM((3, 2, 2, S, LN), f32),
            pltpu.VMEM((2, 2, 2, S, LN), f32),
            pltpu.VMEM((6, 2, S, LN), f32),
            pltpu.VMEM((3, 2, 7, 2, S, LN), f32),
            pltpu.VMEM((3, 2, 3, 2, S, LN), f32),
            pltpu.VMEM((6, 3, 2, S, LN), f32),
            pltpu.VMEM((18 * 2 * S, 4, 8, LN), f32),
            pltpu.VMEM((18 * 2 * S, 4, 8, LN), f32),
            pltpu.VMEM((4, 256, LN), f32),
            pltpu.VMEM((LN, LN), jnp.int32),
            pltpu.VMEM((subs, 2 * subs, LN), f32),
            pltpu.SemaphoreType.DMA((2, 8)),
            pltpu.SemaphoreType.DMA((2, 8)),
            pltpu.SemaphoreType.DMA((4,)),
            pltpu.SemaphoreType.DMA((4,)),
            pltpu.SemaphoreType.DMA((4, 6)),
            pltpu.SemaphoreType.DMA((4, 6)),
            pltpu.SemaphoreType.DMA((4,)),
        ],
        compiler_params=pltpu.CompilerParams(collective_id=0, has_side_effects=True, vmem_limit_bytes=62 * 1024 * 1024),
        name="substeps",
    )(off, vel, mas, ent, cnt, tgt)
    arrived = pl.pallas_call(
        lay_kernel,
        grid=(STEPS,),
        out_shape=jax.ShapeDtypeStruct((subs * TILES, 8, LN), f32),
        in_specs=[
            pl.BlockSpec(memory_space=pltpu.SMEM),
            pl.BlockSpec((subs, LN // 2 // STEPS, 2, 8, LN), lambda i: (0, i, 0, 0, 0)),
        ],
        out_specs=pl.BlockSpec((subs * TILES, 8, LN), lambda i: (0, 0, 0)),
        scratch_shapes=[pltpu.VMEM((subs, TILES + 2, 8, LN), f32), pltpu.VMEM((subs, 8, LN), f32)],
        name="lay",
    )(runs, gathered)
    return jnp.transpose(arrived, (1, 0, 2)).reshape(8, subs * TILES * LN)


def solution(mesh):
    tiles, subs = mesh.shape["tile"], mesh.shape["sub"]
    placed = (
        P(None, None, "tile", "sub"),
        P(None, None, "tile", "sub"),
        P(None, "tile", "sub"),
        P(None, "tile", "sub"),
        P(None, "tile", "sub"),
        P(None, "tile", "sub"),
    )
    return jax.shard_map(
        functools.partial(shards, tiles, subs),
        mesh=mesh,
        in_specs=placed,
        out_specs=P(None, ("tile", "sub")),
        check_vma=False,
    )
```

```python
import functools
import math

import jax
import jax.numpy as jnp
from jax import lax
from jax.experimental import pallas as pl
from jax.experimental.pallas import tpu as pltpu
from jax.sharding import PartitionSpec as P

MESH = pl.DeviceIdType.MESH

S = 32
LN = 128
KERNEL_NORM = 21.0 / (2.0 * math.pi)
NACT = (32, 16, 8)
NMOVED = (32, 32, 16)

X, Y, Z, VX, VY, VZ, MS, Q, C, R = range(10)
NF = 10


def field(row, comp, b, h):
    return ((row * NF + comp) * 3 + b) * 2 + h


def lane_iota():
    return lax.broadcasted_iota(jnp.int32, (8, LN), 1)


def stage_ids(stage, c):
    if stage == 0:
        return c // 2, 1 + c % 2, 1
    if stage == 1:
        return c // 4, 1 + (c // 2) % 2, 2 * (c % 2)
    return c // 3, 3 * (c // 3), c % 3


STAGE_SIZE = (4, 8, 6)
STAGE_BASE = (0, 4, 12)


def substeps_kernel(
    tiles, subs, off, vel, mass, ent, cnt, tgt, done, runs, gathered, fld, st, pr, dens, acc, sq, ysend, xin, pin, yin,
    cache_w, cache_a, raw, back, pos, tab, send_sem, recv_sem, tab_send, tab_recv, piece_send, piece_recv, done_sem
):
    t, u = lax.axis_index("tile"), lax.axis_index("sub")
    up, down = lax.rem(t + 1, tiles), lax.rem(t + tiles - 1, tiles)
    right, left = lax.rem(u + 1, subs), lax.rem(u + subs - 1, subs)
    tile_of = (down, t, up)

    barrier = pltpu.get_barrier_semaphore()
    across = lax.rem(u + 2, subs)
    near = ((down, u), (up, u), (down, left), (t, left), (up, left), (down, right), (t, right), (up, right))
    for dev in near + ((t, across),):
        pl.semaphore_signal(barrier, inc=1, device_id=dev, device_id_type=MESH)

    for row in range(2):
        for h in range(2):
            count = jnp.broadcast_to(cnt[0, pl.ds(h * 2 + row, 1), :], (8, LN))
            for g in range(4):
                rows = pl.ds(g * 32 + h * 2 + row, 8, stride=4)
                dst = (row, h, pl.ds(g * 8, 8))
                for c in range(3):
                    st[(c,) + dst] = off[c, rows, :] * 4.0
                    st[(3 + c,) + dst] = vel[c, rows, :] * 16.0
                slot = lax.broadcasted_iota(jnp.int32, (8, LN), 0) + g * 8
                st[(6,) + dst] = jnp.where(slot < count, mass[rows, :] * (KERNEL_NORM / 64.0), 0.0)
                e = ent[rows, :]
                sq[(0,) + dst] = e
                sq[(1,) + dst] = jnp.sqrt(e * (5.0 / 3.0))
                pr[(2,) + dst] = jnp.full((8, LN), 4.0, jnp.float32)
    pl.semaphore_wait(barrier, 9)

    lane = lane_iota()

    def start_round(rnd, src, ncomp, n, inbox):
        for side in range(2):
            for g in range(n // 8):
                packed = jnp.zeros((8, LN), jnp.float32)
                for c in range(ncomp):
                    for row in range(2):
                        code = c * 2 + row
                        v = src[c, row, side, pl.ds(g * 8, 8), :]
                        from_lane = 127 if side == 1 else 0
                        v = pltpu.roll(v, (code - from_lane) % LN, 1)
                        packed = jnp.where(lane == code, v, packed)
                ysend[rnd, side, pl.ds(g * 8, 8), :] = packed
        copies = []
        for row, dst_t, slot in ((0, down, 1), (1, up, 0)):
            f = row
            copies.append(
                pltpu.make_async_remote_copy(
                    src_ref=src.at[pl.ds(0, ncomp), row, :, pl.ds(0, n)],
                    dst_ref=inbox.at[rnd // 2, slot, pl.ds(0, ncomp), :, pl.ds(0, n)],
                    send_sem=send_sem.at[rnd % 2, f],
                    recv_sem=recv_sem.at[rnd % 2, f],
                    device_id=(dst_t, u),
                    device_id_type=MESH,
                )
            )
        for dt in range(3):
            for side in range(2):
                f = 2 + dt * 2 + side
                copies.append(
                    pltpu.make_async_remote_copy(
                        src_ref=ysend.at[rnd, side, pl.ds(0, n)],
                        dst_ref=yin.at[rnd, 2 - dt, 1 - side, pl.ds(0, n)],
                        send_sem=send_sem.at[rnd % 2, f],
                        recv_sem=recv_sem.at[rnd % 2, f],
                        device_id=(tile_of[dt], right if side == 1 else left),
                        device_id_type=MESH,
                    )
                )
        for f in (4, 5, 0, 1, 2, 3, 6, 7):
            copies[f].start()
        return copies

    def shift_of(comp, r):
        return 4.0 * (r - 1) if comp == X else 0.0

    def centre(load, comps, r, n):
        for c, comp in enumerate(comps):
            for h in range(2):
                v = load(c, h, pl.ds(0, n))
                if comp == X and r != 1:
                    v = v + 4.0 * (r - 1)
                fld[field(r, comp, 1, h), pl.ds(0, n), :] = v

    def sides(load, comps, r, n, rnd, dt, sender_row):
        for c, comp in enumerate(comps):
            code = c * 2 + sender_row
            dx = 4.0 * (r - 1) if comp == X else 0.0
            for g in range(n // 8):
                rows = pl.ds(g * 8, 8)
                a0, a1 = load(c, 0, rows), load(c, 1, rows)
                lo = pltpu.roll(yin[rnd, dt, 0, rows, :], (0 - code) % LN, 1)
                hi = pltpu.roll(yin[rnd, dt, 1, rows, :], (127 - code) % LN, 1)
                r0, r1 = pltpu.roll(a0, 1, 1), pltpu.roll(a1, 1, 1)
                l0, l1 = pltpu.roll(a0, 127, 1), pltpu.roll(a1, 127, 1)
                first, last = lane == 0, lane == 127
                minus = [jnp.where(first, lo, r0), jnp.where(first, r0, r1)]
                plus = [jnp.where(last, l1, l0), jnp.where(last, hi, l1)]
                for h in range(2):
                    m, p = minus[h], plus[h]
                    if comp == Y:
                        m, p = m - 4.0, p + 4.0
                    elif comp == X and r != 1:
                        m, p = m + dx, p + dx
                    fld[field(r, comp, 0, h), rows, :] = m
                    fld[field(r, comp, 2, h), rows, :] = p

    def other(r, comp, b, h, j):
        return fld[field(r, comp, b, h), pl.ds(j, 8, stride=0), :]

    def own(row, comp, h, g, n):
        return fld[field(row + 1, comp, 1, h), pl.ds(g * 8, n * 8), :].reshape(n, 8, LN)

    EDGE_SLOT = 14

    def edges(comps):
        for comp in comps:
            for g in range(4):
                rows = pl.ds(g * 8, 8)

                def packed(zero, one, two, three):
                    v = fld[zero, rows, :]
                    v = jnp.where(lane == 1, pltpu.roll(fld[one, rows, :], 1, 1), v)
                    v = jnp.where(lane == 2, pltpu.roll(fld[two, rows, :], 2, 1), v)
                    return jnp.where(lane == 3, pltpu.roll(fld[three, rows, :], 4, 1), v)

                low0, low1 = field(1, comp, 1, 0), field(2, comp, 1, 0)
                fld[field(4, comp, 1, 0), rows, :] = packed(low0, low1, low1, field(2, comp, 1, 1))
                low0, low1 = field(1, comp, 0, 0), field(2, comp, 0, 0)
                fld[field(4, comp, 0, 0), rows, :] = packed(low0, low1, low0, field(1, comp, 2, 1))

    def spread_edges(sums):
        for g in range(4):
            rows = pl.ds(g * 8, 8)
            v = sums[2, 1, rows, :]
            one_two = pltpu.roll(v, 127, 1) + pltpu.roll(v, 126, 1)
            sums[0, 1, rows, :] += jnp.where(lane == 0, v, 0.0)
            sums[1, 1, rows, :] += jnp.where(lane == 0, one_two, 0.0)
            sums[1, 2, rows, :] += jnp.where(lane == 127, pltpu.roll(v, 124, 1), 0.0)

    def paired_stage(stage, body):
        if stage == 0:

            def alone(i, _):
                body(i // 2, 1 + i // 2, 1, i % 2, i, True)
                return 0

            def straight(h, _):
                body(0, 2, 1, h, 4 + h, False)
                return 0

            lax.fori_loop(0, 4, alone, 0)
            lax.fori_loop(0, 2, straight, 0)
        else:

            def slanted(ih, _):
                i, h = ih // 2, ih % 2
                body(i // 3, 1 + (i + 2) // 3, 2 - 2 * (i // 2 - i // 3), h, 6 + ih, False, True)
                return 0

            lax.fori_loop(0, 8, slanted, 0)

    def give_back(sums, which, r, b, h, alone, shifted, sign):
        for jg in range(2 if alone else 0, 4):
            rows = pl.ds(jg * 8, 8)
            part = back[which, pl.ds(jg * 64, 8, stride=8), :]
            for sub in range(1, 8):
                part = part + back[which, pl.ds(jg * 64 + sub, 8, stride=8), :]
            part = part * sign if sign != 1.0 else part
            if not shifted:
                sums[r - 1, 1 + h, rows, :] += part
            else:
                part = pltpu.roll(part, (b + (LN - 1)) % LN, 1)
                over = lane == (LN - 1) * (1 - b // 2)
                sums[r - 1, 1 + h, rows, :] += jnp.where(over, 0.0, part)
                sums[r - 1, h + b, rows, :] += jnp.where(over, part, 0.0)

    def density_paired(row, r, b, h, slot, alone, shifted=False):
        mine = [[own(row, comp, h, g, 2) for comp in (X, Y, Z, MS)] for g in (0, 2)]
        totals = [dens[row, 1 + h, pl.ds(g * 8, 16), :].reshape(2, 8, LN) for g in (0, 2)]
        for j in range(S):
            given = None
            mj = other(r, MS, b, h, j)
            for g in (0,) if alone and j < 16 else (0, 1):
                xi, yi, zi, mi = mine[g]
                dx = xi - other(r, X, b, h, j)
                dy = yi - other(r, Y, b, h, j)
                dz = zi - other(r, Z, b, h, j)
                r2 = dx * dx + dy * dy + dz * dz
                rad = r2 * lax.rsqrt(jnp.maximum(r2, 1e-30))
                s = jnp.maximum(4.0 - rad, 0.0)
                s3 = s * (s * s)
                w = s3 * (s * (5.0 - s))
                totals[g] = totals[g] + w * mj
                cache_w[slot * S + j, pl.ds(g * 2, 2)] = s3
                cache_a[slot * S + j, pl.ds(g * 2, 2)] = 1.0 / (r2 + 0.16)
                if not alone or (g == 0 and j >= 16):
                    wi = w * mi
                    wi = wi[0] + wi[1]
                    given = wi if given is None else given + wi
            if given is not None:
                back[0, pl.ds(j * 8, 8), :] = given
        for g in (0, 1):
            dens[row, 1 + h, pl.ds(g * 16, 16), :] = totals[g].reshape(16, LN)
        give_back(dens, 0, r, b, h, alone, shifted, 1.0)

    def force_paired(row, r, b, h, slot, alone, shifted=False):
        def half(g, first, backward):
            xi, yi, zi, vxi, vyi, vzi, qi, ci, ri, mi = (
                own(row, comp, h, g, 2) for comp in (X, Y, Z, VX, VY, VZ, Q, C, R, MS)
            )
            ax, ay, az = (acc[d, row, 1 + h, pl.ds(g * 8, 16), :].reshape(2, 8, LN) for d in range(3))
            for j in range(first, S):
                dx = xi - other(r, X, b, h, j)
                dy = yi - other(r, Y, b, h, j)
                dz = zi - other(r, Z, b, h, j)
                n = (
                    dx * (vxi - other(r, VX, b, h, j))
                    + dy * (vyi - other(r, VY, b, h, j))
                    + dz * (vzi - other(r, VZ, b, h, j))
                )
                mu = jnp.minimum(n, 0.0) * cache_a[slot * S + j, pl.ds(g, 2)]
                visc = (mu * (mu - (ci + other(r, C, b, h, j)))) / (ri + other(r, R, b, h, j))
                f = cache_w[slot * S + j, pl.ds(g, 2)] * (qi + other(r, Q, b, h, j) + visc)
                fi = f * other(r, MS, b, h, j)
                ax, ay, az = ax + fi * dx, ay + fi * dy, az + fi * dz
                if j >= backward:
                    fj = f * mi
                    for d, delta in enumerate((dx, dy, dz)):
                        back_d = fj * delta
                        back[d, pl.ds(j * 8, 8), :] = back_d[0] + back_d[1]
            for d, total in enumerate((ax, ay, az)):
                acc[d, row, 1 + h, pl.ds(g * 8, 16), :] = total.reshape(16, LN)
            if backward < S:
                for d in range(3):
                    give_back(acc.at[d], d, r, b, h, alone, shifted, -1.0)

        if alone:
            half(0, 0, 16)
            half(2, 16, S)
        else:

            def part(i, _):
                half(i * 2, 0, 0)
                return 0

            lax.fori_loop(0, 2, part, 0)

    def density_stage(stage, k, first=0, last=2):
        per = NACT[k] // 8
        halves = 2 if per == 1 else 1
        base = STAGE_BASE[stage]

        def pairs(c, h, edge=False):
            row, r, b = (2, 4, 0) if edge else stage_ids(stage, c)
            xi, yi, zi = (own(3 if edge else row, comp, h, 0, per) for comp in (X, Y, Z))
            slot = EDGE_SLOT if edge else (base + c) * 2 + h
            total = dens[row, 1 + h, pl.ds(0, per * 8), :].reshape(per, 8, LN)
            for j in range(S):
                dx = xi - other(r, X, b, h, j)
                dy = yi - other(r, Y, b, h, j)
                dz = zi - other(r, Z, b, h, j)
                r2 = dx * dx + dy * dy + dz * dz
                rad = r2 * lax.rsqrt(jnp.maximum(r2, 1e-30))
                s = jnp.maximum(4.0 - rad, 0.0)
                w3 = (s * other(r, MS, b, h, j)) * (s * s)
                total = total + w3 * (s * (5.0 - s))
                cache_w[slot * S + j, pl.ds(0, per)] = w3
                cache_a[slot * S + j, pl.ds(0, per)] = 1.0 / (r2 + 0.16)
            dens[row, 1 + h, pl.ds(0, per * 8), :] = total.reshape(per * 8, LN)

        def combo(i, _):
            if halves == 2:
                pairs(i, 0)
                pairs(i, 1)
            else:
                pairs(i // 2, i % 2)
            return 0

        if k == 0 and stage < 2:
            paired_stage(stage, density_paired)
            if stage == 1:
                pairs(0, 0, edge=True)
                spread_edges(dens)
            return
        per_row = STAGE_SIZE[stage] // halves
        lax.fori_loop(first * per_row, last * per_row, combo, 0)

    def force_stage(stage, k, first=0, last=2):
        groups = NACT[k] // 8
        per = min(groups, 2)
        sets = groups // per
        halves = 2 if per == 1 else 1
        base = STAGE_BASE[stage]

        def pairs(c, h, g, edge=False):
            row, r, b = (2, 4, 0) if edge else stage_ids(stage, c)
            xi, yi, zi, vxi, vyi, vzi, qi, ci, ri = (
                own(3 if edge else row, comp, h, g, per) for comp in (X, Y, Z, VX, VY, VZ, Q, C, R)
            )
            slot = EDGE_SLOT if edge else (base + c) * 2 + h
            ax, ay, az = (acc[d, row, 1 + h, pl.ds(g * 8, per * 8), :].reshape(per, 8, LN) for d in range(3))
            for j in range(S):
                dx = xi - other(r, X, b, h, j)
                dy = yi - other(r, Y, b, h, j)
                dz = zi - other(r, Z, b, h, j)
                n = (
                    dx * (vxi - other(r, VX, b, h, j))
                    + dy * (vyi - other(r, VY, b, h, j))
                    + dz * (vzi - other(r, VZ, b, h, j))
                )
                mu = jnp.minimum(n, 0.0) * cache_a[slot * S + j, pl.ds(g, per)]
                sound = ci + other(r, C, b, h, j)
                visc = (mu * (mu - sound)) / (ri + other(r, R, b, h, j))
                f = cache_w[slot * S + j, pl.ds(g, per)] * (qi + other(r, Q, b, h, j) + visc)
                ax, ay, az = ax + f * dx, ay + f * dy, az + f * dz
            for d, total in enumerate((ax, ay, az)):
                acc[d, row, 1 + h, pl.ds(g * 8, per * 8), :] = total.reshape(per * 8, LN)

        def combo(i, _):
            if halves == 2:
                pairs(i, 0, 0)
                pairs(i, 1, 0)
            else:
                ch, g = i // sets, (i % sets) * per
                pairs(ch // 2, ch % 2, g)
            return 0

        if k == 0 and stage < 2:
            paired_stage(stage, force_paired)
            if stage == 1:

                def edge(i, _):
                    pairs(0, 0, i * 2, edge=True)
                    return 0

                lax.fori_loop(0, 2, edge, 0)
                for d in range(3):
                    spread_edges(acc.at[d])
            return
        per_row = STAGE_SIZE[stage] * sets // halves
        lax.fori_loop(first * per_row, last * per_row, combo, 0)

    def plan():
        row_i = lax.broadcasted_iota(jnp.int32, (LN, LN), 0)
        col_i = lax.broadcasted_iota(jnp.int32, (LN, LN), 1)
        before = jnp.where(row_i < col_i, 1.0, 0.0).astype(jnp.bfloat16)
        ones = jnp.ones((LN, LN), jnp.bfloat16)
        row8 = lax.broadcasted_iota(jnp.int32, (8, LN), 0)
        dest = tgt[...]
        start = jnp.zeros((LN, LN), jnp.float32)
        place = jnp.zeros((LN, LN), jnp.float32)
        start_t = jnp.zeros((8, LN), jnp.float32)
        info = jnp.zeros((8, LN), jnp.float32)
        for d in range(subs):
            mine = dest == d
            hot = jnp.where(mine, 1.0, 0.0).astype(jnp.bfloat16)
            inside = jnp.dot(hot, before, preferred_element_type=jnp.float32)
            place = jnp.where(mine, start + inside, place)
            start = start + jnp.dot(hot, ones, preferred_element_type=jnp.float32)
            count_t = lax.dot_general(
                ones[0:8], hot, (((1,), (1,)), ((), ())), preferred_element_type=jnp.float32
            )
            info = jnp.where(row8 == d, start_t, info)
            info = jnp.where(row8 == subs + d, count_t, info)
            start_t = start_t + count_t
        pos[...] = place.astype(jnp.int32)
        tab[u] = info
        sends = []
        for k in range(1, subs):
            copy = pltpu.make_async_remote_copy(
                src_ref=tab.at[u],
                dst_ref=tab.at[u],
                send_sem=tab_send.at[k],
                recv_sem=tab_recv.at[k],
                device_id=(t, lax.rem(u + k, subs)),
                device_id_type=MESH,
            )
            copy.start()
            sends.append(copy)
        return sends

    def emit(g, own_rows):
        row_q = lax.broadcasted_iota(jnp.int32, (LN, LN), 0)
        for row in own_rows:
            for h in range(2):
                count = jnp.broadcast_to(cnt[0, pl.ds(h * 2 + row, 1), :], (8, LN))
                rows = pl.ds(g * 8, 8)
                slot = lax.broadcasted_iota(jnp.int32, (8, LN), 0) + g * 8
                in_rows = pl.ds(g * 32 + h * 2 + row, 8, stride=4)
                values = [st[d, row, h, rows, :] * 0.25 for d in range(3)]
                values += [st[3 + d, row, h, rows, :] * 0.0625 for d in range(3)]
                values += [pr[2, row, h, rows, :] * 0.25]
                values += [jnp.where(slot < count, mass[in_rows, :], 0.0)]
                for i, v in enumerate(values):
                    raw[g, pl.ds((row * 2 + h) * 64 + i, 8, stride=8), :] = v

        def sort(rh, _):
            row, h = rh // 2, rh % 2
            for i in range(8):
                slot = g * 8 + i
                line = pos[pl.ds(slot * 4 + h * 2 + row, 1), :]
                hot = jnp.where(row_q == jnp.broadcast_to(line, (LN, LN)), 1.0, 0.0)
                v = raw[g, pl.ds(rh * 64 + i * 8, 8), :]
                hi = v.astype(jnp.bfloat16)
                rest = v - hi.astype(jnp.float32)
                mid = rest.astype(jnp.bfloat16)
                low = (rest - mid.astype(jnp.float32)).astype(jnp.bfloat16)
                pieces = jnp.concatenate([hi, mid, low], axis=0)
                moved = lax.dot_general(
                    pieces, hot.astype(jnp.bfloat16), (((1,), (1,)), ((), ())), preferred_element_type=jnp.float32
                )
                gathered[u, slot * 2 + h, row] = (moved[0:8] + moved[8:16]) + moved[16:24]
            return 0

        lax.fori_loop(own_rows[0] * 2, own_rows[-1] * 2 + 2, sort, 0)

    PIECES = ((32, 32, (0, 1)), (16, 16, (0, 1)), (0, 16, (0,)), (0, 16, (1,)))

    def piece_copy(p, flow, owner, second_half, dst):
        first, rows, own_rows = PIECES[p]
        half = rows // 2
        part = pl.ds(first + half * second_half, half)
        which = slice(None) if len(own_rows) == 2 else own_rows[0]
        return pltpu.make_async_remote_copy(
            src_ref=gathered.at[owner, part, which],
            dst_ref=gathered.at[owner, part, which],
            send_sem=piece_send.at[p, flow],
            recv_sem=piece_recv.at[p, flow],
            device_id=(t, dst),
            device_id_type=MESH,
        )

    def start_piece(p, before_rest=None):
        first, rows, own_rows = PIECES[p]
        for g in range(first // 16, (first + rows) // 16):
            emit(g, own_rows)
        copies = [
            piece_copy(p, 0, u, 0, right),
            piece_copy(p, 1, u, 1, right),
            piece_copy(p, 2, u, 1, left),
            piece_copy(p, 3, u, 0, left),
        ]
        arriving[p] = copies
        copies[0].start()
        copies[2].start()
        if before_rest is not None:
            before_rest()
        copies[1].start()
        copies[3].start()

    def forward_piece(p):
        arriving[p][0].wait_recv()
        arriving[p][2].wait_recv()
        copies = [piece_copy(p, 4, left, 0, right), piece_copy(p, 5, right, 1, left)]
        for copy in copies:
            copy.start()
        arriving[p] += copies

    leaving = []

    def finish_piece(p):
        for f in (1, 3, 4, 5):
            arriving[p][f].wait_recv()
        for copy in arriving[p]:
            copy.wait_send()
        first, rows, own_rows = PIECES[p]
        which = slice(None) if len(own_rows) == 2 else own_rows[0]
        copy = pltpu.make_async_copy(
            gathered.at[:, pl.ds(first, rows), which], done.at[:, pl.ds(first, rows), which], done_sem.at[p]
        )
        copy.start()
        leaving.append(copy)

    def exchange_and_sum(rnd, src, inbox, comps, n, stage_fn, k, meanwhile, row_done=None):
        copies = start_round(rnd, src, len(comps), n, inbox)
        meanwhile()
        loads = [None] * 4
        for r in (1, 2):
            loads[r] = functools.partial(lambda row, c, h, rows: src[c, row, h, rows, :], r - 1)
        loads[0] = lambda c, h, rows: inbox[rnd // 2, 0, c, h, rows, :]
        loads[3] = lambda c, h, rows: inbox[rnd // 2, 1, c, h, rows, :]
        for r in (1, 2):
            centre(loads[r], comps, r, n)
        stage_fn(0, k)
        copies[4].wait_recv()
        copies[5].wait_recv()
        for r in (1, 2):
            sides(loads[r], comps, r, n, rnd, 1, r - 1)
        if k == 0:
            edges(comps)
        stage_fn(1, k, 0, 2 if row_done is None else 1)
        for f in (0, 1, 2, 3, 6, 7):
            copies[f].wait_recv()
        for r, dt, sender_row in ((0, 0, 1), (3, 2, 0)):
            centre(loads[r], comps, r, n)
            sides(loads[r], comps, r, n, rnd, dt, sender_row)
        if row_done is None:
            stage_fn(2, k)
            return copies
        for copy in copies:
            copy.wait_send()
        stage_fn(2, k, 0, 1)
        row_done(0)
        stage_fn(1, k, 1, 2)
        row_done(1)
        stage_fn(2, k, 1, 2)
        row_done(2)
        return []

    arriving = {}

    def lay_plan():
        for copy in arriving["tab"]:
            copy.wait_recv()
        row_i = lax.broadcasted_iota(jnp.int32, (LN, LN), 0)
        col_i = lax.broadcasted_iota(jnp.int32, (LN, LN), 1)

        def order(i):
            return (i // 4) * 4 + (i % 2) * 2 + (i // 2) % 2

        earlier = jnp.where(order(row_i) < order(col_i), 1.0, 0.0).astype(jnp.bfloat16)
        starts = jnp.concatenate([tab[src, pl.ds(u, 1), :] for src in range(subs)], axis=0)
        counts = jnp.concatenate([tab[src, pl.ds(subs + u, 1), :] for src in range(subs)], axis=0)
        padded = jnp.concatenate([counts, jnp.zeros_like(counts)], axis=0).astype(jnp.bfloat16)
        base = jnp.dot(padded, earlier, preferred_element_type=jnp.float32)[0:subs]
        base = base.astype(jnp.int32)
        skip = base & (LN - 1)
        runs[0:subs, :] = (skip - starts.astype(jnp.int32)) & (LN - 1)
        runs[subs : 2 * subs, :] = skip
        runs[2 * subs : 3 * subs, :] = skip + counts.astype(jnp.int32)
        runs[3 * subs : 4 * subs, :] = base >> 7

    def during(rnd):
        if rnd == 0:
            arriving["tab"] = plan()
        elif rnd == 1:
            lay_plan()
        elif rnd in (2, 4):
            if rnd == 4:
                finish_piece(0)
            start_piece(rnd // 2 - 1)
        elif rnd in (3, 5):
            forward_piece(rnd // 2 - 1)

    def move(k, row):
        for h in range(2):
            count = jnp.broadcast_to(cnt[k, pl.ds(h * 2 + row, 1), :], (8, LN))
            for g in range(NACT[k] // 8):
                rows = pl.ds(g * 8, 8)
                slot = lax.broadcasted_iota(jnp.int32, (8, LN), 0) + g * 8
                active = slot < count
                for d in range(3):
                    v = st[3 + d, row, h, rows, :]
                    x = st[d, row, h, rows, :]
                    v_new = v + 4.0 * acc[d, row, 1 + h, rows, :]
                    st[3 + d, row, h, rows, :] = jnp.where(active, v_new, v)
                    st[d, row, h, rows, :] = jnp.where(active, x + 0.0125 * v_new, x)

    def last_rows(step):
        if step == 0:
            move(2, 0)
            start_piece(2)
        elif step == 2:
            finish_piece(1)
            move(2, 1)
            start_piece(3, lambda: forward_piece(2))
            forward_piece(3)

    for k in range(3):
        n = NACT[k]
        dens[...] = jnp.zeros_like(dens)
        comps = (X, Y, Z, VX, VY, VZ) + ((MS,) if k == 0 else ())
        moved = exchange_and_sum(2 * k, st, xin, comps, NMOVED[k], density_stage, k, lambda: during(2 * k))
        for row in range(2):
            for h in range(2):
                count = jnp.broadcast_to(cnt[k, pl.ds(h * 2 + row, 1), :], (8, LN))
                for g in range(n // 8):
                    rows = pl.ds(g * 8, 8)
                    slot = lax.broadcasted_iota(jnp.int32, (8, LN), 0) + g * 8
                    rho4 = jnp.where(slot < count, dens[row, 1 + h, rows, :], pr[2, row, h, rows, :])
                    root = jnp.exp(jnp.log(rho4 * 0.25) * (1.0 / 3.0))
                    pr[0, row, h, rows, :] = sq[0, row, h, rows, :] / root
                    pr[1, row, h, rows, :] = sq[1, row, h, rows, :] * root
                    pr[2, row, h, rows, :] = rho4
        acc[...] = jnp.zeros_like(acc)
        if k == 2:
            for copy in moved:
                copy.wait_send()
        pressed = exchange_and_sum(
            2 * k + 1, pr, pin, (Q, C, R), n, force_stage, k, lambda: during(2 * k + 1), last_rows if k == 2 else None
        )
        if k < 2:
            for copy in moved + pressed:
                copy.wait_send()
            for row in range(2):
                move(k, row)
    for copy in arriving["tab"]:
        copy.wait_send()
    for p in (2, 3):
        finish_piece(p)
    for copy in leaving:
        copy.wait()


TILES = 48


STEPS = 4


def lay_kernel(runs, gathered, out, tiles, edge):
    subs = gathered.shape[0]
    lane = lane_iota()
    beyond = lane + LN
    step = pl.program_id(0)

    @pl.when(step == 0)
    def _():
        tiles[...] = jnp.zeros_like(tiles)
        edge[...] = jnp.zeros_like(edge)

    def lay(slot, currents):
        for row in range(2):
            for h in range(2):
                at = (step * (S // STEPS) + slot) * 4 + h * 2 + row
                later = []
                for src in range(subs):
                    end = jnp.full((8, LN), runs[2 * subs + src, at])
                    turned = pltpu.roll(gathered[src, slot * 2 + h, row], runs[src, at], 1)
                    kept = jnp.where(lane < end, turned, 0.0)
                    merged = jnp.where(lane < runs[subs + src, at], currents[src], kept)
                    tiles[src, runs[3 * subs + src, at]] = merged
                    wrapped = jnp.where(beyond < end, turned, 0.0)
                    later.append(jnp.where(end >= LN, wrapped, merged))
                currents = later
        return tuple(currents)

    currents = lax.fori_loop(0, S // STEPS, lay, tuple(edge[src] for src in range(subs)))
    for src in range(subs):
        edge[src] = currents[src]

    @pl.when(step == STEPS - 1)
    def _():
        for src in range(subs):
            last = runs[2 * subs + src, LN - 1]
            tiles[src, runs[3 * subs + src, LN - 1] + jnp.where(last >= LN, 1, 0)] = currents[src]
        for src in range(subs):
            out[pl.ds(src * TILES, TILES)] = tiles[src, pl.ds(0, TILES)]


def rows_of(a):
    lead = a.shape[:-2]
    a = a.reshape(lead + (2, 2, LN))
    a = jnp.swapaxes(a, -3, -2)
    return a


def shards(tiles, subs, offsets, velocity, mass, entropy, active_counts, targets):
    off = rows_of(offsets).reshape(3, LN, LN)
    vel = rows_of(velocity).reshape(3, LN, LN)
    mas = rows_of(mass).reshape(LN, LN)
    ent = rows_of(entropy).reshape(LN, LN)
    cnt = rows_of(active_counts).reshape(3, 4, LN)
    tgt = rows_of(targets).reshape(LN, LN)
    vmem = pl.BlockSpec(memory_space=pltpu.VMEM)
    f32 = jnp.float32
    gathered, runs = pl.pallas_call(
        functools.partial(substeps_kernel, tiles, subs),
        out_shape=[
            jax.ShapeDtypeStruct((subs, LN // 2, 2, 8, LN), f32),
            jax.ShapeDtypeStruct((4 * subs, LN), jnp.int32),
        ],
        in_specs=[vmem] * 6,
        out_specs=[pl.BlockSpec(memory_space=pl.ANY), vmem],
        scratch_shapes=[
            pltpu.VMEM((subs, LN // 2, 2, 8, LN), f32),
            pltpu.VMEM((5 * NF * 6, S, LN), f32),
            pltpu.VMEM((7, 2, 2, S, LN), f32),
            pltpu.VMEM((3, 2, 2, S, LN), f32),
            pltpu.VMEM((3, 4, S, LN), f32),
            pltpu.VMEM((3, 3, 4, S, LN), f32),
            pltpu.VMEM((2, 2, 2, S, LN), f32),
            pltpu.VMEM((6, 2, S, LN), f32),
            pltpu.VMEM((3, 2, 7, 2, S, LN), f32),
            pltpu.VMEM((3, 2, 3, 2, S, LN), f32),
            pltpu.VMEM((6, 3, 2, S, LN), f32),
            pltpu.VMEM((18 * 2 * S, 4, 8, LN), f32),
            pltpu.VMEM((18 * 2 * S, 4, 8, LN), f32),
            pltpu.VMEM((4, 256, LN), f32),
            pltpu.VMEM((3, 256, LN), f32),
            pltpu.VMEM((LN, LN), jnp.int32),
            pltpu.VMEM((subs, 2 * subs, LN), f32),
            pltpu.SemaphoreType.DMA((2, 8)),
            pltpu.SemaphoreType.DMA((2, 8)),
            pltpu.SemaphoreType.DMA((4,)),
            pltpu.SemaphoreType.DMA((4,)),
            pltpu.SemaphoreType.DMA((4, 6)),
            pltpu.SemaphoreType.DMA((4, 6)),
            pltpu.SemaphoreType.DMA((4,)),
        ],
        compiler_params=pltpu.CompilerParams(collective_id=0, has_side_effects=True, vmem_limit_bytes=62 * 1024 * 1024),
        name="substeps",
    )(off, vel, mas, ent, cnt, tgt)
    arrived = pl.pallas_call(
        lay_kernel,
        grid=(STEPS,),
        out_shape=jax.ShapeDtypeStruct((subs * TILES, 8, LN), f32),
        in_specs=[
            pl.BlockSpec(memory_space=pltpu.SMEM),
            pl.BlockSpec((subs, LN // 2 // STEPS, 2, 8, LN), lambda i: (0, i, 0, 0, 0)),
        ],
        out_specs=pl.BlockSpec((subs * TILES, 8, LN), lambda i: (0, 0, 0)),
        scratch_shapes=[pltpu.VMEM((subs, TILES + 2, 8, LN), f32), pltpu.VMEM((subs, 8, LN), f32)],
        name="lay",
    )(runs, gathered)
    return jnp.transpose(arrived, (1, 0, 2)).reshape(8, subs * TILES * LN)


def solution(mesh):
    tiles, subs = mesh.shape["tile"], mesh.shape["sub"]
    placed = (
        P(None, None, "tile", "sub"),
        P(None, None, "tile", "sub"),
        P(None, "tile", "sub"),
        P(None, "tile", "sub"),
        P(None, "tile", "sub"),
        P(None, "tile", "sub"),
    )
    return jax.shard_map(
        functools.partial(shards, tiles, subs),
        mesh=mesh,
        in_specs=placed,
        out_specs=P(None, ("tile", "sub")),
        check_vma=False,
    )
```

```python
import functools
import math

import jax
import jax.numpy as jnp
from jax import lax
from jax.experimental import pallas as pl
from jax.experimental.pallas import tpu as pltpu
from jax.sharding import PartitionSpec as P

MESH = pl.DeviceIdType.MESH

S = 32
LN = 128
KERNEL_NORM = 21.0 / (2.0 * math.pi)
NACT = (32, 16, 8)
NMOVED = (32, 32, 16)

X, Y, Z, VX, VY, VZ, MS, Q, C, R = range(10)
NF = 10


def field(row, comp, b, h):
    return ((row * NF + comp) * 3 + b) * 2 + h


def lane_iota():
    return lax.broadcasted_iota(jnp.int32, (8, LN), 1)


def stage_ids(stage, c):
    if stage == 0:
        return c // 2, 1 + c % 2, 1
    if stage == 1:
        return c // 4, 1 + (c // 2) % 2, 2 * (c % 2)
    return c // 3, 3 * (c // 3), c % 3


STAGE_SIZE = (4, 8, 6)
STAGE_BASE = (0, 4, 12)


def substeps_kernel(
    tiles, subs, off, vel, mass, ent, cnt, tgt, done, runs, gathered, fld, st, pr, dens, acc, sq, ysend, xin, pin, yin,
    cache_w, cache_a, raw, back, pos, tab, send_sem, recv_sem, tab_send, tab_recv, piece_send, piece_recv, done_sem
):
    t, u = lax.axis_index("tile"), lax.axis_index("sub")
    up, down = lax.rem(t + 1, tiles), lax.rem(t + tiles - 1, tiles)
    right, left = lax.rem(u + 1, subs), lax.rem(u + subs - 1, subs)
    tile_of = (down, t, up)

    barrier = pltpu.get_barrier_semaphore()
    across = lax.rem(u + 2, subs)
    near = ((down, u), (up, u), (down, left), (t, left), (up, left), (down, right), (t, right), (up, right))
    for dev in near + ((t, across),):
        pl.semaphore_signal(barrier, inc=1, device_id=dev, device_id_type=MESH)

    for row in range(2):
        for h in range(2):
            count = jnp.broadcast_to(cnt[0, pl.ds(h * 2 + row, 1), :], (8, LN))
            for g in range(4):
                rows = pl.ds(g * 32 + h * 2 + row, 8, stride=4)
                dst = (row, h, pl.ds(g * 8, 8))
                for c in range(3):
                    st[(c,) + dst] = off[c, rows, :] * 4.0
                    st[(3 + c,) + dst] = vel[c, rows, :] * 16.0
                slot = lax.broadcasted_iota(jnp.int32, (8, LN), 0) + g * 8
                st[(6,) + dst] = jnp.where(slot < count, mass[rows, :] * (KERNEL_NORM / 64.0), 0.0)
                e = ent[rows, :]
                sq[(0,) + dst] = e
                sq[(1,) + dst] = jnp.sqrt(e * (5.0 / 3.0))
                pr[(2,) + dst] = jnp.full((8, LN), 4.0, jnp.float32)
    pl.semaphore_wait(barrier, 9)

    lane = lane_iota()

    def start_round(rnd, src, ncomp, n, inbox):
        for side in range(2):
            for g in range(n // 8):
                packed = jnp.zeros((8, LN), jnp.float32)
                for c in range(ncomp):
                    for row in range(2):
                        code = c * 2 + row
                        v = src[c, row, side, pl.ds(g * 8, 8), :]
                        from_lane = 127 if side == 1 else 0
                        v = pltpu.roll(v, (code - from_lane) % LN, 1)
                        packed = jnp.where(lane == code, v, packed)
                ysend[rnd, side, pl.ds(g * 8, 8), :] = packed
        copies = []
        for row, dst_t, slot in ((0, down, 1), (1, up, 0)):
            f = row
            copies.append(
                pltpu.make_async_remote_copy(
                    src_ref=src.at[pl.ds(0, ncomp), row, :, pl.ds(0, n)],
                    dst_ref=inbox.at[rnd // 2, slot, pl.ds(0, ncomp), :, pl.ds(0, n)],
                    send_sem=send_sem.at[rnd % 2, f],
                    recv_sem=recv_sem.at[rnd % 2, f],
                    device_id=(dst_t, u),
                    device_id_type=MESH,
                )
            )
        for dt in range(3):
            for side in range(2):
                f = 2 + dt * 2 + side
                copies.append(
                    pltpu.make_async_remote_copy(
                        src_ref=ysend.at[rnd, side, pl.ds(0, n)],
                        dst_ref=yin.at[rnd, 2 - dt, 1 - side, pl.ds(0, n)],
                        send_sem=send_sem.at[rnd % 2, f],
                        recv_sem=recv_sem.at[rnd % 2, f],
                        device_id=(tile_of[dt], right if side == 1 else left),
                        device_id_type=MESH,
                    )
                )
        for f in (4, 5, 0, 1, 2, 3, 6, 7):
            copies[f].start()
        return copies

    def shift_of(comp, r):
        return 4.0 * (r - 1) if comp == X else 0.0

    def centre(load, comps, r, n):
        for c, comp in enumerate(comps):
            for h in range(2):
                v = load(c, h, pl.ds(0, n))
                if comp == X and r != 1:
                    v = v + 4.0 * (r - 1)
                fld[field(r, comp, 1, h), pl.ds(0, n), :] = v

    def sides(load, comps, r, n, rnd, dt, sender_row):
        for c, comp in enumerate(comps):
            code = c * 2 + sender_row
            dx = 4.0 * (r - 1) if comp == X else 0.0
            for g in range(n // 8):
                rows = pl.ds(g * 8, 8)
                a0, a1 = load(c, 0, rows), load(c, 1, rows)
                lo = pltpu.roll(yin[rnd, dt, 0, rows, :], (0 - code) % LN, 1)
                hi = pltpu.roll(yin[rnd, dt, 1, rows, :], (127 - code) % LN, 1)
                r0, r1 = pltpu.roll(a0, 1, 1), pltpu.roll(a1, 1, 1)
                l0, l1 = pltpu.roll(a0, 127, 1), pltpu.roll(a1, 127, 1)
                first, last = lane == 0, lane == 127
                minus = [jnp.where(first, lo, r0), jnp.where(first, r0, r1)]
                plus = [jnp.where(last, l1, l0), jnp.where(last, hi, l1)]
                for h in range(2):
                    m, p = minus[h], plus[h]
                    if comp == Y:
                        m, p = m - 4.0, p + 4.0
                    elif comp == X and r != 1:
                        m, p = m + dx, p + dx
                    fld[field(r, comp, 0, h), rows, :] = m
                    fld[field(r, comp, 2, h), rows, :] = p

    def other(r, comp, b, h, j):
        return fld[field(r, comp, b, h), pl.ds(j, 8, stride=0), :]

    def own(row, comp, h, g, n):
        return fld[field(row + 1, comp, 1, h), pl.ds(g * 8, n * 8), :].reshape(n, 8, LN)

    EDGE_SLOT = 14

    def edges(comps):
        for comp in comps:
            for g in range(4):
                rows = pl.ds(g * 8, 8)

                def packed(zero, one, two, three):
                    v = fld[zero, rows, :]
                    v = jnp.where(lane == 1, pltpu.roll(fld[one, rows, :], 1, 1), v)
                    v = jnp.where(lane == 2, pltpu.roll(fld[two, rows, :], 2, 1), v)
                    return jnp.where(lane == 3, pltpu.roll(fld[three, rows, :], 4, 1), v)

                low0, low1 = field(1, comp, 1, 0), field(2, comp, 1, 0)
                fld[field(4, comp, 1, 0), rows, :] = packed(low0, low1, low1, field(2, comp, 1, 1))
                low0, low1 = field(1, comp, 0, 0), field(2, comp, 0, 0)
                fld[field(4, comp, 0, 0), rows, :] = packed(low0, low1, low0, field(1, comp, 2, 1))

    def spread_edges(sums):
        for g in range(4):
            rows = pl.ds(g * 8, 8)
            v = sums[2, 1, rows, :]
            one_two = pltpu.roll(v, 127, 1) + pltpu.roll(v, 126, 1)
            sums[0, 1, rows, :] += jnp.where(lane == 0, v, 0.0)
            sums[1, 1, rows, :] += jnp.where(lane == 0, one_two, 0.0)
            sums[1, 2, rows, :] += jnp.where(lane == 127, pltpu.roll(v, 124, 1), 0.0)

    def paired_stage(stage, body):
        if stage == 0:

            def alone(i, _):
                body(i // 2, 1 + i // 2, 1, i % 2, i, True)
                return 0

            def straight(h, _):
                body(0, 2, 1, h, 4 + h, False)
                return 0

            lax.fori_loop(0, 4, alone, 0)
            lax.fori_loop(0, 2, straight, 0)
        else:

            def slanted(ih, _):
                i, h = ih // 2, ih % 2
                body(i // 3, 1 + (i + 2) // 3, 2 - 2 * (i // 2 - i // 3), h, 6 + ih, False, True)
                return 0

            lax.fori_loop(0, 8, slanted, 0)

    def give_back(sums, which, r, b, h, alone, shifted, sign):
        for jg in range(2 if alone else 0, 4):
            rows = pl.ds(jg * 8, 8)
            part = back[which, pl.ds(jg * 64, 8, stride=8), :]
            for sub in range(1, 8):
                part = part + back[which, pl.ds(jg * 64 + sub, 8, stride=8), :]
            part = part * sign if sign != 1.0 else part
            if not shifted:
                sums[r - 1, 1 + h, rows, :] += part
            else:
                part = pltpu.roll(part, (b + (LN - 1)) % LN, 1)
                over = lane == (LN - 1) * (1 - b // 2)
                sums[r - 1, 1 + h, rows, :] += jnp.where(over, 0.0, part)
                sums[r - 1, h + b, rows, :] += jnp.where(over, part, 0.0)

    def density_paired(row, r, b, h, slot, alone, shifted=False):
        mine = [[own(row, comp, h, g, 2) for comp in (X, Y, Z, MS)] for g in (0, 2)]
        totals = [dens[row, 1 + h, pl.ds(g * 8, 16), :].reshape(2, 8, LN) for g in (0, 2)]
        for j in range(S):
            given = None
            mj = other(r, MS, b, h, j)
            for g in (0,) if alone and j < 16 else (0, 1):
                xi, yi, zi, mi = mine[g]
                dx = xi - other(r, X, b, h, j)
                dy = yi - other(r, Y, b, h, j)
                dz = zi - other(r, Z, b, h, j)
                r2 = dx * dx + dy * dy + dz * dz
                rad = r2 * lax.rsqrt(jnp.maximum(r2, 1e-30))
                s = jnp.maximum(4.0 - rad, 0.0)
                s3 = s * (s * s)
                w = s3 * (s * (5.0 - s))
                totals[g] = totals[g] + w * mj
                cache_w[slot * S + j, pl.ds(g * 2, 2)] = s3
                cache_a[slot * S + j, pl.ds(g * 2, 2)] = 1.0 / (r2 + 0.16)
                if not alone or (g == 0 and j >= 16):
                    wi = w * mi
                    wi = wi[0] + wi[1]
                    given = wi if given is None else given + wi
            if given is not None:
                back[0, pl.ds(j * 8, 8), :] = given
        for g in (0, 1):
            dens[row, 1 + h, pl.ds(g * 16, 16), :] = totals[g].reshape(16, LN)
        give_back(dens, 0, r, b, h, alone, shifted, 1.0)

    def force_paired(row, r, b, h, slot, alone, shifted=False):
        def half(g, first, backward):
            xi, yi, zi, vxi, vyi, vzi, qi, ci, ri, mi = (
                own(row, comp, h, g, 2) for comp in (X, Y, Z, VX, VY, VZ, Q, C, R, MS)
            )
            ax, ay, az = (acc[d, row, 1 + h, pl.ds(g * 8, 16), :].reshape(2, 8, LN) for d in range(3))
            for j in range(first, S):
                dx = xi - other(r, X, b, h, j)
                dy = yi - other(r, Y, b, h, j)
                dz = zi - other(r, Z, b, h, j)
                n = (
                    dx * (vxi - other(r, VX, b, h, j))
                    + dy * (vyi - other(r, VY, b, h, j))
                    + dz * (vzi - other(r, VZ, b, h, j))
                )
                mu = jnp.minimum(n, 0.0) * cache_a[slot * S + j, pl.ds(g, 2)]
                visc = (mu * (mu - (ci + other(r, C, b, h, j)))) / (ri + other(r, R, b, h, j))
                f = cache_w[slot * S + j, pl.ds(g, 2)] * (qi + other(r, Q, b, h, j) + visc)
                fi = f * other(r, MS, b, h, j)
                ax, ay, az = ax + fi * dx, ay + fi * dy, az + fi * dz
                if j >= backward:
                    fj = f * mi
                    for d, delta in enumerate((dx, dy, dz)):
                        back_d = fj * delta
                        back[d, pl.ds(j * 8, 8), :] = back_d[0] + back_d[1]
            for d, total in enumerate((ax, ay, az)):
                acc[d, row, 1 + h, pl.ds(g * 8, 16), :] = total.reshape(16, LN)
            if backward < S:
                for d in range(3):
                    give_back(acc.at[d], d, r, b, h, alone, shifted, -1.0)

        if alone:
            half(0, 0, 16)
            half(2, 16, S)
        else:

            def part(i, _):
                half(i * 2, 0, 0)
                return 0

            lax.fori_loop(0, 2, part, 0)

    def density_stage(stage, k, first=0, last=2):
        per = NACT[k] // 8
        halves = 2 if per == 1 else 1
        base = STAGE_BASE[stage]

        def pairs(c, h, edge=False):
            row, r, b = (2, 4, 0) if edge else stage_ids(stage, c)
            xi, yi, zi = (own(3 if edge else row, comp, h, 0, per) for comp in (X, Y, Z))
            slot = EDGE_SLOT if edge else (base + c) * 2 + h
            total = dens[row, 1 + h, pl.ds(0, per * 8), :].reshape(per, 8, LN)
            for j in range(S):
                dx = xi - other(r, X, b, h, j)
                dy = yi - other(r, Y, b, h, j)
                dz = zi - other(r, Z, b, h, j)
                r2 = dx * dx + dy * dy + dz * dz
                rad = r2 * lax.rsqrt(jnp.maximum(r2, 1e-30))
                s = jnp.maximum(4.0 - rad, 0.0)
                w3 = (s * other(r, MS, b, h, j)) * (s * s)
                total = total + w3 * (s * (5.0 - s))
                cache_w[slot * S + j, pl.ds(0, per)] = w3
                cache_a[slot * S + j, pl.ds(0, per)] = 1.0 / (r2 + 0.16)
            dens[row, 1 + h, pl.ds(0, per * 8), :] = total.reshape(per * 8, LN)

        def combo(i, _):
            if halves == 2:
                pairs(i, 0)
                pairs(i, 1)
            else:
                pairs(i // 2, i % 2)
            return 0

        if k == 0 and stage < 2:
            paired_stage(stage, density_paired)
            if stage == 1:
                pairs(0, 0, edge=True)
                spread_edges(dens)
            return
        per_row = STAGE_SIZE[stage] // halves
        lax.fori_loop(first * per_row, last * per_row, combo, 0)

    def force_stage(stage, k, first=0, last=2):
        groups = NACT[k] // 8
        per = min(groups, 2)
        sets = groups // per
        halves = 2 if per == 1 else 1
        base = STAGE_BASE[stage]

        def pairs(c, h, g, edge=False):
            row, r, b = (2, 4, 0) if edge else stage_ids(stage, c)
            xi, yi, zi, vxi, vyi, vzi, qi, ci, ri = (
                own(3 if edge else row, comp, h, g, per) for comp in (X, Y, Z, VX, VY, VZ, Q, C, R)
            )
            slot = EDGE_SLOT if edge else (base + c) * 2 + h
            ax, ay, az = (acc[d, row, 1 + h, pl.ds(g * 8, per * 8), :].reshape(per, 8, LN) for d in range(3))
            for j in range(S):
                dx = xi - other(r, X, b, h, j)
                dy = yi - other(r, Y, b, h, j)
                dz = zi - other(r, Z, b, h, j)
                n = (
                    dx * (vxi - other(r, VX, b, h, j))
                    + dy * (vyi - other(r, VY, b, h, j))
                    + dz * (vzi - other(r, VZ, b, h, j))
                )
                mu = jnp.minimum(n, 0.0) * cache_a[slot * S + j, pl.ds(g, per)]
                sound = ci + other(r, C, b, h, j)
                visc = (mu * (mu - sound)) / (ri + other(r, R, b, h, j))
                f = cache_w[slot * S + j, pl.ds(g, per)] * (qi + other(r, Q, b, h, j) + visc)
                ax, ay, az = ax + f * dx, ay + f * dy, az + f * dz
            for d, total in enumerate((ax, ay, az)):
                acc[d, row, 1 + h, pl.ds(g * 8, per * 8), :] = total.reshape(per * 8, LN)

        def combo(i, _):
            if halves == 2:
                pairs(i, 0, 0)
                pairs(i, 1, 0)
            else:
                ch, g = i // sets, (i % sets) * per
                pairs(ch // 2, ch % 2, g)
            return 0

        if k == 0 and stage < 2:
            paired_stage(stage, force_paired)
            if stage == 1:

                def edge(i, _):
                    pairs(0, 0, i * 2, edge=True)
                    return 0

                lax.fori_loop(0, 2, edge, 0)
                for d in range(3):
                    spread_edges(acc.at[d])
            return
        per_row = STAGE_SIZE[stage] * sets // halves
        lax.fori_loop(first * per_row, last * per_row, combo, 0)

    def plan():
        row_i = lax.broadcasted_iota(jnp.int32, (LN, LN), 0)
        col_i = lax.broadcasted_iota(jnp.int32, (LN, LN), 1)
        before = jnp.where(row_i < col_i, 1.0, 0.0).astype(jnp.bfloat16)
        ones = jnp.ones((LN, LN), jnp.bfloat16)
        row8 = lax.broadcasted_iota(jnp.int32, (8, LN), 0)
        dest = tgt[...]
        start = jnp.zeros((LN, LN), jnp.float32)
        place = jnp.zeros((LN, LN), jnp.float32)
        start_t = jnp.zeros((8, LN), jnp.float32)
        info = jnp.zeros((8, LN), jnp.float32)
        for d in range(subs):
            mine = dest == d
            hot = jnp.where(mine, 1.0, 0.0).astype(jnp.bfloat16)
            inside = jnp.dot(hot, before, preferred_element_type=jnp.float32)
            place = jnp.where(mine, start + inside, place)
            start = start + jnp.dot(hot, ones, preferred_element_type=jnp.float32)
            count_t = lax.dot_general(
                ones[0:8], hot, (((1,), (1,)), ((), ())), preferred_element_type=jnp.float32
            )
            info = jnp.where(row8 == d, start_t, info)
            info = jnp.where(row8 == subs + d, count_t, info)
            start_t = start_t + count_t
        pos[...] = place.astype(jnp.int32)
        tab[u] = info
        sends = []
        for k in range(1, subs):
            copy = pltpu.make_async_remote_copy(
                src_ref=tab.at[u],
                dst_ref=tab.at[u],
                send_sem=tab_send.at[k],
                recv_sem=tab_recv.at[k],
                device_id=(t, lax.rem(u + k, subs)),
                device_id_type=MESH,
            )
            copy.start()
            sends.append(copy)
        return sends

    def emit(g, own_rows):
        row_q = lax.broadcasted_iota(jnp.int32, (LN, LN), 0)
        for row in own_rows:
            for h in range(2):
                count = jnp.broadcast_to(cnt[0, pl.ds(h * 2 + row, 1), :], (8, LN))
                rows = pl.ds(g * 8, 8)
                slot = lax.broadcasted_iota(jnp.int32, (8, LN), 0) + g * 8
                in_rows = pl.ds(g * 32 + h * 2 + row, 8, stride=4)
                values = [st[d, row, h, rows, :] * 0.25 for d in range(3)]
                values += [st[3 + d, row, h, rows, :] * 0.0625 for d in range(3)]
                values += [pr[2, row, h, rows, :] * 0.25]
                values += [jnp.where(slot < count, mass[in_rows, :], 0.0)]
                for i, v in enumerate(values):
                    raw[g, pl.ds((row * 2 + h) * 64 + i, 8, stride=8), :] = v

        def sort(rh, _):
            row, h = rh // 2, rh % 2
            for i in range(8):
                slot = g * 8 + i
                line = pos[pl.ds(slot * 4 + h * 2 + row, 1), :]
                hot = jnp.where(row_q == jnp.broadcast_to(line, (LN, LN)), 1.0, 0.0)
                v = raw[g, pl.ds(rh * 64 + i * 8, 8), :]
                hi = v.astype(jnp.bfloat16)
                rest = v - hi.astype(jnp.float32)
                mid = rest.astype(jnp.bfloat16)
                low = (rest - mid.astype(jnp.float32)).astype(jnp.bfloat16)
                pieces = jnp.concatenate([hi, mid, low], axis=0)
                moved = lax.dot_general(
                    pieces, hot.astype(jnp.bfloat16), (((1,), (1,)), ((), ())), preferred_element_type=jnp.float32
                )
                gathered[u, slot * 2 + h, row] = (moved[0:8] + moved[8:16]) + moved[16:24]
            return 0

        lax.fori_loop(own_rows[0] * 2, own_rows[-1] * 2 + 2, sort, 0)

    PIECES = ((32, 32, (0, 1)), (16, 16, (0, 1)), (0, 16, (0,)), (0, 16, (1,)))

    def piece_copy(p, flow, owner, second_half, dst):
        first, rows, own_rows = PIECES[p]
        half = rows // 2
        part = pl.ds(first + half * second_half, half)
        which = slice(None) if len(own_rows) == 2 else own_rows[0]
        landing = done if p >= 2 and flow not in (0, 2) else gathered
        return pltpu.make_async_remote_copy(
            src_ref=gathered.at[owner, part, which],
            dst_ref=landing.at[owner, part, which],
            send_sem=piece_send.at[p, flow],
            recv_sem=piece_recv.at[p, flow],
            device_id=(t, dst),
            device_id_type=MESH,
        )

    leaving = []

    def write_out(p, at, owner, first, rows):
        own_rows = PIECES[p][2]
        which = slice(None) if len(own_rows) == 2 else own_rows[0]
        copy = pltpu.make_async_copy(
            gathered.at[owner, pl.ds(first, rows), which], done.at[owner, pl.ds(first, rows), which], done_sem.at[p, at]
        )
        copy.start()
        leaving.append(copy)

    def start_piece(p, before_rest=None):
        first, rows, own_rows = PIECES[p]
        for g in range(first // 16, (first + rows) // 16):
            emit(g, own_rows)
        copies = [
            piece_copy(p, 0, u, 0, right),
            piece_copy(p, 1, u, 1, right),
            piece_copy(p, 2, u, 1, left),
            piece_copy(p, 3, u, 0, left),
        ]
        arriving[p] = copies
        copies[0].start()
        copies[2].start()
        if before_rest is not None:
            before_rest()
        copies[1].start()
        copies[3].start()
        if p >= 2:
            write_out(p, 0, u, first, rows)

    def forward_piece(p):
        arriving[p][0].wait_recv()
        arriving[p][2].wait_recv()
        copies = [piece_copy(p, 4, left, 0, right), piece_copy(p, 5, right, 1, left)]
        for copy in copies:
            copy.start()
        arriving[p] += copies
        if p >= 2:
            first, rows, _ = PIECES[p]
            write_out(p, 1, left, first, rows // 2)
            write_out(p, 2, right, first + rows // 2, rows // 2)

    def finish_piece(p):
        for f in (1, 3, 4, 5):
            arriving[p][f].wait_recv()
        for copy in arriving[p]:
            copy.wait_send()
        if p < 2:
            write_out(p, 0, slice(None), PIECES[p][0], PIECES[p][1])

    def exchange_and_sum(rnd, src, inbox, comps, n, stage_fn, k, meanwhile, row_done=None):
        copies = start_round(rnd, src, len(comps), n, inbox)
        meanwhile()
        loads = [None] * 4
        for r in (1, 2):
            loads[r] = functools.partial(lambda row, c, h, rows: src[c, row, h, rows, :], r - 1)
        loads[0] = lambda c, h, rows: inbox[rnd // 2, 0, c, h, rows, :]
        loads[3] = lambda c, h, rows: inbox[rnd // 2, 1, c, h, rows, :]
        for r in (1, 2):
            centre(loads[r], comps, r, n)
        stage_fn(0, k)
        copies[4].wait_recv()
        copies[5].wait_recv()
        for r in (1, 2):
            sides(loads[r], comps, r, n, rnd, 1, r - 1)
        if k == 0:
            edges(comps)
        stage_fn(1, k, 0, 2 if row_done is None else 1)
        for f in (0, 1, 2, 3, 6, 7):
            copies[f].wait_recv()
        for r, dt, sender_row in ((0, 0, 1), (3, 2, 0)):
            centre(loads[r], comps, r, n)
            sides(loads[r], comps, r, n, rnd, dt, sender_row)
        if row_done is None:
            stage_fn(2, k)
            return copies
        for copy in copies:
            copy.wait_send()
        stage_fn(2, k, 0, 1)
        row_done(0)
        stage_fn(1, k, 1, 2)
        row_done(1)
        stage_fn(2, k, 1, 2)
        row_done(2)
        return []

    arriving = {}

    def lay_plan():
        for copy in arriving["tab"]:
            copy.wait_recv()
        row_i = lax.broadcasted_iota(jnp.int32, (LN, LN), 0)
        col_i = lax.broadcasted_iota(jnp.int32, (LN, LN), 1)

        def order(i):
            return (i // 4) * 4 + (i % 2) * 2 + (i // 2) % 2

        earlier = jnp.where(order(row_i) < order(col_i), 1.0, 0.0).astype(jnp.bfloat16)
        starts = jnp.concatenate([tab[src, pl.ds(u, 1), :] for src in range(subs)], axis=0)
        counts = jnp.concatenate([tab[src, pl.ds(subs + u, 1), :] for src in range(subs)], axis=0)
        padded = jnp.concatenate([counts, jnp.zeros_like(counts)], axis=0).astype(jnp.bfloat16)
        base = jnp.dot(padded, earlier, preferred_element_type=jnp.float32)[0:subs]
        base = base.astype(jnp.int32)
        skip = base & (LN - 1)
        turn = (skip - starts.astype(jnp.int32)) & (LN - 1)
        end = skip + counts.astype(jnp.int32)
        runs[0:subs, :] = turn + skip * 128 + end * 16384 + (base >> 7) * 4194304
        runs[subs : 2 * subs, :] = jnp.zeros((subs, LN), jnp.int32)

    def during(rnd):
        if rnd == 0:
            arriving["tab"] = plan()
        elif rnd == 1:
            lay_plan()
        elif rnd in (2, 4):
            if rnd == 4:
                finish_piece(0)
            start_piece(rnd // 2 - 1)
        elif rnd in (3, 5):
            forward_piece(rnd // 2 - 1)

    def move(k, row):
        for h in range(2):
            count = jnp.broadcast_to(cnt[k, pl.ds(h * 2 + row, 1), :], (8, LN))
            for g in range(NACT[k] // 8):
                rows = pl.ds(g * 8, 8)
                slot = lax.broadcasted_iota(jnp.int32, (8, LN), 0) + g * 8
                active = slot < count
                for d in range(3):
                    v = st[3 + d, row, h, rows, :]
                    x = st[d, row, h, rows, :]
                    v_new = v + 4.0 * acc[d, row, 1 + h, rows, :]
                    st[3 + d, row, h, rows, :] = jnp.where(active, v_new, v)
                    st[d, row, h, rows, :] = jnp.where(active, x + 0.0125 * v_new, x)

    def last_rows(step):
        if step == 0:
            move(2, 0)
            start_piece(2)
        elif step == 2:
            finish_piece(1)
            move(2, 1)
            start_piece(3, lambda: forward_piece(2))
            forward_piece(3)

    for k in range(3):
        n = NACT[k]
        dens[...] = jnp.zeros_like(dens)
        comps = (X, Y, Z, VX, VY, VZ) + ((MS,) if k == 0 else ())
        moved = exchange_and_sum(2 * k, st, xin, comps, NMOVED[k], density_stage, k, lambda: during(2 * k))
        for row in range(2):
            for h in range(2):
                count = jnp.broadcast_to(cnt[k, pl.ds(h * 2 + row, 1), :], (8, LN))
                for g in range(n // 8):
                    rows = pl.ds(g * 8, 8)
                    slot = lax.broadcasted_iota(jnp.int32, (8, LN), 0) + g * 8
                    rho4 = jnp.where(slot < count, dens[row, 1 + h, rows, :], pr[2, row, h, rows, :])
                    root = jnp.exp(jnp.log(rho4 * 0.25) * (1.0 / 3.0))
                    pr[0, row, h, rows, :] = sq[0, row, h, rows, :] / root
                    pr[1, row, h, rows, :] = sq[1, row, h, rows, :] * root
                    pr[2, row, h, rows, :] = rho4
        acc[...] = jnp.zeros_like(acc)
        if k == 2:
            for copy in moved:
                copy.wait_send()
        pressed = exchange_and_sum(
            2 * k + 1, pr, pin, (Q, C, R), n, force_stage, k, lambda: during(2 * k + 1), last_rows if k == 2 else None
        )
        if k < 2:
            for copy in moved + pressed:
                copy.wait_send()
            for row in range(2):
                move(k, row)
    for copy in arriving["tab"]:
        copy.wait_send()
    for p in (2, 3):
        finish_piece(p)
    for copy in leaving:
        copy.wait()


TILES = 48


STEPS = 4


def lay_kernel(runs, gathered, out, tiles, edge):
    subs = gathered.shape[0]
    lane = lane_iota()
    beyond = lane + LN
    step = pl.program_id(0)

    @pl.when(step == 0)
    def _():
        tiles[...] = jnp.zeros_like(tiles)
        edge[...] = jnp.zeros_like(edge)

    def lay(slot, currents):
        for row in range(2):
            for h in range(2):
                at = (step * (S // STEPS) + slot) * 4 + h * 2 + row
                later = []
                for src in range(subs):
                    word = runs[src, at]
                    words = jnp.full((8, LN), word)
                    end = (words >> 14) & 255
                    turned = pltpu.roll(gathered[src, slot * 2 + h, row], word & (LN - 1), 1)
                    kept = jnp.where(lane < end, turned, 0.0)
                    merged = jnp.where(lane < ((words >> 7) & (LN - 1)), currents[src], kept)
                    tiles[src, word >> 22] = merged
                    wrapped = jnp.where(beyond < end, turned, 0.0)
                    later.append(jnp.where(end >= LN, wrapped, merged))
                currents = later
        return tuple(currents)

    currents = lax.fori_loop(0, S // STEPS, lay, tuple(edge[src] for src in range(subs)))
    for src in range(subs):
        edge[src] = currents[src]

    @pl.when(step == STEPS - 1)
    def _():
        for src in range(subs):
            word = runs[src, LN - 1]
            tiles[src, (word >> 22) + jnp.where((word >> 14) & 255 >= LN, 1, 0)] = currents[src]
        for src in range(subs):
            out[pl.ds(src * TILES, TILES)] = tiles[src, pl.ds(0, TILES)]


def rows_of(a):
    lead = a.shape[:-2]
    a = a.reshape(lead + (2, 2, LN))
    a = jnp.swapaxes(a, -3, -2)
    return a


def shards(tiles, subs, offsets, velocity, mass, entropy, active_counts, targets):
    off = rows_of(offsets).reshape(3, LN, LN)
    vel = rows_of(velocity).reshape(3, LN, LN)
    mas = rows_of(mass).reshape(LN, LN)
    ent = rows_of(entropy).reshape(LN, LN)
    cnt = rows_of(active_counts).reshape(3, 4, LN)
    tgt = rows_of(targets).reshape(LN, LN)
    vmem = pl.BlockSpec(memory_space=pltpu.VMEM)
    f32 = jnp.float32
    gathered, runs = pl.pallas_call(
        functools.partial(substeps_kernel, tiles, subs),
        out_shape=[
            jax.ShapeDtypeStruct((subs, LN // 2, 2, 8, LN), f32),
            jax.ShapeDtypeStruct((2 * subs, LN), jnp.int32),
        ],
        in_specs=[vmem] * 6,
        out_specs=[pl.BlockSpec(memory_space=pl.ANY), vmem],
        scratch_shapes=[
            pltpu.VMEM((subs, LN // 2, 2, 8, LN), f32),
            pltpu.VMEM((5 * NF * 6, S, LN), f32),
            pltpu.VMEM((7, 2, 2, S, LN), f32),
            pltpu.VMEM((3, 2, 2, S, LN), f32),
            pltpu.VMEM((3, 4, S, LN), f32),
            pltpu.VMEM((3, 3, 4, S, LN), f32),
            pltpu.VMEM((2, 2, 2, S, LN), f32),
            pltpu.VMEM((6, 2, S, LN), f32),
            pltpu.VMEM((3, 2, 7, 2, S, LN), f32),
            pltpu.VMEM((3, 2, 3, 2, S, LN), f32),
            pltpu.VMEM((6, 3, 2, S, LN), f32),
            pltpu.VMEM((18 * 2 * S, 4, 8, LN), f32),
            pltpu.VMEM((18 * 2 * S, 4, 8, LN), f32),
            pltpu.VMEM((4, 256, LN), f32),
            pltpu.VMEM((3, 256, LN), f32),
            pltpu.VMEM((LN, LN), jnp.int32),
            pltpu.VMEM((subs, 2 * subs, LN), f32),
            pltpu.SemaphoreType.DMA((2, 8)),
            pltpu.SemaphoreType.DMA((2, 8)),
            pltpu.SemaphoreType.DMA((4,)),
            pltpu.SemaphoreType.DMA((4,)),
            pltpu.SemaphoreType.DMA((4, 6)),
            pltpu.SemaphoreType.DMA((4, 6)),
            pltpu.SemaphoreType.DMA((4, 3)),
        ],
        compiler_params=pltpu.CompilerParams(collective_id=0, has_side_effects=True, vmem_limit_bytes=62 * 1024 * 1024),
        name="substeps",
    )(off, vel, mas, ent, cnt, tgt)
    arrived = pl.pallas_call(
        lay_kernel,
        grid=(STEPS,),
        out_shape=jax.ShapeDtypeStruct((subs * TILES, 8, LN), f32),
        in_specs=[
            pl.BlockSpec(memory_space=pltpu.SMEM),
            pl.BlockSpec((subs, LN // 2 // STEPS, 2, 8, LN), lambda i: (0, i, 0, 0, 0)),
        ],
        out_specs=pl.BlockSpec((subs * TILES, 8, LN), lambda i: (0, 0, 0)),
        scratch_shapes=[pltpu.VMEM((subs, TILES + 2, 8, LN), f32), pltpu.VMEM((subs, 8, LN), f32)],
        name="lay",
    )(runs, gathered)
    return jnp.transpose(arrived, (1, 0, 2)).reshape(8, subs * TILES * LN)


def solution(mesh):
    tiles, subs = mesh.shape["tile"], mesh.shape["sub"]
    placed = (
        P(None, None, "tile", "sub"),
        P(None, None, "tile", "sub"),
        P(None, "tile", "sub"),
        P(None, "tile", "sub"),
        P(None, "tile", "sub"),
        P(None, "tile", "sub"),
    )
    return jax.shard_map(
        functools.partial(shards, tiles, subs),
        mesh=mesh,
        in_specs=placed,
        out_specs=P(None, ("tile", "sub")),
        check_vma=False,
    )
```

```python
import functools
import math

import jax
import jax.numpy as jnp
from jax import lax
from jax.experimental import pallas as pl
from jax.experimental.pallas import tpu as pltpu
from jax.sharding import PartitionSpec as P

MESH = pl.DeviceIdType.MESH

S = 32
LN = 128
KERNEL_NORM = 21.0 / (2.0 * math.pi)
NACT = (32, 16, 8)
NMOVED = (32, 32, 16)

X, Y, Z, VX, VY, VZ, MS, Q, C, R = range(10)
NF = 10


def field(row, comp, b, h):
    return ((row * NF + comp) * 3 + b) * 2 + h


def lane_iota():
    return lax.broadcasted_iota(jnp.int32, (8, LN), 1)


def stage_ids(stage, c):
    if stage == 0:
        return c // 2, 1 + c % 2, 1
    if stage == 1:
        return c // 4, 1 + (c // 2) % 2, 2 * (c % 2)
    return c // 3, 3 * (c // 3), c % 3


STAGE_SIZE = (4, 8, 6)
STAGE_BASE = (0, 4, 12)


def substeps_kernel(
    tiles, subs, off_in, vel_in, mass_in, ent_in, cnt_in, tgt_in, done, runs_out, gathered, off, vel, mass, ent, cnt,
    tgt, runs, fld, st, pr, dens, acc, sq, ysend, xin, pin, yin,
    cache_w, cache_a, raw, back, pos, tab, send_sem, recv_sem, tab_send, tab_recv, piece_send, piece_recv, done_sem, in_sem, runs_sem
):
    t, u = lax.axis_index("tile"), lax.axis_index("sub")
    up, down = lax.rem(t + 1, tiles), lax.rem(t + tiles - 1, tiles)
    right, left = lax.rem(u + 1, subs), lax.rem(u + subs - 1, subs)
    tile_of = (down, t, up)

    barrier = pltpu.get_barrier_semaphore()
    across = lax.rem(u + 2, subs)
    near = ((down, u), (up, u), (down, left), (t, left), (up, left), (down, right), (t, right), (up, right))
    for dev in near + ((t, across),):
        pl.semaphore_signal(barrier, inc=1, device_id=dev, device_id_type=MESH)

    inputs = [
        pltpu.make_async_copy(src, dst, in_sem.at[i])
        for i, (src, dst) in enumerate(
            ((cnt_in, cnt), (off_in, off), (vel_in, vel), (mass_in, mass), (ent_in, ent), (tgt_in, tgt))
        )
    ]
    for copy in inputs:
        copy.start()
    for copy in inputs:
        copy.wait()

    for row in range(2):
        for h in range(2):
            count = jnp.broadcast_to(cnt[0, pl.ds(h * 2 + row, 1), :], (8, LN))
            for g in range(4):
                rows = pl.ds(g * 32 + h * 2 + row, 8, stride=4)
                dst = (row, h, pl.ds(g * 8, 8))
                for c in range(3):
                    st[(c,) + dst] = off[c, rows, :] * 4.0
                    st[(3 + c,) + dst] = vel[c, rows, :] * 16.0
                slot = lax.broadcasted_iota(jnp.int32, (8, LN), 0) + g * 8
                st[(6,) + dst] = jnp.where(slot < count, mass[rows, :] * (KERNEL_NORM / 64.0), 0.0)
                e = ent[rows, :]
                sq[(0,) + dst] = e
                sq[(1,) + dst] = jnp.sqrt(e * (5.0 / 3.0))
                pr[(2,) + dst] = jnp.full((8, LN), 4.0, jnp.float32)
    pl.semaphore_wait(barrier, 9)

    lane = lane_iota()

    def start_round(rnd, src, ncomp, n, inbox):
        for side in range(2):
            for g in range(n // 8):
                packed = jnp.zeros((8, LN), jnp.float32)
                for c in range(ncomp):
                    for row in range(2):
                        code = c * 2 + row
                        v = src[c, row, side, pl.ds(g * 8, 8), :]
                        from_lane = 127 if side == 1 else 0
                        v = pltpu.roll(v, (code - from_lane) % LN, 1)
                        packed = jnp.where(lane == code, v, packed)
                ysend[rnd, side, pl.ds(g * 8, 8), :] = packed
        copies = []
        for row, dst_t, slot in ((0, down, 1), (1, up, 0)):
            f = row
            copies.append(
                pltpu.make_async_remote_copy(
                    src_ref=src.at[pl.ds(0, ncomp), row, :, pl.ds(0, n)],
                    dst_ref=inbox.at[rnd // 2, slot, pl.ds(0, ncomp), :, pl.ds(0, n)],
                    send_sem=send_sem.at[rnd % 2, f],
                    recv_sem=recv_sem.at[rnd % 2, f],
                    device_id=(dst_t, u),
                    device_id_type=MESH,
                )
            )
        for dt in range(3):
            for side in range(2):
                f = 2 + dt * 2 + side
                copies.append(
                    pltpu.make_async_remote_copy(
                        src_ref=ysend.at[rnd, side, pl.ds(0, n)],
                        dst_ref=yin.at[rnd, 2 - dt, 1 - side, pl.ds(0, n)],
                        send_sem=send_sem.at[rnd % 2, f],
                        recv_sem=recv_sem.at[rnd % 2, f],
                        device_id=(tile_of[dt], right if side == 1 else left),
                        device_id_type=MESH,
                    )
                )
        for f in (4, 5, 0, 1, 2, 3, 6, 7):
            copies[f].start()
        return copies

    def shift_of(comp, r):
        return 4.0 * (r - 1) if comp == X else 0.0

    def centre(load, comps, r, n):
        for c, comp in enumerate(comps):
            for h in range(2):
                v = load(c, h, pl.ds(0, n))
                if comp == X and r != 1:
                    v = v + 4.0 * (r - 1)
                fld[field(r, comp, 1, h), pl.ds(0, n), :] = v

    def sides(load, comps, r, n, rnd, dt, sender_row):
        for c, comp in enumerate(comps):
            code = c * 2 + sender_row
            dx = 4.0 * (r - 1) if comp == X else 0.0
            for g in range(n // 8):
                rows = pl.ds(g * 8, 8)
                a0, a1 = load(c, 0, rows), load(c, 1, rows)
                lo = pltpu.roll(yin[rnd, dt, 0, rows, :], (0 - code) % LN, 1)
                hi = pltpu.roll(yin[rnd, dt, 1, rows, :], (127 - code) % LN, 1)
                r0, r1 = pltpu.roll(a0, 1, 1), pltpu.roll(a1, 1, 1)
                l0, l1 = pltpu.roll(a0, 127, 1), pltpu.roll(a1, 127, 1)
                first, last = lane == 0, lane == 127
                minus = [jnp.where(first, lo, r0), jnp.where(first, r0, r1)]
                plus = [jnp.where(last, l1, l0), jnp.where(last, hi, l1)]
                for h in range(2):
                    m, p = minus[h], plus[h]
                    if comp == Y:
                        m, p = m - 4.0, p + 4.0
                    elif comp == X and r != 1:
                        m, p = m + dx, p + dx
                    fld[field(r, comp, 0, h), rows, :] = m
                    fld[field(r, comp, 2, h), rows, :] = p

    def other(r, comp, b, h, j):
        return fld[field(r, comp, b, h), pl.ds(j, 8, stride=0), :]

    def own(row, comp, h, g, n):
        return fld[field(row + 1, comp, 1, h), pl.ds(g * 8, n * 8), :].reshape(n, 8, LN)

    EDGE_SLOT = 14

    def edges(comps):
        for comp in comps:
            for g in range(4):
                rows = pl.ds(g * 8, 8)

                def packed(zero, one, two, three):
                    v = fld[zero, rows, :]
                    v = jnp.where(lane == 1, pltpu.roll(fld[one, rows, :], 1, 1), v)
                    v = jnp.where(lane == 2, pltpu.roll(fld[two, rows, :], 2, 1), v)
                    return jnp.where(lane == 3, pltpu.roll(fld[three, rows, :], 4, 1), v)

                low0, low1 = field(1, comp, 1, 0), field(2, comp, 1, 0)
                fld[field(4, comp, 1, 0), rows, :] = packed(low0, low1, low1, field(2, comp, 1, 1))
                low0, low1 = field(1, comp, 0, 0), field(2, comp, 0, 0)
                fld[field(4, comp, 0, 0), rows, :] = packed(low0, low1, low0, field(1, comp, 2, 1))

    def spread_edges(sums):
        for g in range(4):
            rows = pl.ds(g * 8, 8)
            v = sums[2, 1, rows, :]
            one_two = pltpu.roll(v, 127, 1) + pltpu.roll(v, 126, 1)
            sums[0, 1, rows, :] += jnp.where(lane == 0, v, 0.0)
            sums[1, 1, rows, :] += jnp.where(lane == 0, one_two, 0.0)
            sums[1, 2, rows, :] += jnp.where(lane == 127, pltpu.roll(v, 124, 1), 0.0)

    def paired_stage(stage, body):
        if stage == 0:

            def alone(i, _):
                body(i // 2, 1 + i // 2, 1, i % 2, i, True)
                return 0

            def straight(h, _):
                body(0, 2, 1, h, 4 + h, False)
                return 0

            lax.fori_loop(0, 4, alone, 0)
            lax.fori_loop(0, 2, straight, 0)
        else:

            def slanted(ih, _):
                i, h = ih // 2, ih % 2
                body(i // 3, 1 + (i + 2) // 3, 2 - 2 * (i // 2 - i // 3), h, 6 + ih, False, True)
                return 0

            lax.fori_loop(0, 8, slanted, 0)

    def give_back(sums, which, r, b, h, alone, shifted, sign):
        for jg in range(2 if alone else 0, 4):
            rows = pl.ds(jg * 8, 8)
            part = back[which, pl.ds(jg * 64, 8, stride=8), :]
            for sub in range(1, 8):
                part = part + back[which, pl.ds(jg * 64 + sub, 8, stride=8), :]
            part = part * sign if sign != 1.0 else part
            if not shifted:
                sums[r - 1, 1 + h, rows, :] += part
            else:
                part = pltpu.roll(part, (b + (LN - 1)) % LN, 1)
                over = lane == (LN - 1) * (1 - b // 2)
                sums[r - 1, 1 + h, rows, :] += jnp.where(over, 0.0, part)
                sums[r - 1, h + b, rows, :] += jnp.where(over, part, 0.0)

    def density_paired(row, r, b, h, slot, alone, shifted=False):
        mine = [[own(row, comp, h, g, 2) for comp in (X, Y, Z, MS)] for g in (0, 2)]
        totals = [dens[row, 1 + h, pl.ds(g * 8, 16), :].reshape(2, 8, LN) for g in (0, 2)]
        for j in range(S):
            given = None
            mj = other(r, MS, b, h, j)
            for g in (0,) if alone and j < 16 else (0, 1):
                xi, yi, zi, mi = mine[g]
                dx = xi - other(r, X, b, h, j)
                dy = yi - other(r, Y, b, h, j)
                dz = zi - other(r, Z, b, h, j)
                r2 = dx * dx + dy * dy + dz * dz
                rad = r2 * lax.rsqrt(jnp.maximum(r2, 1e-30))
                s = jnp.maximum(4.0 - rad, 0.0)
                s3 = s * (s * s)
                w = s3 * (s * (5.0 - s))
                totals[g] = totals[g] + w * mj
                cache_w[slot * S + j, pl.ds(g * 2, 2)] = s3
                cache_a[slot * S + j, pl.ds(g * 2, 2)] = 1.0 / (r2 + 0.16)
                if not alone or (g == 0 and j >= 16):
                    wi = w * mi
                    wi = wi[0] + wi[1]
                    given = wi if given is None else given + wi
            if given is not None:
                back[0, pl.ds(j * 8, 8), :] = given
        for g in (0, 1):
            dens[row, 1 + h, pl.ds(g * 16, 16), :] = totals[g].reshape(16, LN)
        give_back(dens, 0, r, b, h, alone, shifted, 1.0)

    def force_paired(row, r, b, h, slot, alone, shifted=False):
        def half(g, first, backward):
            xi, yi, zi, vxi, vyi, vzi, qi, ci, ri, mi = (
                own(row, comp, h, g, 2) for comp in (X, Y, Z, VX, VY, VZ, Q, C, R, MS)
            )
            ax, ay, az = (acc[d, row, 1 + h, pl.ds(g * 8, 16), :].reshape(2, 8, LN) for d in range(3))
            for j in range(first, S):
                dx = xi - other(r, X, b, h, j)
                dy = yi - other(r, Y, b, h, j)
                dz = zi - other(r, Z, b, h, j)
                n = (
                    dx * (vxi - other(r, VX, b, h, j))
                    + dy * (vyi - other(r, VY, b, h, j))
                    + dz * (vzi - other(r, VZ, b, h, j))
                )
                mu = jnp.minimum(n, 0.0) * cache_a[slot * S + j, pl.ds(g, 2)]
                visc = (mu * (mu - (ci + other(r, C, b, h, j)))) / (ri + other(r, R, b, h, j))
                f = cache_w[slot * S + j, pl.ds(g, 2)] * (qi + other(r, Q, b, h, j) + visc)
                fi = f * other(r, MS, b, h, j)
                ax, ay, az = ax + fi * dx, ay + fi * dy, az + fi * dz
                if j >= backward:
                    fj = f * mi
                    for d, delta in enumerate((dx, dy, dz)):
                        back_d = fj * delta
                        back[d, pl.ds(j * 8, 8), :] = back_d[0] + back_d[1]
            for d, total in enumerate((ax, ay, az)):
                acc[d, row, 1 + h, pl.ds(g * 8, 16), :] = total.reshape(16, LN)
            if backward < S:
                for d in range(3):
                    give_back(acc.at[d], d, r, b, h, alone, shifted, -1.0)

        if alone:
            half(0, 0, 16)
            half(2, 16, S)
        else:

            def part(i, _):
                half(i * 2, 0, 0)
                return 0

            lax.fori_loop(0, 2, part, 0)

    def density_stage(stage, k, first=0, last=2):
        per = NACT[k] // 8
        halves = 2 if per == 1 else 1
        base = STAGE_BASE[stage]

        def pairs(c, h, edge=False):
            row, r, b = (2, 4, 0) if edge else stage_ids(stage, c)
            xi, yi, zi = (own(3 if edge else row, comp, h, 0, per) for comp in (X, Y, Z))
            slot = EDGE_SLOT if edge else (base + c) * 2 + h
            total = dens[row, 1 + h, pl.ds(0, per * 8), :].reshape(per, 8, LN)
            for j in range(S):
                dx = xi - other(r, X, b, h, j)
                dy = yi - other(r, Y, b, h, j)
                dz = zi - other(r, Z, b, h, j)
                r2 = dx * dx + dy * dy + dz * dz
                rad = r2 * lax.rsqrt(jnp.maximum(r2, 1e-30))
                s = jnp.maximum(4.0 - rad, 0.0)
                w3 = (s * other(r, MS, b, h, j)) * (s * s)
                total = total + w3 * (s * (5.0 - s))
                cache_w[slot * S + j, pl.ds(0, per)] = w3
                cache_a[slot * S + j, pl.ds(0, per)] = 1.0 / (r2 + 0.16)
            dens[row, 1 + h, pl.ds(0, per * 8), :] = total.reshape(per * 8, LN)

        def combo(i, _):
            if halves == 2:
                pairs(i, 0)
                pairs(i, 1)
            else:
                pairs(i // 2, i % 2)
            return 0

        if k == 0 and stage < 2:
            paired_stage(stage, density_paired)
            if stage == 1:
                pairs(0, 0, edge=True)
                spread_edges(dens)
            return
        per_row = STAGE_SIZE[stage] // halves
        lax.fori_loop(first * per_row, last * per_row, combo, 0)

    def force_stage(stage, k, first=0, last=2):
        groups = NACT[k] // 8
        per = min(groups, 2)
        sets = groups // per
        halves = 2 if per == 1 else 1
        base = STAGE_BASE[stage]

        def pairs(c, h, g, edge=False):
            row, r, b = (2, 4, 0) if edge else stage_ids(stage, c)
            xi, yi, zi, vxi, vyi, vzi, qi, ci, ri = (
                own(3 if edge else row, comp, h, g, per) for comp in (X, Y, Z, VX, VY, VZ, Q, C, R)
            )
            slot = EDGE_SLOT if edge else (base + c) * 2 + h
            ax, ay, az = (acc[d, row, 1 + h, pl.ds(g * 8, per * 8), :].reshape(per, 8, LN) for d in range(3))
            for j in range(S):
                dx = xi - other(r, X, b, h, j)
                dy = yi - other(r, Y, b, h, j)
                dz = zi - other(r, Z, b, h, j)
                n = (
                    dx * (vxi - other(r, VX, b, h, j))
                    + dy * (vyi - other(r, VY, b, h, j))
                    + dz * (vzi - other(r, VZ, b, h, j))
                )
                mu = jnp.minimum(n, 0.0) * cache_a[slot * S + j, pl.ds(g, per)]
                sound = ci + other(r, C, b, h, j)
                visc = (mu * (mu - sound)) / (ri + other(r, R, b, h, j))
                f = cache_w[slot * S + j, pl.ds(g, per)] * (qi + other(r, Q, b, h, j) + visc)
                ax, ay, az = ax + f * dx, ay + f * dy, az + f * dz
            for d, total in enumerate((ax, ay, az)):
                acc[d, row, 1 + h, pl.ds(g * 8, per * 8), :] = total.reshape(per * 8, LN)

        def combo(i, _):
            if halves == 2:
                pairs(i, 0, 0)
                pairs(i, 1, 0)
            else:
                ch, g = i // sets, (i % sets) * per
                pairs(ch // 2, ch % 2, g)
            return 0

        if k == 0 and stage < 2:
            paired_stage(stage, force_paired)
            if stage == 1:

                def edge(i, _):
                    pairs(0, 0, i * 2, edge=True)
                    return 0

                lax.fori_loop(0, 2, edge, 0)
                for d in range(3):
                    spread_edges(acc.at[d])
            return
        per_row = STAGE_SIZE[stage] * sets // halves
        lax.fori_loop(first * per_row, last * per_row, combo, 0)

    def plan():
        row_i = lax.broadcasted_iota(jnp.int32, (LN, LN), 0)
        col_i = lax.broadcasted_iota(jnp.int32, (LN, LN), 1)
        before = jnp.where(row_i < col_i, 1.0, 0.0).astype(jnp.bfloat16)
        ones = jnp.ones((LN, LN), jnp.bfloat16)
        row8 = lax.broadcasted_iota(jnp.int32, (8, LN), 0)
        dest = tgt[...]
        start = jnp.zeros((LN, LN), jnp.float32)
        place = jnp.zeros((LN, LN), jnp.float32)
        start_t = jnp.zeros((8, LN), jnp.float32)
        info = jnp.zeros((8, LN), jnp.float32)
        for d in range(subs):
            mine = dest == d
            hot = jnp.where(mine, 1.0, 0.0).astype(jnp.bfloat16)
            inside = jnp.dot(hot, before, preferred_element_type=jnp.float32)
            place = jnp.where(mine, start + inside, place)
            start = start + jnp.dot(hot, ones, preferred_element_type=jnp.float32)
            count_t = lax.dot_general(
                ones[0:8], hot, (((1,), (1,)), ((), ())), preferred_element_type=jnp.float32
            )
            info = jnp.where(row8 == d, start_t, info)
            info = jnp.where(row8 == subs + d, count_t, info)
            start_t = start_t + count_t
        pos[...] = place.astype(jnp.int32)
        tab[u] = info
        sends = []
        for k in range(1, subs):
            copy = pltpu.make_async_remote_copy(
                src_ref=tab.at[u],
                dst_ref=tab.at[u],
                send_sem=tab_send.at[k],
                recv_sem=tab_recv.at[k],
                device_id=(t, lax.rem(u + k, subs)),
                device_id_type=MESH,
            )
            copy.start()
            sends.append(copy)
        return sends

    def emit(g, own_rows):
        row_q = lax.broadcasted_iota(jnp.int32, (LN, LN), 0)
        for row in own_rows:
            for h in range(2):
                count = jnp.broadcast_to(cnt[0, pl.ds(h * 2 + row, 1), :], (8, LN))
                rows = pl.ds(g * 8, 8)
                slot = lax.broadcasted_iota(jnp.int32, (8, LN), 0) + g * 8
                in_rows = pl.ds(g * 32 + h * 2 + row, 8, stride=4)
                values = [st[d, row, h, rows, :] * 0.25 for d in range(3)]
                values += [st[3 + d, row, h, rows, :] * 0.0625 for d in range(3)]
                values += [pr[2, row, h, rows, :] * 0.25]
                values += [jnp.where(slot < count, mass[in_rows, :], 0.0)]
                for i, v in enumerate(values):
                    raw[g, pl.ds((row * 2 + h) * 64 + i, 8, stride=8), :] = v

        def sort(rh, _):
            row, h = rh // 2, rh % 2
            for i in range(8):
                slot = g * 8 + i
                line = pos[pl.ds(slot * 4 + h * 2 + row, 1), :]
                hot = jnp.where(row_q == jnp.broadcast_to(line, (LN, LN)), 1.0, 0.0)
                v = raw[g, pl.ds(rh * 64 + i * 8, 8), :]
                hi = v.astype(jnp.bfloat16)
                rest = v - hi.astype(jnp.float32)
                mid = rest.astype(jnp.bfloat16)
                low = (rest - mid.astype(jnp.float32)).astype(jnp.bfloat16)
                pieces = jnp.concatenate([hi, mid, low], axis=0)
                moved = lax.dot_general(
                    pieces, hot.astype(jnp.bfloat16), (((1,), (1,)), ((), ())), preferred_element_type=jnp.float32
                )
                gathered[u, slot * 2 + h, row] = (moved[0:8] + moved[8:16]) + moved[16:24]
            return 0

        lax.fori_loop(own_rows[0] * 2, own_rows[-1] * 2 + 2, sort, 0)

    PIECES = ((32, 32, (0, 1)), (16, 16, (0, 1)), (0, 16, (0,)), (0, 16, (1,)))

    def piece_copy(p, flow, owner, second_half, dst):
        first, rows, own_rows = PIECES[p]
        half = rows // 2
        part = pl.ds(first + half * second_half, half)
        which = slice(None) if len(own_rows) == 2 else own_rows[0]
        landing = done if p >= 2 and flow not in (0, 2) else gathered
        return pltpu.make_async_remote_copy(
            src_ref=gathered.at[owner, part, which],
            dst_ref=landing.at[owner, part, which],
            send_sem=piece_send.at[p, flow],
            recv_sem=piece_recv.at[p, flow],
            device_id=(t, dst),
            device_id_type=MESH,
        )

    leaving = []

    def write_out(p, at, owner, first, rows):
        own_rows = PIECES[p][2]
        which = slice(None) if len(own_rows) == 2 else own_rows[0]
        copy = pltpu.make_async_copy(
            gathered.at[owner, pl.ds(first, rows), which], done.at[owner, pl.ds(first, rows), which], done_sem.at[p, at]
        )
        copy.start()
        leaving.append(copy)

    def start_piece(p, before_rest=None):
        first, rows, own_rows = PIECES[p]
        for g in range(first // 16, (first + rows) // 16):
            emit(g, own_rows)
        copies = [
            piece_copy(p, 0, u, 0, right),
            piece_copy(p, 1, u, 1, right),
            piece_copy(p, 2, u, 1, left),
            piece_copy(p, 3, u, 0, left),
        ]
        arriving[p] = copies
        copies[0].start()
        copies[2].start()
        if before_rest is not None:
            before_rest()
        copies[1].start()
        copies[3].start()
        if p >= 2:
            write_out(p, 0, u, first, rows)

    def forward_piece(p):
        arriving[p][0].wait_recv()
        arriving[p][2].wait_recv()
        copies = [piece_copy(p, 4, left, 0, right), piece_copy(p, 5, right, 1, left)]
        for copy in copies:
            copy.start()
        arriving[p] += copies
        if p >= 2:
            first, rows, _ = PIECES[p]
            write_out(p, 1, left, first, rows // 2)
            write_out(p, 2, right, first + rows // 2, rows // 2)

    def finish_piece(p):
        for f in (1, 3, 4, 5):
            arriving[p][f].wait_recv()
        for copy in arriving[p]:
            copy.wait_send()
        if p < 2:
            write_out(p, 0, slice(None), PIECES[p][0], PIECES[p][1])

    def exchange_and_sum(rnd, src, inbox, comps, n, stage_fn, k, meanwhile, row_done=None):
        copies = start_round(rnd, src, len(comps), n, inbox)
        meanwhile()
        loads = [None] * 4
        for r in (1, 2):
            loads[r] = functools.partial(lambda row, c, h, rows: src[c, row, h, rows, :], r - 1)
        loads[0] = lambda c, h, rows: inbox[rnd // 2, 0, c, h, rows, :]
        loads[3] = lambda c, h, rows: inbox[rnd // 2, 1, c, h, rows, :]
        for r in (1, 2):
            centre(loads[r], comps, r, n)
        stage_fn(0, k)
        copies[4].wait_recv()
        copies[5].wait_recv()
        for r in (1, 2):
            sides(loads[r], comps, r, n, rnd, 1, r - 1)
        if k == 0:
            edges(comps)
        stage_fn(1, k, 0, 2 if row_done is None else 1)
        for f in (0, 1, 2, 3, 6, 7):
            copies[f].wait_recv()
        for r, dt, sender_row in ((0, 0, 1), (3, 2, 0)):
            centre(loads[r], comps, r, n)
            sides(loads[r], comps, r, n, rnd, dt, sender_row)
        if row_done is None:
            stage_fn(2, k)
            return copies
        for copy in copies:
            copy.wait_send()
        stage_fn(2, k, 0, 1)
        row_done(0)
        stage_fn(1, k, 1, 2)
        row_done(1)
        stage_fn(2, k, 1, 2)
        row_done(2)
        return []

    arriving = {}

    def lay_plan():
        for copy in arriving["tab"]:
            copy.wait_recv()
        row_i = lax.broadcasted_iota(jnp.int32, (LN, LN), 0)
        col_i = lax.broadcasted_iota(jnp.int32, (LN, LN), 1)

        def order(i):
            return (i // 4) * 4 + (i % 2) * 2 + (i // 2) % 2

        earlier = jnp.where(order(row_i) < order(col_i), 1.0, 0.0).astype(jnp.bfloat16)
        starts = jnp.concatenate([tab[src, pl.ds(u, 1), :] for src in range(subs)], axis=0)
        counts = jnp.concatenate([tab[src, pl.ds(subs + u, 1), :] for src in range(subs)], axis=0)
        padded = jnp.concatenate([counts, jnp.zeros_like(counts)], axis=0).astype(jnp.bfloat16)
        base = jnp.dot(padded, earlier, preferred_element_type=jnp.float32)[0:subs]
        base = base.astype(jnp.int32)
        skip = base & (LN - 1)
        turn = (skip - starts.astype(jnp.int32)) & (LN - 1)
        end = skip + counts.astype(jnp.int32)
        runs[0:subs, :] = turn + skip * 128 + end * 16384 + (base >> 7) * 4194304
        runs[subs : 2 * subs, :] = jnp.zeros((subs, LN), jnp.int32)
        arriving["runs"] = pltpu.make_async_copy(runs, runs_out, runs_sem)
        arriving["runs"].start()

    def during(rnd):
        if rnd == 0:
            arriving["tab"] = plan()
        elif rnd == 1:
            lay_plan()
        elif rnd in (2, 4):
            if rnd == 4:
                finish_piece(0)
            start_piece(rnd // 2 - 1)
        elif rnd in (3, 5):
            forward_piece(rnd // 2 - 1)

    def move(k, row):
        for h in range(2):
            count = jnp.broadcast_to(cnt[k, pl.ds(h * 2 + row, 1), :], (8, LN))
            for g in range(NACT[k] // 8):
                rows = pl.ds(g * 8, 8)
                slot = lax.broadcasted_iota(jnp.int32, (8, LN), 0) + g * 8
                active = slot < count
                for d in range(3):
                    v = st[3 + d, row, h, rows, :]
                    x = st[d, row, h, rows, :]
                    v_new = v + 4.0 * acc[d, row, 1 + h, rows, :]
                    st[3 + d, row, h, rows, :] = jnp.where(active, v_new, v)
                    st[d, row, h, rows, :] = jnp.where(active, x + 0.0125 * v_new, x)

    def last_rows(step):
        if step == 0:
            move(2, 0)
            start_piece(2)
        elif step == 2:
            finish_piece(1)
            move(2, 1)
            start_piece(3, lambda: forward_piece(2))
            forward_piece(3)

    for k in range(3):
        n = NACT[k]
        dens[...] = jnp.zeros_like(dens)
        comps = (X, Y, Z, VX, VY, VZ) + ((MS,) if k == 0 else ())
        moved = exchange_and_sum(2 * k, st, xin, comps, NMOVED[k], density_stage, k, lambda: during(2 * k))
        for row in range(2):
            for h in range(2):
                count = jnp.broadcast_to(cnt[k, pl.ds(h * 2 + row, 1), :], (8, LN))
                for g in range(n // 8):
                    rows = pl.ds(g * 8, 8)
                    slot = lax.broadcasted_iota(jnp.int32, (8, LN), 0) + g * 8
                    rho4 = jnp.where(slot < count, dens[row, 1 + h, rows, :], pr[2, row, h, rows, :])
                    root = jnp.exp(jnp.log(rho4 * 0.25) * (1.0 / 3.0))
                    pr[0, row, h, rows, :] = sq[0, row, h, rows, :] / root
                    pr[1, row, h, rows, :] = sq[1, row, h, rows, :] * root
                    pr[2, row, h, rows, :] = rho4
        acc[...] = jnp.zeros_like(acc)
        if k == 2:
            for copy in moved:
                copy.wait_send()
        pressed = exchange_and_sum(
            2 * k + 1, pr, pin, (Q, C, R), n, force_stage, k, lambda: during(2 * k + 1), last_rows if k == 2 else None
        )
        if k < 2:
            for copy in moved + pressed:
                copy.wait_send()
            for row in range(2):
                move(k, row)
    for copy in arriving["tab"]:
        copy.wait_send()
    for p in (2, 3):
        finish_piece(p)
    for copy in leaving:
        copy.wait()
    arriving["runs"].wait()


TILES = 48


STEPS = 4


def lay_kernel(runs, gathered_in, out, gathered, tiles, in_sem, out_sem):
    subs = gathered.shape[0]
    lane = lane_iota()
    beyond = lane + LN
    block = LN // 2 // STEPS
    inputs = [
        pltpu.make_async_copy(
            gathered_in.at[:, pl.ds(i * block, block)], gathered.at[:, pl.ds(i * block, block)], in_sem.at[i]
        )
        for i in range(STEPS)
    ]
    for copy in inputs:
        copy.start()
    tiles[...] = jnp.zeros_like(tiles)

    def lay(slot, currents):
        for row in range(2):
            for h in range(2):
                at = slot * 4 + h * 2 + row
                later = []
                for src in range(subs):
                    word = runs[src, at]
                    words = jnp.full((8, LN), word)
                    end = (words >> 14) & 255
                    turned = pltpu.roll(gathered[src, slot * 2 + h, row], word & (LN - 1), 1)
                    kept = jnp.where(lane < end, turned, 0.0)
                    merged = jnp.where(lane < ((words >> 7) & (LN - 1)), currents[src], kept)
                    tiles[src, word >> 22] = merged
                    wrapped = jnp.where(beyond < end, turned, 0.0)
                    later.append(jnp.where(end >= LN, wrapped, merged))
                currents = later
        return tuple(currents)

    currents = (jnp.zeros((8, LN), jnp.float32),) * subs
    for i in range(STEPS):
        inputs[i].wait()
        currents = lax.fori_loop(i * (S // STEPS), (i + 1) * (S // STEPS), lay, currents)
    outputs = []
    for src in range(subs):
        word = runs[src, LN - 1]
        tiles[src, (word >> 22) + jnp.where((word >> 14) & 255 >= LN, 1, 0)] = currents[src]
    for src in range(subs):
        copy = pltpu.make_async_copy(
            tiles.at[src, pl.ds(0, TILES)], out.at[pl.ds(src * TILES, TILES)], out_sem.at[src]
        )
        copy.start()
        outputs.append(copy)
    for copy in outputs:
        copy.wait()


def rows_of(a):
    lead = a.shape[:-2]
    a = a.reshape(lead + (2, 2, LN))
    a = jnp.swapaxes(a, -3, -2)
    return a


def shards(tiles, subs, offsets, velocity, mass, entropy, active_counts, targets):
    off = rows_of(offsets).reshape(3, LN, LN)
    vel = rows_of(velocity).reshape(3, LN, LN)
    mas = rows_of(mass).reshape(LN, LN)
    ent = rows_of(entropy).reshape(LN, LN)
    cnt = rows_of(active_counts).reshape(3, 4, LN)
    tgt = rows_of(targets).reshape(LN, LN)
    anywhere = pl.BlockSpec(memory_space=pl.ANY)
    f32 = jnp.float32
    gathered, runs = pl.pallas_call(
        functools.partial(substeps_kernel, tiles, subs),
        out_shape=[
            jax.ShapeDtypeStruct((subs, LN // 2, 2, 8, LN), f32),
            jax.ShapeDtypeStruct((2 * subs, LN), jnp.int32),
        ],
        in_specs=[anywhere] * 6,
        out_specs=[anywhere] * 2,
        scratch_shapes=[
            pltpu.VMEM((subs, LN // 2, 2, 8, LN), f32),
            pltpu.VMEM((3, LN, LN), f32),
            pltpu.VMEM((3, LN, LN), f32),
            pltpu.VMEM((LN, LN), f32),
            pltpu.VMEM((LN, LN), f32),
            pltpu.VMEM((3, 4, LN), jnp.int32),
            pltpu.VMEM((LN, LN), jnp.int32),
            pltpu.VMEM((2 * subs, LN), jnp.int32),
            pltpu.VMEM((5 * NF * 6, S, LN), f32),
            pltpu.VMEM((7, 2, 2, S, LN), f32),
            pltpu.VMEM((3, 2, 2, S, LN), f32),
            pltpu.VMEM((3, 4, S, LN), f32),
            pltpu.VMEM((3, 3, 4, S, LN), f32),
            pltpu.VMEM((2, 2, 2, S, LN), f32),
            pltpu.VMEM((6, 2, S, LN), f32),
            pltpu.VMEM((3, 2, 7, 2, S, LN), f32),
            pltpu.VMEM((3, 2, 3, 2, S, LN), f32),
            pltpu.VMEM((6, 3, 2, S, LN), f32),
            pltpu.VMEM((18 * 2 * S, 4, 8, LN), f32),
            pltpu.VMEM((18 * 2 * S, 4, 8, LN), f32),
            pltpu.VMEM((4, 256, LN), f32),
            pltpu.VMEM((3, 256, LN), f32),
            pltpu.VMEM((LN, LN), jnp.int32),
            pltpu.VMEM((subs, 2 * subs, LN), f32),
            pltpu.SemaphoreType.DMA((2, 8)),
            pltpu.SemaphoreType.DMA((2, 8)),
            pltpu.SemaphoreType.DMA((4,)),
            pltpu.SemaphoreType.DMA((4,)),
            pltpu.SemaphoreType.DMA((4, 6)),
            pltpu.SemaphoreType.DMA((4, 6)),
            pltpu.SemaphoreType.DMA((4, 3)),
            pltpu.SemaphoreType.DMA((6,)),
            pltpu.SemaphoreType.DMA,
        ],
        compiler_params=pltpu.CompilerParams(collective_id=0, has_side_effects=True, vmem_limit_bytes=62 * 1024 * 1024),
        name="substeps",
    )(off, vel, mas, ent, cnt, tgt)
    arrived = pl.pallas_call(
        lay_kernel,
        out_shape=jax.ShapeDtypeStruct((subs * TILES, 8, LN), f32),
        in_specs=[pl.BlockSpec(memory_space=pltpu.SMEM), anywhere],
        out_specs=anywhere,
        scratch_shapes=[
            pltpu.VMEM((subs, LN // 2, 2, 8, LN), f32),
            pltpu.VMEM((subs, TILES + 2, 8, LN), f32),
            pltpu.SemaphoreType.DMA((STEPS,)),
            pltpu.SemaphoreType.DMA((subs,)),
        ],
        name="lay",
    )(runs, gathered)
    return jnp.transpose(arrived, (1, 0, 2)).reshape(8, subs * TILES * LN)


def solution(mesh):
    tiles, subs = mesh.shape["tile"], mesh.shape["sub"]
    placed = (
        P(None, None, "tile", "sub"),
        P(None, None, "tile", "sub"),
        P(None, "tile", "sub"),
        P(None, "tile", "sub"),
        P(None, "tile", "sub"),
        P(None, "tile", "sub"),
    )
    return jax.shard_map(
        functools.partial(shards, tiles, subs),
        mesh=mesh,
        in_specs=placed,
        out_specs=P(None, ("tile", "sub")),
        check_vma=False,
    )
```

```python
import functools
import math

import jax
import jax.numpy as jnp
from jax import lax
from jax.experimental import pallas as pl
from jax.experimental.pallas import tpu as pltpu
from jax.sharding import PartitionSpec as P

MESH = pl.DeviceIdType.MESH

S = 32
LN = 128
KERNEL_NORM = 21.0 / (2.0 * math.pi)
NACT = (32, 16, 8)
NMOVED = (32, 32, 16)

X, Y, Z, VX, VY, VZ, MS, Q, C, R = range(10)
NF = 10


def field(row, comp, b, h):
    return ((row * NF + comp) * 3 + b) * 2 + h


def lane_iota():
    return lax.broadcasted_iota(jnp.int32, (8, LN), 1)


def stage_ids(stage, c):
    if stage == 0:
        return c // 2, 1 + c % 2, 1
    if stage == 1:
        return c // 4, 1 + (c // 2) % 2, 2 * (c % 2)
    return c // 3, 3 * (c // 3), c % 3


STAGE_SIZE = (4, 8, 6)
STAGE_BASE = (0, 4, 12)


def substeps_kernel(
    tiles, subs, off_in, vel_in, mass_in, ent_in, cnt_in, tgt_in, done, runs_out, gathered, off, vel, mass, ent, cnt,
    tgt, runs, fld, st, pr, dens, acc, sq, ysend, xin, pin, yin,
    cache_w, cache_a, raw, back, pos, tab, send_sem, recv_sem, tab_send, tab_recv, piece_send, piece_recv, done_sem, in_sem, runs_sem
):
    t, u = lax.axis_index("tile"), lax.axis_index("sub")
    up, down = lax.rem(t + 1, tiles), lax.rem(t + tiles - 1, tiles)
    right, left = lax.rem(u + 1, subs), lax.rem(u + subs - 1, subs)
    tile_of = (down, t, up)

    barrier = pltpu.get_barrier_semaphore()
    across = lax.rem(u + 2, subs)
    near = ((down, u), (up, u), (down, left), (t, left), (up, left), (down, right), (t, right), (up, right))
    for dev in near + ((t, across),):
        pl.semaphore_signal(barrier, inc=1, device_id=dev, device_id_type=MESH)

    inputs = [
        pltpu.make_async_copy(src, dst, in_sem.at[i])
        for i, (src, dst) in enumerate(
            ((cnt_in, cnt), (off_in, off), (vel_in, vel), (mass_in, mass), (ent_in, ent), (tgt_in, tgt))
        )
    ]
    for copy in inputs:
        copy.start()
    for copy in inputs:
        copy.wait()

    for row in range(2):
        for h in range(2):
            count = jnp.broadcast_to(cnt[0, pl.ds(h * 2 + row, 1), :], (8, LN))
            for g in range(4):
                rows = pl.ds(g * 32 + h * 2 + row, 8, stride=4)
                dst = (row, h, pl.ds(g * 8, 8))
                for c in range(3):
                    st[(c,) + dst] = off[c, rows, :] * 4.0
                    st[(3 + c,) + dst] = vel[c, rows, :] * 16.0
                slot = lax.broadcasted_iota(jnp.int32, (8, LN), 0) + g * 8
                st[(6,) + dst] = jnp.where(slot < count, mass[rows, :] * (KERNEL_NORM / 64.0), 0.0)
                e = ent[rows, :]
                sq[(0,) + dst] = e
                sq[(1,) + dst] = jnp.sqrt(e * (5.0 / 3.0))
                pr[(2,) + dst] = jnp.full((8, LN), 4.0, jnp.float32)
    pl.semaphore_wait(barrier, 9)

    lane = lane_iota()

    def start_round(rnd, src, ncomp, n, inbox):
        for side in range(2):
            for g in range(n // 8):
                packed = jnp.zeros((8, LN), jnp.float32)
                for c in range(ncomp):
                    for row in range(2):
                        code = c * 2 + row
                        v = src[c, row, side, pl.ds(g * 8, 8), :]
                        from_lane = 127 if side == 1 else 0
                        v = pltpu.roll(v, (code - from_lane) % LN, 1)
                        packed = jnp.where(lane == code, v, packed)
                ysend[rnd, side, pl.ds(g * 8, 8), :] = packed
        copies = []
        for row, dst_t, slot in ((0, down, 1), (1, up, 0)):
            f = row
            copies.append(
                pltpu.make_async_remote_copy(
                    src_ref=src.at[pl.ds(0, ncomp), row, :, pl.ds(0, n)],
                    dst_ref=inbox.at[rnd // 2, slot, pl.ds(0, ncomp), :, pl.ds(0, n)],
                    send_sem=send_sem.at[rnd % 2, f],
                    recv_sem=recv_sem.at[rnd % 2, f],
                    device_id=(dst_t, u),
                    device_id_type=MESH,
                )
            )
        for dt in range(3):
            for side in range(2):
                f = 2 + dt * 2 + side
                copies.append(
                    pltpu.make_async_remote_copy(
                        src_ref=ysend.at[rnd, side, pl.ds(0, n)],
                        dst_ref=yin.at[rnd, 2 - dt, 1 - side, pl.ds(0, n)],
                        send_sem=send_sem.at[rnd % 2, f],
                        recv_sem=recv_sem.at[rnd % 2, f],
                        device_id=(tile_of[dt], right if side == 1 else left),
                        device_id_type=MESH,
                    )
                )
        for f in (4, 5, 0, 1, 2, 3, 6, 7):
            copies[f].start()
        return copies

    def shift_of(comp, r):
        return 4.0 * (r - 1) if comp == X else 0.0

    def centre(load, comps, r, n):
        for c, comp in enumerate(comps):
            for h in range(2):
                v = load(c, h, pl.ds(0, n))
                if comp == X and r != 1:
                    v = v + 4.0 * (r - 1)
                fld[field(r, comp, 1, h), pl.ds(0, n), :] = v

    def sides(load, comps, r, n, rnd, dt, sender_row):
        for c, comp in enumerate(comps):
            code = c * 2 + sender_row
            dx = 4.0 * (r - 1) if comp == X else 0.0
            for g in range(n // 8):
                rows = pl.ds(g * 8, 8)
                a0, a1 = load(c, 0, rows), load(c, 1, rows)
                lo = pltpu.roll(yin[rnd, dt, 0, rows, :], (0 - code) % LN, 1)
                hi = pltpu.roll(yin[rnd, dt, 1, rows, :], (127 - code) % LN, 1)
                r0, r1 = pltpu.roll(a0, 1, 1), pltpu.roll(a1, 1, 1)
                l0, l1 = pltpu.roll(a0, 127, 1), pltpu.roll(a1, 127, 1)
                first, last = lane == 0, lane == 127
                minus = [jnp.where(first, lo, r0), jnp.where(first, r0, r1)]
                plus = [jnp.where(last, l1, l0), jnp.where(last, hi, l1)]
                for h in range(2):
                    m, p = minus[h], plus[h]
                    if comp == Y:
                        m, p = m - 4.0, p + 4.0
                    elif comp == X and r != 1:
                        m, p = m + dx, p + dx
                    fld[field(r, comp, 0, h), rows, :] = m
                    fld[field(r, comp, 2, h), rows, :] = p

    def other(r, comp, b, h, j):
        return fld[field(r, comp, b, h), pl.ds(j, 8, stride=0), :]

    def own(row, comp, h, g, n):
        return fld[field(row + 1, comp, 1, h), pl.ds(g * 8, n * 8), :].reshape(n, 8, LN)

    EDGE_SLOT = 14

    def edges(comps):
        for comp in comps:
            for g in range(4):
                rows = pl.ds(g * 8, 8)

                def packed(zero, one, two, three):
                    v = fld[zero, rows, :]
                    v = jnp.where(lane == 1, pltpu.roll(fld[one, rows, :], 1, 1), v)
                    v = jnp.where(lane == 2, pltpu.roll(fld[two, rows, :], 2, 1), v)
                    return jnp.where(lane == 3, pltpu.roll(fld[three, rows, :], 4, 1), v)

                low0, low1 = field(1, comp, 1, 0), field(2, comp, 1, 0)
                fld[field(4, comp, 1, 0), rows, :] = packed(low0, low1, low1, field(2, comp, 1, 1))
                low0, low1 = field(1, comp, 0, 0), field(2, comp, 0, 0)
                fld[field(4, comp, 0, 0), rows, :] = packed(low0, low1, low0, field(1, comp, 2, 1))

    def spread_edges(sums):
        for g in range(4):
            rows = pl.ds(g * 8, 8)
            v = sums[2, 1, rows, :]
            one_two = pltpu.roll(v, 127, 1) + pltpu.roll(v, 126, 1)
            sums[0, 1, rows, :] += jnp.where(lane == 0, v, 0.0)
            sums[1, 1, rows, :] += jnp.where(lane == 0, one_two, 0.0)
            sums[1, 2, rows, :] += jnp.where(lane == 127, pltpu.roll(v, 124, 1), 0.0)

    def paired_stage(stage, body):
        if stage == 0:

            def alone(i, _):
                body(i // 2, 1 + i // 2, 1, i % 2, i, True)
                return 0

            def straight(h, _):
                body(0, 2, 1, h, 4 + h, False)
                return 0

            lax.fori_loop(0, 4, alone, 0)
            lax.fori_loop(0, 2, straight, 0)
        else:

            def slanted(ih, _):
                i, h = ih // 2, ih % 2
                body(i // 3, 1 + (i + 2) // 3, 2 - 2 * (i // 2 - i // 3), h, 6 + ih, False, True)
                return 0

            lax.fori_loop(0, 8, slanted, 0)

    def give_back(sums, which, r, b, h, alone, shifted, sign):
        for jg in range(2 if alone else 0, 4):
            rows = pl.ds(jg * 8, 8)
            part = back[which, pl.ds(jg * 64, 8, stride=8), :]
            for sub in range(1, 8):
                part = part + back[which, pl.ds(jg * 64 + sub, 8, stride=8), :]
            part = part * sign if sign != 1.0 else part
            if not shifted:
                sums[r - 1, 1 + h, rows, :] += part
            else:
                part = pltpu.roll(part, (b + (LN - 1)) % LN, 1)
                over = lane == (LN - 1) * (1 - b // 2)
                sums[r - 1, 1 + h, rows, :] += jnp.where(over, 0.0, part)
                sums[r - 1, h + b, rows, :] += jnp.where(over, part, 0.0)

    def density_paired(row, r, b, h, slot, alone, shifted=False):
        mine = [[own(row, comp, h, g, 2) for comp in (X, Y, Z, MS)] for g in (0, 2)]
        totals = [dens[row, 1 + h, pl.ds(g * 8, 16), :].reshape(2, 8, LN) for g in (0, 2)]
        for j in range(S):
            given = None
            mj = other(r, MS, b, h, j)
            for g in (0,) if alone and j < 16 else (0, 1):
                xi, yi, zi, mi = mine[g]
                dx = xi - other(r, X, b, h, j)
                dy = yi - other(r, Y, b, h, j)
                dz = zi - other(r, Z, b, h, j)
                r2 = dx * dx + dy * dy + dz * dz
                rad = r2 * lax.rsqrt(jnp.maximum(r2, 1e-30))
                s = jnp.maximum(4.0 - rad, 0.0)
                s3 = s * (s * s)
                w = s3 * (s * (5.0 - s))
                totals[g] = totals[g] + w * mj
                cache_w[slot * S + j, pl.ds(g * 2, 2)] = s3
                cache_a[slot * S + j, pl.ds(g * 2, 2)] = 1.0 / (r2 + 0.16)
                if not alone or (g == 0 and j >= 16):
                    wi = w * mi
                    wi = wi[0] + wi[1]
                    given = wi if given is None else given + wi
            if given is not None:
                back[0, pl.ds(j * 8, 8), :] = given
        for g in (0, 1):
            dens[row, 1 + h, pl.ds(g * 16, 16), :] = totals[g].reshape(16, LN)
        give_back(dens, 0, r, b, h, alone, shifted, 1.0)

    def force_paired(row, r, b, h, slot, alone, shifted=False):
        def half(g, first, backward):
            xi, yi, zi, vxi, vyi, vzi, qi, ci, ri, mi = (
                own(row, comp, h, g, 2) for comp in (X, Y, Z, VX, VY, VZ, Q, C, R, MS)
            )
            ax, ay, az = (acc[d, row, 1 + h, pl.ds(g * 8, 16), :].reshape(2, 8, LN) for d in range(3))
            for j in range(first, S):
                dx = xi - other(r, X, b, h, j)
                dy = yi - other(r, Y, b, h, j)
                dz = zi - other(r, Z, b, h, j)
                n = (
                    dx * (vxi - other(r, VX, b, h, j))
                    + dy * (vyi - other(r, VY, b, h, j))
                    + dz * (vzi - other(r, VZ, b, h, j))
                )
                mu = jnp.minimum(n, 0.0) * cache_a[slot * S + j, pl.ds(g, 2)]
                visc = (mu * (mu - (ci + other(r, C, b, h, j)))) / (ri + other(r, R, b, h, j))
                f = cache_w[slot * S + j, pl.ds(g, 2)] * (qi + other(r, Q, b, h, j) + visc)
                fi = f * other(r, MS, b, h, j)
                ax, ay, az = ax + fi * dx, ay + fi * dy, az + fi * dz
                if j >= backward:
                    fj = f * mi
                    for d, delta in enumerate((dx, dy, dz)):
                        back_d = fj * delta
                        back[d, pl.ds(j * 8, 8), :] = back_d[0] + back_d[1]
            for d, total in enumerate((ax, ay, az)):
                acc[d, row, 1 + h, pl.ds(g * 8, 16), :] = total.reshape(16, LN)
            if backward < S:
                for d in range(3):
                    give_back(acc.at[d], d, r, b, h, alone, shifted, -1.0)

        if alone:
            half(0, 0, 16)
            half(2, 16, S)
        else:

            def part(i, _):
                half(i * 2, 0, 0)
                return 0

            lax.fori_loop(0, 2, part, 0)

    def density_stage(stage, k, first=0, last=2):
        per = NACT[k] // 8
        halves = 2 if per == 1 else 1
        base = STAGE_BASE[stage]

        def pairs(c, h, edge=False):
            row, r, b = (2, 4, 0) if edge else stage_ids(stage, c)
            xi, yi, zi = (own(3 if edge else row, comp, h, 0, per) for comp in (X, Y, Z))
            slot = EDGE_SLOT if edge else (base + c) * 2 + h
            total = dens[row, 1 + h, pl.ds(0, per * 8), :].reshape(per, 8, LN)
            for j in range(S):
                dx = xi - other(r, X, b, h, j)
                dy = yi - other(r, Y, b, h, j)
                dz = zi - other(r, Z, b, h, j)
                r2 = dx * dx + dy * dy + dz * dz
                rad = r2 * lax.rsqrt(jnp.maximum(r2, 1e-30))
                s = jnp.maximum(4.0 - rad, 0.0)
                w3 = (s * other(r, MS, b, h, j)) * (s * s)
                total = total + w3 * (s * (5.0 - s))
                cache_w[slot * S + j, pl.ds(0, per)] = w3
                cache_a[slot * S + j, pl.ds(0, per)] = 1.0 / (r2 + 0.16)
            dens[row, 1 + h, pl.ds(0, per * 8), :] = total.reshape(per * 8, LN)

        def combo(i, _):
            if halves == 2:
                pairs(i, 0)
                pairs(i, 1)
            else:
                pairs(i // 2, i % 2)
            return 0

        if k == 0 and stage < 2:
            paired_stage(stage, density_paired)
            if stage == 1:
                pairs(0, 0, edge=True)
                spread_edges(dens)
            return
        per_row = STAGE_SIZE[stage] // halves
        lax.fori_loop(first * per_row, last * per_row, combo, 0)

    def force_stage(stage, k, first=0, last=2):
        groups = NACT[k] // 8
        per = min(groups, 2)
        sets = groups // per
        halves = 2 if per == 1 else 1
        base = STAGE_BASE[stage]

        def pairs(c, h, g, edge=False):
            row, r, b = (2, 4, 0) if edge else stage_ids(stage, c)
            xi, yi, zi, vxi, vyi, vzi, qi, ci, ri = (
                own(3 if edge else row, comp, h, g, per) for comp in (X, Y, Z, VX, VY, VZ, Q, C, R)
            )
            slot = EDGE_SLOT if edge else (base + c) * 2 + h
            ax, ay, az = (acc[d, row, 1 + h, pl.ds(g * 8, per * 8), :].reshape(per, 8, LN) for d in range(3))
            for j in range(S):
                dx = xi - other(r, X, b, h, j)
                dy = yi - other(r, Y, b, h, j)
                dz = zi - other(r, Z, b, h, j)
                n = (
                    dx * (vxi - other(r, VX, b, h, j))
                    + dy * (vyi - other(r, VY, b, h, j))
                    + dz * (vzi - other(r, VZ, b, h, j))
                )
                mu = jnp.minimum(n, 0.0) * cache_a[slot * S + j, pl.ds(g, per)]
                sound = ci + other(r, C, b, h, j)
                visc = (mu * (mu - sound)) / (ri + other(r, R, b, h, j))
                f = cache_w[slot * S + j, pl.ds(g, per)] * (qi + other(r, Q, b, h, j) + visc)
                ax, ay, az = ax + f * dx, ay + f * dy, az + f * dz
            for d, total in enumerate((ax, ay, az)):
                acc[d, row, 1 + h, pl.ds(g * 8, per * 8), :] = total.reshape(per * 8, LN)

        def combo(i, _):
            if halves == 2:
                pairs(i, 0, 0)
                pairs(i, 1, 0)
            else:
                ch, g = i // sets, (i % sets) * per
                pairs(ch // 2, ch % 2, g)
            return 0

        if k == 0 and stage < 2:
            paired_stage(stage, force_paired)
            if stage == 1:

                def edge(i, _):
                    pairs(0, 0, i * 2, edge=True)
                    return 0

                lax.fori_loop(0, 2, edge, 0)
                for d in range(3):
                    spread_edges(acc.at[d])
            return
        per_row = STAGE_SIZE[stage] * sets // halves
        lax.fori_loop(first * per_row, last * per_row, combo, 0)

    def plan():
        row_i = lax.broadcasted_iota(jnp.int32, (LN, LN), 0)
        col_i = lax.broadcasted_iota(jnp.int32, (LN, LN), 1)
        before = jnp.where(row_i < col_i, 1.0, 0.0).astype(jnp.bfloat16)
        ones = jnp.ones((LN, LN), jnp.bfloat16)
        row8 = lax.broadcasted_iota(jnp.int32, (8, LN), 0)
        dest = tgt[...]
        start = jnp.zeros((LN, LN), jnp.float32)
        place = jnp.zeros((LN, LN), jnp.float32)
        start_t = jnp.zeros((8, LN), jnp.float32)
        info = jnp.zeros((8, LN), jnp.float32)
        for d in range(subs):
            mine = dest == d
            hot = jnp.where(mine, 1.0, 0.0).astype(jnp.bfloat16)
            inside = jnp.dot(hot, before, preferred_element_type=jnp.float32)
            place = jnp.where(mine, start + inside, place)
            start = start + jnp.dot(hot, ones, preferred_element_type=jnp.float32)
            count_t = lax.dot_general(
                ones[0:8], hot, (((1,), (1,)), ((), ())), preferred_element_type=jnp.float32
            )
            info = jnp.where(row8 == d, start_t, info)
            info = jnp.where(row8 == subs + d, count_t, info)
            start_t = start_t + count_t
        pos[...] = place.astype(jnp.int32)
        tab[u] = info
        sends = []
        for k in range(1, subs):
            copy = pltpu.make_async_remote_copy(
                src_ref=tab.at[u],
                dst_ref=tab.at[u],
                send_sem=tab_send.at[k],
                recv_sem=tab_recv.at[k],
                device_id=(t, lax.rem(u + k, subs)),
                device_id_type=MESH,
            )
            copy.start()
            sends.append(copy)
        return sends

    def emit(g, own_rows):
        row_q = lax.broadcasted_iota(jnp.int32, (LN, LN), 0)
        for row in own_rows:
            for h in range(2):
                count = jnp.broadcast_to(cnt[0, pl.ds(h * 2 + row, 1), :], (8, LN))
                rows = pl.ds(g * 8, 8)
                slot = lax.broadcasted_iota(jnp.int32, (8, LN), 0) + g * 8
                in_rows = pl.ds(g * 32 + h * 2 + row, 8, stride=4)
                values = [st[d, row, h, rows, :] * 0.25 for d in range(3)]
                values += [st[3 + d, row, h, rows, :] * 0.0625 for d in range(3)]
                values += [pr[2, row, h, rows, :] * 0.25]
                values += [jnp.where(slot < count, mass[in_rows, :], 0.0)]
                for i, v in enumerate(values):
                    raw[g, pl.ds((row * 2 + h) * 64 + i, 8, stride=8), :] = v

        def sort(rh, _):
            row, h = rh // 2, rh % 2
            for i in range(8):
                slot = g * 8 + i
                line = pos[pl.ds(slot * 4 + h * 2 + row, 1), :]
                hot = jnp.where(row_q == jnp.broadcast_to(line, (LN, LN)), 1.0, 0.0)
                v = raw[g, pl.ds(rh * 64 + i * 8, 8), :]
                hi = v.astype(jnp.bfloat16)
                rest = v - hi.astype(jnp.float32)
                mid = rest.astype(jnp.bfloat16)
                low = (rest - mid.astype(jnp.float32)).astype(jnp.bfloat16)
                pieces = jnp.concatenate([hi, mid, low], axis=0)
                moved = lax.dot_general(
                    pieces, hot.astype(jnp.bfloat16), (((1,), (1,)), ((), ())), preferred_element_type=jnp.float32
                )
                gathered[u, slot * 2 + h, row] = (moved[0:8] + moved[8:16]) + moved[16:24]
            return 0

        lax.fori_loop(own_rows[0] * 2, own_rows[-1] * 2 + 2, sort, 0)

    PIECES = ((32, 32, (0, 1)), (16, 16, (0, 1)), (0, 16, (0,)), (0, 16, (1,)))

    def piece_copy(p, flow, owner, second_half, dst):
        first, rows, own_rows = PIECES[p]
        half = rows // 2
        part = pl.ds(first + half * second_half, half)
        which = slice(None) if len(own_rows) == 2 else own_rows[0]
        landing = done if p >= 2 and flow not in (0, 2) else gathered
        return pltpu.make_async_remote_copy(
            src_ref=gathered.at[owner, part, which],
            dst_ref=landing.at[owner, part, which],
            send_sem=piece_send.at[p, flow],
            recv_sem=piece_recv.at[p, flow],
            device_id=(t, dst),
            device_id_type=MESH,
        )

    leaving = []

    def write_out(p, at, owner, first, rows):
        own_rows = PIECES[p][2]
        which = slice(None) if len(own_rows) == 2 else own_rows[0]
        copy = pltpu.make_async_copy(
            gathered.at[owner, pl.ds(first, rows), which], done.at[owner, pl.ds(first, rows), which], done_sem.at[p, at]
        )
        copy.start()
        leaving.append(copy)

    def start_piece(p, before_rest=None):
        first, rows, own_rows = PIECES[p]
        for g in range(first // 16, (first + rows) // 16):
            emit(g, own_rows)
        copies = [
            piece_copy(p, 0, u, 0, right),
            piece_copy(p, 1, u, 1, right),
            piece_copy(p, 2, u, 1, left),
            piece_copy(p, 3, u, 0, left),
        ]
        arriving[p] = copies
        copies[0].start()
        copies[2].start()
        if before_rest is not None:
            before_rest()
        copies[1].start()
        copies[3].start()
        if p >= 2:
            write_out(p, 0, u, first, rows)

    def forward_piece(p):
        arriving[p][0].wait_recv()
        arriving[p][2].wait_recv()
        copies = [piece_copy(p, 4, left, 0, right), piece_copy(p, 5, right, 1, left)]
        for copy in copies:
            copy.start()
        arriving[p] += copies
        if p >= 2:
            first, rows, _ = PIECES[p]
            write_out(p, 1, left, first, rows // 2)
            write_out(p, 2, right, first + rows // 2, rows // 2)

    def finish_piece(p):
        for f in (1, 3, 4, 5):
            arriving[p][f].wait_recv()
        for copy in arriving[p]:
            copy.wait_send()
        if p < 2:
            write_out(p, 0, slice(None), PIECES[p][0], PIECES[p][1])

    def exchange_and_sum(rnd, src, inbox, comps, n, stage_fn, k, meanwhile, row_done=None):
        copies = start_round(rnd, src, len(comps), n, inbox)
        meanwhile()
        loads = [None] * 4
        for r in (1, 2):
            loads[r] = functools.partial(lambda row, c, h, rows: src[c, row, h, rows, :], r - 1)
        loads[0] = lambda c, h, rows: inbox[rnd // 2, 0, c, h, rows, :]
        loads[3] = lambda c, h, rows: inbox[rnd // 2, 1, c, h, rows, :]
        for r in (1, 2):
            centre(loads[r], comps, r, n)
        stage_fn(0, k)
        copies[4].wait_recv()
        copies[5].wait_recv()
        for r in (1, 2):
            sides(loads[r], comps, r, n, rnd, 1, r - 1)
        if k == 0:
            edges(comps)
        stage_fn(1, k, 0, 2 if row_done is None else 1)
        for f in (0, 1, 2, 3, 6, 7):
            copies[f].wait_recv()
        for r, dt, sender_row in ((0, 0, 1), (3, 2, 0)):
            centre(loads[r], comps, r, n)
            sides(loads[r], comps, r, n, rnd, dt, sender_row)
        if row_done is None:
            stage_fn(2, k)
            return copies
        for copy in copies:
            copy.wait_send()
        stage_fn(2, k, 0, 1)
        row_done(0)
        stage_fn(1, k, 1, 2)
        row_done(1)
        stage_fn(2, k, 1, 2)
        row_done(2)
        return []

    arriving = {}

    def lay_plan():
        for copy in arriving["tab"]:
            copy.wait_recv()
        row_i = lax.broadcasted_iota(jnp.int32, (LN, LN), 0)
        col_i = lax.broadcasted_iota(jnp.int32, (LN, LN), 1)

        def order(i):
            return (i // 4) * 4 + (i % 2) * 2 + (i // 2) % 2

        earlier = jnp.where(order(row_i) < order(col_i), 1.0, 0.0).astype(jnp.bfloat16)
        starts = jnp.concatenate([tab[src, pl.ds(u, 1), :] for src in range(subs)], axis=0)
        counts = jnp.concatenate([tab[src, pl.ds(subs + u, 1), :] for src in range(subs)], axis=0)
        padded = jnp.concatenate([counts, jnp.zeros_like(counts)], axis=0).astype(jnp.bfloat16)
        base = jnp.dot(padded, earlier, preferred_element_type=jnp.float32)[0:subs]
        base = base.astype(jnp.int32)
        skip = base & (LN - 1)
        turn = (skip - starts.astype(jnp.int32)) & (LN - 1)
        end = skip + counts.astype(jnp.int32)
        runs[0:subs, :] = turn + skip * 128 + end * 16384 + (base >> 7) * 4194304
        runs[subs : 2 * subs, :] = jnp.zeros((subs, LN), jnp.int32)
        arriving["runs"] = pltpu.make_async_copy(runs, runs_out, runs_sem)
        arriving["runs"].start()

    def during(rnd):
        if rnd == 0:
            arriving["tab"] = plan()
        elif rnd == 1:
            lay_plan()
        elif rnd in (2, 4):
            if rnd == 4:
                finish_piece(0)
            start_piece(rnd // 2 - 1)
        elif rnd in (3, 5):
            forward_piece(rnd // 2 - 1)

    def move(k, row):
        for h in range(2):
            count = jnp.broadcast_to(cnt[k, pl.ds(h * 2 + row, 1), :], (8, LN))
            for g in range(NACT[k] // 8):
                rows = pl.ds(g * 8, 8)
                slot = lax.broadcasted_iota(jnp.int32, (8, LN), 0) + g * 8
                active = slot < count
                for d in range(3):
                    v = st[3 + d, row, h, rows, :]
                    x = st[d, row, h, rows, :]
                    v_new = v + 4.0 * acc[d, row, 1 + h, rows, :]
                    st[3 + d, row, h, rows, :] = jnp.where(active, v_new, v)
                    st[d, row, h, rows, :] = jnp.where(active, x + 0.0125 * v_new, x)

    def last_rows(step):
        if step == 0:
            move(2, 0)
            start_piece(2)
        elif step == 2:
            finish_piece(1)
            move(2, 1)
            start_piece(3, lambda: forward_piece(2))
            forward_piece(3)

    for k in range(3):
        n = NACT[k]
        dens[...] = jnp.zeros_like(dens)
        comps = (X, Y, Z, VX, VY, VZ) + ((MS,) if k == 0 else ())
        moved = exchange_and_sum(2 * k, st, xin, comps, NMOVED[k], density_stage, k, lambda: during(2 * k))
        for row in range(2):
            for h in range(2):
                count = jnp.broadcast_to(cnt[k, pl.ds(h * 2 + row, 1), :], (8, LN))
                for g in range(n // 8):
                    rows = pl.ds(g * 8, 8)
                    slot = lax.broadcasted_iota(jnp.int32, (8, LN), 0) + g * 8
                    rho4 = jnp.where(slot < count, dens[row, 1 + h, rows, :], pr[2, row, h, rows, :])
                    root = jnp.exp(jnp.log(rho4 * 0.25) * (1.0 / 3.0))
                    pr[0, row, h, rows, :] = sq[0, row, h, rows, :] / root
                    pr[1, row, h, rows, :] = sq[1, row, h, rows, :] * root
                    pr[2, row, h, rows, :] = rho4
        acc[...] = jnp.zeros_like(acc)
        if k == 2:
            for copy in moved:
                copy.wait_send()
        pressed = exchange_and_sum(
            2 * k + 1, pr, pin, (Q, C, R), n, force_stage, k, lambda: during(2 * k + 1), last_rows if k == 2 else None
        )
        if k < 2:
            for copy in moved + pressed:
                copy.wait_send()
            for row in range(2):
                move(k, row)
    for copy in arriving["tab"]:
        copy.wait_send()
    for p in (2, 3):
        finish_piece(p)
    for copy in leaving:
        copy.wait()
    arriving["runs"].wait()


TILES = 48


STEPS = 4


def lay_kernel(runs_in, gathered_in, out, runs, gathered, tiles, runs_sem, in_sem, out_sem):
    subs = gathered.shape[0]
    lane = lane_iota()
    beyond = lane + LN
    block = LN // 2 // STEPS
    inputs = [
        pltpu.make_async_copy(
            gathered_in.at[:, pl.ds(i * block, block)], gathered.at[:, pl.ds(i * block, block)], in_sem.at[i]
        )
        for i in range(STEPS)
    ]
    table = pltpu.make_async_copy(runs_in, runs, runs_sem)
    table.start()
    inputs[0].start()
    inputs[1].start()
    tiles[...] = jnp.zeros_like(tiles)
    table.wait()

    def lay(slot, currents):
        for row in range(2):
            for h in range(2):
                at = slot * 4 + h * 2 + row
                later = []
                for src in range(subs):
                    word = runs[src, at]
                    words = jnp.full((8, LN), word)
                    end = (words >> 14) & 255
                    turned = pltpu.roll(gathered[src, slot * 2 + h, row], word & (LN - 1), 1)
                    kept = jnp.where(lane < end, turned, 0.0)
                    merged = jnp.where(lane < ((words >> 7) & (LN - 1)), currents[src], kept)
                    tiles[src, word >> 22] = merged
                    wrapped = jnp.where(beyond < end, turned, 0.0)
                    later.append(jnp.where(end >= LN, wrapped, merged))
                currents = later
        return tuple(currents)

    currents = (jnp.zeros((8, LN), jnp.float32),) * subs
    for i in range(STEPS):
        inputs[i].wait()
        if i + 2 < STEPS:
            inputs[i + 2].start()
        currents = lax.fori_loop(i * (S // STEPS), (i + 1) * (S // STEPS), lay, currents)
    outputs = []
    for src in range(subs):
        word = runs[src, LN - 1]
        tiles[src, (word >> 22) + jnp.where((word >> 14) & 255 >= LN, 1, 0)] = currents[src]
    for src in range(subs):
        copy = pltpu.make_async_copy(
            tiles.at[src, pl.ds(0, TILES)], out.at[pl.ds(src * TILES, TILES)], out_sem.at[src]
        )
        copy.start()
        outputs.append(copy)
    for copy in outputs:
        copy.wait()


def rows_of(a):
    lead = a.shape[:-2]
    a = a.reshape(lead + (2, 2, LN))
    a = jnp.swapaxes(a, -3, -2)
    return a


def shards(tiles, subs, offsets, velocity, mass, entropy, active_counts, targets):
    off = rows_of(offsets).reshape(3, LN, LN)
    vel = rows_of(velocity).reshape(3, LN, LN)
    mas = rows_of(mass).reshape(LN, LN)
    ent = rows_of(entropy).reshape(LN, LN)
    cnt = rows_of(active_counts).reshape(3, 4, LN)
    tgt = rows_of(targets).reshape(LN, LN)
    anywhere = pl.BlockSpec(memory_space=pl.ANY)
    f32 = jnp.float32
    gathered, runs = pl.pallas_call(
        functools.partial(substeps_kernel, tiles, subs),
        out_shape=[
            jax.ShapeDtypeStruct((subs, LN // 2, 2, 8, LN), f32),
            jax.ShapeDtypeStruct((2 * subs, LN), jnp.int32),
        ],
        in_specs=[anywhere] * 6,
        out_specs=[anywhere] * 2,
        scratch_shapes=[
            pltpu.VMEM((subs, LN // 2, 2, 8, LN), f32),
            pltpu.VMEM((3, LN, LN), f32),
            pltpu.VMEM((3, LN, LN), f32),
            pltpu.VMEM((LN, LN), f32),
            pltpu.VMEM((LN, LN), f32),
            pltpu.VMEM((3, 4, LN), jnp.int32),
            pltpu.VMEM((LN, LN), jnp.int32),
            pltpu.VMEM((2 * subs, LN), jnp.int32),
            pltpu.VMEM((5 * NF * 6, S, LN), f32),
            pltpu.VMEM((7, 2, 2, S, LN), f32),
            pltpu.VMEM((3, 2, 2, S, LN), f32),
            pltpu.VMEM((3, 4, S, LN), f32),
            pltpu.VMEM((3, 3, 4, S, LN), f32),
            pltpu.VMEM((2, 2, 2, S, LN), f32),
            pltpu.VMEM((6, 2, S, LN), f32),
            pltpu.VMEM((3, 2, 7, 2, S, LN), f32),
            pltpu.VMEM((3, 2, 3, 2, S, LN), f32),
            pltpu.VMEM((6, 3, 2, S, LN), f32),
            pltpu.VMEM((18 * 2 * S, 4, 8, LN), f32),
            pltpu.VMEM((18 * 2 * S, 4, 8, LN), f32),
            pltpu.VMEM((4, 256, LN), f32),
            pltpu.VMEM((3, 256, LN), f32),
            pltpu.VMEM((LN, LN), jnp.int32),
            pltpu.VMEM((subs, 2 * subs, LN), f32),
            pltpu.SemaphoreType.DMA((2, 8)),
            pltpu.SemaphoreType.DMA((2, 8)),
            pltpu.SemaphoreType.DMA((4,)),
            pltpu.SemaphoreType.DMA((4,)),
            pltpu.SemaphoreType.DMA((4, 6)),
            pltpu.SemaphoreType.DMA((4, 6)),
            pltpu.SemaphoreType.DMA((4, 3)),
            pltpu.SemaphoreType.DMA((6,)),
            pltpu.SemaphoreType.DMA,
        ],
        compiler_params=pltpu.CompilerParams(collective_id=0, has_side_effects=True, vmem_limit_bytes=62 * 1024 * 1024),
        name="substeps",
    )(off, vel, mas, ent, cnt, tgt)
    arrived = pl.pallas_call(
        lay_kernel,
        out_shape=jax.ShapeDtypeStruct((subs * TILES, 8, LN), f32),
        in_specs=[anywhere] * 2,
        out_specs=anywhere,
        scratch_shapes=[
            pltpu.SMEM((2 * subs, LN), jnp.int32),
            pltpu.VMEM((subs, LN // 2, 2, 8, LN), f32),
            pltpu.VMEM((subs, TILES + 2, 8, LN), f32),
            pltpu.SemaphoreType.DMA,
            pltpu.SemaphoreType.DMA((STEPS,)),
            pltpu.SemaphoreType.DMA((subs,)),
        ],
        name="lay",
    )(runs, gathered)
    return jnp.transpose(arrived, (1, 0, 2)).reshape(8, subs * TILES * LN)


def solution(mesh):
    tiles, subs = mesh.shape["tile"], mesh.shape["sub"]
    placed = (
        P(None, None, "tile", "sub"),
        P(None, None, "tile", "sub"),
        P(None, "tile", "sub"),
        P(None, "tile", "sub"),
        P(None, "tile", "sub"),
        P(None, "tile", "sub"),
    )
    return jax.shard_map(
        functools.partial(shards, tiles, subs),
        mesh=mesh,
        in_specs=placed,
        out_specs=P(None, ("tile", "sub")),
        check_vma=False,
    )
```

```python
import functools
import math

import jax
import jax.numpy as jnp
from jax import lax
from jax.experimental import pallas as pl
from jax.experimental.pallas import tpu as pltpu
from jax.sharding import PartitionSpec as P

MESH = pl.DeviceIdType.MESH

S = 32
LN = 128
KERNEL_NORM = 21.0 / (2.0 * math.pi)
NACT = (32, 16, 8)
NMOVED = (32, 32, 16)

X, Y, Z, VX, VY, VZ, MS, Q, C, R = range(10)
NF = 10


def field(row, comp, b, h):
    return ((row * NF + comp) * 3 + b) * 2 + h


def lane_iota():
    return lax.broadcasted_iota(jnp.int32, (8, LN), 1)


def stage_ids(stage, c):
    if stage == 0:
        return c // 2, 1 + c % 2, 1
    if stage == 1:
        return c // 4, 1 + (c // 2) % 2, 2 * (c % 2)
    return c // 3, 3 * (c // 3), c % 3


STAGE_SIZE = (4, 8, 6)
STAGE_BASE = (0, 4, 12)


def substeps_kernel(
    tiles, subs, off_in, vel_in, mass_in, ent_in, cnt_in, tgt_in, done, runs_out, gathered, off, vel, mass, ent, cnt,
    tgt, runs, fld, st, pr, dens, acc, sq, ysend, xin, pin, yin,
    cache_w, cache_a, raw, back, pos, tab, send_sem, recv_sem, tab_send, tab_recv, piece_send, piece_recv, done_sem, in_sem, runs_sem
):
    t, u = lax.axis_index("tile"), lax.axis_index("sub")
    up, down = lax.rem(t + 1, tiles), lax.rem(t + tiles - 1, tiles)
    right, left = lax.rem(u + 1, subs), lax.rem(u + subs - 1, subs)
    tile_of = (down, t, up)

    barrier = pltpu.get_barrier_semaphore()
    across = lax.rem(u + 2, subs)
    near = ((down, u), (up, u), (down, left), (t, left), (up, left), (down, right), (t, right), (up, right))
    for dev in near + ((t, across),):
        pl.semaphore_signal(barrier, inc=1, device_id=dev, device_id_type=MESH)

    inputs = [
        pltpu.make_async_copy(src, dst, in_sem.at[i])
        for i, (src, dst) in enumerate(
            ((cnt_in, cnt), (off_in, off), (vel_in, vel), (mass_in, mass), (ent_in, ent), (tgt_in, tgt))
        )
    ]
    for copy in inputs:
        copy.start()
    for copy in inputs:
        copy.wait()

    for row in range(2):
        for h in range(2):
            count = jnp.broadcast_to(cnt[0, pl.ds(h * 2 + row, 1), :], (8, LN))
            for g in range(4):
                rows = pl.ds(g * 32 + h * 2 + row, 8, stride=4)
                dst = (row, h, pl.ds(g * 8, 8))
                for c in range(3):
                    st[(c,) + dst] = off[c, rows, :] * 4.0
                    st[(3 + c,) + dst] = vel[c, rows, :] * 16.0
                slot = lax.broadcasted_iota(jnp.int32, (8, LN), 0) + g * 8
                st[(6,) + dst] = jnp.where(slot < count, mass[rows, :] * (KERNEL_NORM / 64.0), 0.0)
                e = ent[rows, :]
                sq[(0,) + dst] = e
                sq[(1,) + dst] = jnp.sqrt(e * (5.0 / 3.0))
                pr[(2,) + dst] = jnp.full((8, LN), 4.0, jnp.float32)
    pl.semaphore_wait(barrier, 9)

    lane = lane_iota()

    def start_round(rnd, src, ncomp, n, inbox):
        for side in range(2):
            for g in range(n // 8):
                packed = jnp.zeros((8, LN), jnp.float32)
                for c in range(ncomp):
                    for row in range(2):
                        code = c * 2 + row
                        v = src[c, row, side, pl.ds(g * 8, 8), :]
                        from_lane = 127 if side == 1 else 0
                        v = pltpu.roll(v, (code - from_lane) % LN, 1)
                        packed = jnp.where(lane == code, v, packed)
                ysend[rnd, side, pl.ds(g * 8, 8), :] = packed
        copies = []
        for row, dst_t, slot in ((0, down, 1), (1, up, 0)):
            f = row
            copies.append(
                pltpu.make_async_remote_copy(
                    src_ref=src.at[pl.ds(0, ncomp), row, :, pl.ds(0, n)],
                    dst_ref=inbox.at[rnd // 2, slot, pl.ds(0, ncomp), :, pl.ds(0, n)],
                    send_sem=send_sem.at[rnd % 2, f],
                    recv_sem=recv_sem.at[rnd % 2, f],
                    device_id=(dst_t, u),
                    device_id_type=MESH,
                )
            )
        for dt in range(3):
            for side in range(2):
                f = 2 + dt * 2 + side
                copies.append(
                    pltpu.make_async_remote_copy(
                        src_ref=ysend.at[rnd, side, pl.ds(0, n)],
                        dst_ref=yin.at[rnd, 2 - dt, 1 - side, pl.ds(0, n)],
                        send_sem=send_sem.at[rnd % 2, f],
                        recv_sem=recv_sem.at[rnd % 2, f],
                        device_id=(tile_of[dt], right if side == 1 else left),
                        device_id_type=MESH,
                    )
                )
        for f in (4, 5, 0, 1, 2, 3, 6, 7):
            copies[f].start()
        return copies

    def shift_of(comp, r):
        return 4.0 * (r - 1) if comp == X else 0.0

    def centre(load, comps, r, n):
        for c, comp in enumerate(comps):
            for h in range(2):
                v = load(c, h, pl.ds(0, n))
                if comp == X and r != 1:
                    v = v + 4.0 * (r - 1)
                fld[field(r, comp, 1, h), pl.ds(0, n), :] = v

    def sides(load, comps, r, n, rnd, dt, sender_row):
        for c, comp in enumerate(comps):
            code = c * 2 + sender_row
            dx = 4.0 * (r - 1) if comp == X else 0.0
            for g in range(n // 8):
                rows = pl.ds(g * 8, 8)
                a0, a1 = load(c, 0, rows), load(c, 1, rows)
                lo = pltpu.roll(yin[rnd, dt, 0, rows, :], (0 - code) % LN, 1)
                hi = pltpu.roll(yin[rnd, dt, 1, rows, :], (127 - code) % LN, 1)
                r0, r1 = pltpu.roll(a0, 1, 1), pltpu.roll(a1, 1, 1)
                l0, l1 = pltpu.roll(a0, 127, 1), pltpu.roll(a1, 127, 1)
                first, last = lane == 0, lane == 127
                minus = [jnp.where(first, lo, r0), jnp.where(first, r0, r1)]
                plus = [jnp.where(last, l1, l0), jnp.where(last, hi, l1)]
                for h in range(2):
                    m, p = minus[h], plus[h]
                    if comp == Y:
                        m, p = m - 4.0, p + 4.0
                    elif comp == X and r != 1:
                        m, p = m + dx, p + dx
                    fld[field(r, comp, 0, h), rows, :] = m
                    fld[field(r, comp, 2, h), rows, :] = p

    def other(r, comp, b, h, j):
        return fld[field(r, comp, b, h), pl.ds(j, 8, stride=0), :]

    def own(row, comp, h, g, n):
        return fld[field(row + 1, comp, 1, h), pl.ds(g * 8, n * 8), :].reshape(n, 8, LN)

    EDGE_SLOT = 14

    def edges(comps):
        for comp in comps:
            for g in range(4):
                rows = pl.ds(g * 8, 8)

                def packed(zero, one, two, three):
                    v = fld[zero, rows, :]
                    v = jnp.where(lane == 1, pltpu.roll(fld[one, rows, :], 1, 1), v)
                    v = jnp.where(lane == 2, pltpu.roll(fld[two, rows, :], 2, 1), v)
                    return jnp.where(lane == 3, pltpu.roll(fld[three, rows, :], 4, 1), v)

                low0, low1 = field(1, comp, 1, 0), field(2, comp, 1, 0)
                fld[field(4, comp, 1, 0), rows, :] = packed(low0, low1, low1, field(2, comp, 1, 1))
                low0, low1 = field(1, comp, 0, 0), field(2, comp, 0, 0)
                fld[field(4, comp, 0, 0), rows, :] = packed(low0, low1, low0, field(1, comp, 2, 1))

    def spread_edges(sums):
        for g in range(4):
            rows = pl.ds(g * 8, 8)
            v = sums[2, 1, rows, :]
            one_two = pltpu.roll(v, 127, 1) + pltpu.roll(v, 126, 1)
            sums[0, 1, rows, :] += jnp.where(lane == 0, v, 0.0)
            sums[1, 1, rows, :] += jnp.where(lane == 0, one_two, 0.0)
            sums[1, 2, rows, :] += jnp.where(lane == 127, pltpu.roll(v, 124, 1), 0.0)

    def paired_stage(stage, body):
        if stage == 0:

            def alone(i, _):
                body(i // 2, 1 + i // 2, 1, i % 2, i, True)
                return 0

            def straight(h, _):
                body(0, 2, 1, h, 4 + h, False)
                return 0

            lax.fori_loop(0, 4, alone, 0)
            lax.fori_loop(0, 2, straight, 0)
        else:

            def slanted(ih, _):
                i, h = ih // 2, ih % 2
                body(i // 3, 1 + (i + 2) // 3, 2 - 2 * (i // 2 - i // 3), h, 6 + ih, False, True)
                return 0

            lax.fori_loop(0, 8, slanted, 0)

    def give_back(sums, which, r, b, h, alone, shifted, sign):
        for jg in range(2 if alone else 0, 4):
            rows = pl.ds(jg * 8, 8)
            part = back[which, pl.ds(jg * 64, 8, stride=8), :]
            for sub in range(1, 8):
                part = part + back[which, pl.ds(jg * 64 + sub, 8, stride=8), :]
            part = part * sign if sign != 1.0 else part
            if not shifted:
                sums[r - 1, 1 + h, rows, :] += part
            else:
                part = pltpu.roll(part, (b + (LN - 1)) % LN, 1)
                over = lane == (LN - 1) * (1 - b // 2)
                sums[r - 1, 1 + h, rows, :] += jnp.where(over, 0.0, part)
                sums[r - 1, h + b, rows, :] += jnp.where(over, part, 0.0)

    def density_paired(row, r, b, h, slot, alone, shifted=False):
        mine = [[own(row, comp, h, g, 2) for comp in (X, Y, Z, MS)] for g in (0, 2)]
        totals = [dens[row, 1 + h, pl.ds(g * 8, 16), :].reshape(2, 8, LN) for g in (0, 2)]
        for j in range(S):
            given = None
            mj = other(r, MS, b, h, j)
            for g in (0,) if alone and j < 16 else (0, 1):
                xi, yi, zi, mi = mine[g]
                dx = xi - other(r, X, b, h, j)
                dy = yi - other(r, Y, b, h, j)
                dz = zi - other(r, Z, b, h, j)
                r2 = dx * dx + dy * dy + dz * dz
                rad = r2 * lax.rsqrt(jnp.maximum(r2, 1e-30))
                s = jnp.maximum(4.0 - rad, 0.0)
                s3 = s * (s * s)
                w = s3 * (s * (5.0 - s))
                totals[g] = totals[g] + w * mj
                cache_w[slot * S + j, pl.ds(g * 2, 2)] = s3
                cache_a[slot * S + j, pl.ds(g * 2, 2)] = 1.0 / (r2 + 0.16)
                if not alone or (g == 0 and j >= 16):
                    wi = w * mi
                    wi = wi[0] + wi[1]
                    given = wi if given is None else given + wi
            if given is not None:
                back[0, pl.ds(j * 8, 8), :] = given
        for g in (0, 1):
            dens[row, 1 + h, pl.ds(g * 16, 16), :] = totals[g].reshape(16, LN)
        give_back(dens, 0, r, b, h, alone, shifted, 1.0)

    def force_paired(row, r, b, h, slot, alone, shifted=False):
        def half(g, first, backward):
            xi, yi, zi, vxi, vyi, vzi, qi, ci, ri, mi = (
                own(row, comp, h, g, 2) for comp in (X, Y, Z, VX, VY, VZ, Q, C, R, MS)
            )
            ax, ay, az = (acc[d, row, 1 + h, pl.ds(g * 8, 16), :].reshape(2, 8, LN) for d in range(3))
            for j in range(first, S):
                dx = xi - other(r, X, b, h, j)
                dy = yi - other(r, Y, b, h, j)
                dz = zi - other(r, Z, b, h, j)
                n = (
                    dx * (vxi - other(r, VX, b, h, j))
                    + dy * (vyi - other(r, VY, b, h, j))
                    + dz * (vzi - other(r, VZ, b, h, j))
                )
                mu = jnp.minimum(n, 0.0) * cache_a[slot * S + j, pl.ds(g, 2)]
                visc = (mu * (mu - (ci + other(r, C, b, h, j)))) / (ri + other(r, R, b, h, j))
                f = cache_w[slot * S + j, pl.ds(g, 2)] * (qi + other(r, Q, b, h, j) + visc)
                fi = f * other(r, MS, b, h, j)
                ax, ay, az = ax + fi * dx, ay + fi * dy, az + fi * dz
                if j >= backward:
                    fj = f * mi
                    for d, delta in enumerate((dx, dy, dz)):
                        back_d = fj * delta
                        back[d, pl.ds(j * 8, 8), :] = back_d[0] + back_d[1]
            for d, total in enumerate((ax, ay, az)):
                acc[d, row, 1 + h, pl.ds(g * 8, 16), :] = total.reshape(16, LN)
            if backward < S:
                for d in range(3):
                    give_back(acc.at[d], d, r, b, h, alone, shifted, -1.0)

        if alone:
            half(0, 0, 16)
            half(2, 16, S)
        else:

            def part(i, _):
                half(i * 2, 0, 0)
                return 0

            lax.fori_loop(0, 2, part, 0)

    def density_stage(stage, k, first=0, last=2):
        per = NACT[k] // 8
        halves = 2 if per == 1 else 1
        base = STAGE_BASE[stage]

        def pairs(c, h, edge=False):
            row, r, b = (2, 4, 0) if edge else stage_ids(stage, c)
            xi, yi, zi = (own(3 if edge else row, comp, h, 0, per) for comp in (X, Y, Z))
            slot = EDGE_SLOT if edge else (base + c) * 2 + h
            total = dens[row, 1 + h, pl.ds(0, per * 8), :].reshape(per, 8, LN)
            for j in range(S):
                dx = xi - other(r, X, b, h, j)
                dy = yi - other(r, Y, b, h, j)
                dz = zi - other(r, Z, b, h, j)
                r2 = dx * dx + dy * dy + dz * dz
                rad = r2 * lax.rsqrt(jnp.maximum(r2, 1e-30))
                s = jnp.maximum(4.0 - rad, 0.0)
                w3 = (s * other(r, MS, b, h, j)) * (s * s)
                total = total + w3 * (s * (5.0 - s))
                cache_w[slot * S + j, pl.ds(0, per)] = w3
                cache_a[slot * S + j, pl.ds(0, per)] = 1.0 / (r2 + 0.16)
            dens[row, 1 + h, pl.ds(0, per * 8), :] = total.reshape(per * 8, LN)

        def combo(i, _):
            if halves == 2:
                pairs(i, 0)
                pairs(i, 1)
            else:
                pairs(i // 2, i % 2)
            return 0

        if k == 0 and stage < 2:
            paired_stage(stage, density_paired)
            if stage == 1:
                pairs(0, 0, edge=True)
                spread_edges(dens)
            return
        per_row = STAGE_SIZE[stage] // halves
        lax.fori_loop(first * per_row, last * per_row, combo, 0)

    def force_stage(stage, k, first=0, last=2):
        groups = NACT[k] // 8
        per = min(groups, 2)
        sets = groups // per
        halves = 2 if per == 1 else 1
        base = STAGE_BASE[stage]

        def pairs(c, h, g, edge=False):
            row, r, b = (2, 4, 0) if edge else stage_ids(stage, c)
            xi, yi, zi, vxi, vyi, vzi, qi, ci, ri = (
                own(3 if edge else row, comp, h, g, per) for comp in (X, Y, Z, VX, VY, VZ, Q, C, R)
            )
            slot = EDGE_SLOT if edge else (base + c) * 2 + h
            ax, ay, az = (acc[d, row, 1 + h, pl.ds(g * 8, per * 8), :].reshape(per, 8, LN) for d in range(3))
            for j in range(S):
                dx = xi - other(r, X, b, h, j)
                dy = yi - other(r, Y, b, h, j)
                dz = zi - other(r, Z, b, h, j)
                n = (
                    dx * (vxi - other(r, VX, b, h, j))
                    + dy * (vyi - other(r, VY, b, h, j))
                    + dz * (vzi - other(r, VZ, b, h, j))
                )
                mu = jnp.minimum(n, 0.0) * cache_a[slot * S + j, pl.ds(g, per)]
                sound = ci + other(r, C, b, h, j)
                visc = (mu * (mu - sound)) / (ri + other(r, R, b, h, j))
                f = cache_w[slot * S + j, pl.ds(g, per)] * (qi + other(r, Q, b, h, j) + visc)
                ax, ay, az = ax + f * dx, ay + f * dy, az + f * dz
            for d, total in enumerate((ax, ay, az)):
                acc[d, row, 1 + h, pl.ds(g * 8, per * 8), :] = total.reshape(per * 8, LN)

        def combo(i, _):
            if halves == 2:
                pairs(i, 0, 0)
                pairs(i, 1, 0)
            else:
                ch, g = i // sets, (i % sets) * per
                pairs(ch // 2, ch % 2, g)
            return 0

        if k == 0 and stage < 2:
            paired_stage(stage, force_paired)
            if stage == 1:

                def edge(i, _):
                    pairs(0, 0, i * 2, edge=True)
                    return 0

                lax.fori_loop(0, 2, edge, 0)
                for d in range(3):
                    spread_edges(acc.at[d])
            return
        per_row = STAGE_SIZE[stage] * sets // halves
        lax.fori_loop(first * per_row, last * per_row, combo, 0)

    def plan():
        row_i = lax.broadcasted_iota(jnp.int32, (LN, LN), 0)
        col_i = lax.broadcasted_iota(jnp.int32, (LN, LN), 1)
        before = jnp.where(row_i < col_i, 1.0, 0.0).astype(jnp.bfloat16)
        ones = jnp.ones((LN, LN), jnp.bfloat16)
        row8 = lax.broadcasted_iota(jnp.int32, (8, LN), 0)
        dest = tgt[...]
        start = jnp.zeros((LN, LN), jnp.float32)
        place = jnp.zeros((LN, LN), jnp.float32)
        start_t = jnp.zeros((8, LN), jnp.float32)
        info = jnp.zeros((8, LN), jnp.float32)
        for d in range(subs):
            mine = dest == d
            hot = jnp.where(mine, 1.0, 0.0).astype(jnp.bfloat16)
            inside = jnp.dot(hot, before, preferred_element_type=jnp.float32)
            place = jnp.where(mine, start + inside, place)
            start = start + jnp.dot(hot, ones, preferred_element_type=jnp.float32)
            count_t = lax.dot_general(
                ones[0:8], hot, (((1,), (1,)), ((), ())), preferred_element_type=jnp.float32
            )
            info = jnp.where(row8 == d, start_t, info)
            info = jnp.where(row8 == subs + d, count_t, info)
            start_t = start_t + count_t
        pos[...] = place.astype(jnp.int32)
        tab[u] = info
        sends = []
        for k in range(1, subs):
            copy = pltpu.make_async_remote_copy(
                src_ref=tab.at[u],
                dst_ref=tab.at[u],
                send_sem=tab_send.at[k],
                recv_sem=tab_recv.at[k],
                device_id=(t, lax.rem(u + k, subs)),
                device_id_type=MESH,
            )
            copy.start()
            sends.append(copy)
        return sends

    def emit(g, own_rows):
        row_q = lax.broadcasted_iota(jnp.int32, (LN, LN), 0)
        for row in own_rows:
            for h in range(2):
                count = jnp.broadcast_to(cnt[0, pl.ds(h * 2 + row, 1), :], (8, LN))
                rows = pl.ds(g * 8, 8)
                slot = lax.broadcasted_iota(jnp.int32, (8, LN), 0) + g * 8
                in_rows = pl.ds(g * 32 + h * 2 + row, 8, stride=4)
                values = [st[d, row, h, rows, :] * 0.25 for d in range(3)]
                values += [st[3 + d, row, h, rows, :] * 0.0625 for d in range(3)]
                values += [pr[2, row, h, rows, :] * 0.25]
                values += [jnp.where(slot < count, mass[in_rows, :], 0.0)]
                for i, v in enumerate(values):
                    raw[g, pl.ds((row * 2 + h) * 64 + i, 8, stride=8), :] = v

        def sort(rh, _):
            row, h = rh // 2, rh % 2
            for i in range(8):
                slot = g * 8 + i
                line = pos[pl.ds(slot * 4 + h * 2 + row, 1), :]
                hot = jnp.where(row_q == jnp.broadcast_to(line, (LN, LN)), 1.0, 0.0)
                v = raw[g, pl.ds(rh * 64 + i * 8, 8), :]
                hi = v.astype(jnp.bfloat16)
                rest = v - hi.astype(jnp.float32)
                mid = rest.astype(jnp.bfloat16)
                low = (rest - mid.astype(jnp.float32)).astype(jnp.bfloat16)
                pieces = jnp.concatenate([hi, mid, low], axis=0)
                moved = lax.dot_general(
                    pieces, hot.astype(jnp.bfloat16), (((1,), (1,)), ((), ())), preferred_element_type=jnp.float32
                )
                gathered[u, slot * 2 + h, row] = (moved[0:8] + moved[8:16]) + moved[16:24]
            return 0

        lax.fori_loop(own_rows[0] * 2, own_rows[-1] * 2 + 2, sort, 0)

    PIECES = ((32, 32, (0, 1)), (16, 16, (0, 1)), (0, 16, (0,)), (0, 16, (1,)))

    def piece_copy(p, flow, owner, second_half, dst):
        first, rows, own_rows = PIECES[p]
        half = rows // 2
        part = pl.ds(first + half * second_half, half)
        which = slice(None) if len(own_rows) == 2 else own_rows[0]
        landing = done if p >= 2 and flow not in (0, 2) else gathered
        return pltpu.make_async_remote_copy(
            src_ref=gathered.at[owner, part, which],
            dst_ref=landing.at[owner, part, which],
            send_sem=piece_send.at[p, flow],
            recv_sem=piece_recv.at[p, flow],
            device_id=(t, dst),
            device_id_type=MESH,
        )

    leaving = []

    def write_out(p, at, owner, first, rows):
        own_rows = PIECES[p][2]
        which = slice(None) if len(own_rows) == 2 else own_rows[0]
        copy = pltpu.make_async_copy(
            gathered.at[owner, pl.ds(first, rows), which], done.at[owner, pl.ds(first, rows), which], done_sem.at[p, at]
        )
        copy.start()
        leaving.append(copy)

    def start_piece(p, before_rest=None):
        first, rows, own_rows = PIECES[p]
        for g in range(first // 16, (first + rows) // 16):
            emit(g, own_rows)
        copies = [
            piece_copy(p, 0, u, 0, right),
            piece_copy(p, 1, u, 1, right),
            piece_copy(p, 2, u, 1, left),
            piece_copy(p, 3, u, 0, left),
        ]
        arriving[p] = copies
        copies[0].start()
        copies[2].start()
        if before_rest is not None:
            before_rest()
        copies[1].start()
        copies[3].start()
        if p >= 2:
            write_out(p, 0, u, first, rows)

    def forward_piece(p):
        arriving[p][0].wait_recv()
        arriving[p][2].wait_recv()
        copies = [piece_copy(p, 4, left, 0, right), piece_copy(p, 5, right, 1, left)]
        for copy in copies:
            copy.start()
        arriving[p] += copies
        if p >= 2:
            first, rows, _ = PIECES[p]
            write_out(p, 1, left, first, rows // 2)
            write_out(p, 2, right, first + rows // 2, rows // 2)

    def finish_piece(p):
        for f in (1, 3, 4, 5):
            arriving[p][f].wait_recv()
        for copy in arriving[p]:
            copy.wait_send()
        if p < 2:
            write_out(p, 0, slice(None), PIECES[p][0], PIECES[p][1])

    def exchange_and_sum(rnd, src, inbox, comps, n, stage_fn, k, meanwhile, row_done=None):
        copies = start_round(rnd, src, len(comps), n, inbox)
        meanwhile()
        loads = [None] * 4
        for r in (1, 2):
            loads[r] = functools.partial(lambda row, c, h, rows: src[c, row, h, rows, :], r - 1)
        loads[0] = lambda c, h, rows: inbox[rnd // 2, 0, c, h, rows, :]
        loads[3] = lambda c, h, rows: inbox[rnd // 2, 1, c, h, rows, :]
        for r in (1, 2):
            centre(loads[r], comps, r, n)
        stage_fn(0, k)
        copies[4].wait_recv()
        copies[5].wait_recv()
        for r in (1, 2):
            sides(loads[r], comps, r, n, rnd, 1, r - 1)
        if k == 0:
            edges(comps)
        stage_fn(1, k, 0, 2 if row_done is None else 1)
        for f in (0, 1, 2, 3, 6, 7):
            copies[f].wait_recv()
        for r, dt, sender_row in ((0, 0, 1), (3, 2, 0)):
            centre(loads[r], comps, r, n)
            sides(loads[r], comps, r, n, rnd, dt, sender_row)
        if row_done is None:
            stage_fn(2, k)
            return copies
        for copy in copies:
            copy.wait_send()
        stage_fn(2, k, 0, 1)
        row_done(0)
        stage_fn(1, k, 1, 2)
        row_done(1)
        stage_fn(2, k, 1, 2)
        row_done(2)
        return []

    arriving = {}

    def lay_plan():
        for copy in arriving["tab"]:
            copy.wait_recv()
        row_i = lax.broadcasted_iota(jnp.int32, (LN, LN), 0)
        col_i = lax.broadcasted_iota(jnp.int32, (LN, LN), 1)

        def order(i):
            return (i // 4) * 4 + (i % 2) * 2 + (i // 2) % 2

        earlier = jnp.where(order(row_i) < order(col_i), 1.0, 0.0).astype(jnp.bfloat16)
        starts = jnp.concatenate([tab[src, pl.ds(u, 1), :] for src in range(subs)], axis=0)
        counts = jnp.concatenate([tab[src, pl.ds(subs + u, 1), :] for src in range(subs)], axis=0)
        padded = jnp.concatenate([counts, jnp.zeros_like(counts)], axis=0).astype(jnp.bfloat16)
        base = jnp.dot(padded, earlier, preferred_element_type=jnp.float32)[0:subs]
        base = base.astype(jnp.int32)
        skip = base & (LN - 1)
        turn = (skip - starts.astype(jnp.int32)) & (LN - 1)
        end = skip + counts.astype(jnp.int32)
        runs[0:subs, :] = turn + skip * 128 + end * 16384 + (base >> 7) * 4194304
        runs[subs : 2 * subs, :] = jnp.zeros((subs, LN), jnp.int32)
        arriving["runs"] = pltpu.make_async_copy(runs, runs_out, runs_sem)
        arriving["runs"].start()

    def during(rnd):
        if rnd == 0:
            arriving["tab"] = plan()
        elif rnd in (2, 4):
            if rnd == 4:
                finish_piece(0)
            start_piece(rnd // 2 - 1)
        elif rnd in (3, 5):
            forward_piece(rnd // 2 - 1)
            if rnd == 5:
                lay_plan()

    def move(k, row):
        for h in range(2):
            count = jnp.broadcast_to(cnt[k, pl.ds(h * 2 + row, 1), :], (8, LN))
            for g in range(NACT[k] // 8):
                rows = pl.ds(g * 8, 8)
                slot = lax.broadcasted_iota(jnp.int32, (8, LN), 0) + g * 8
                active = slot < count
                for d in range(3):
                    v = st[3 + d, row, h, rows, :]
                    x = st[d, row, h, rows, :]
                    v_new = v + 4.0 * acc[d, row, 1 + h, rows, :]
                    st[3 + d, row, h, rows, :] = jnp.where(active, v_new, v)
                    st[d, row, h, rows, :] = jnp.where(active, x + 0.0125 * v_new, x)

    def last_rows(step):
        if step == 0:
            move(2, 0)
            start_piece(2)
        elif step == 2:
            finish_piece(1)
            move(2, 1)
            start_piece(3, lambda: forward_piece(2))
            forward_piece(3)

    for k in range(3):
        n = NACT[k]
        dens[...] = jnp.zeros_like(dens)
        comps = (X, Y, Z, VX, VY, VZ) + ((MS,) if k == 0 else ())
        moved = exchange_and_sum(2 * k, st, xin, comps, NMOVED[k], density_stage, k, lambda: during(2 * k))
        for row in range(2):
            for h in range(2):
                count = jnp.broadcast_to(cnt[k, pl.ds(h * 2 + row, 1), :], (8, LN))
                for g in range(n // 8):
                    rows = pl.ds(g * 8, 8)
                    slot = lax.broadcasted_iota(jnp.int32, (8, LN), 0) + g * 8
                    rho4 = jnp.where(slot < count, dens[row, 1 + h, rows, :], pr[2, row, h, rows, :])
                    root = jnp.exp(jnp.log(rho4 * 0.25) * (1.0 / 3.0))
                    pr[0, row, h, rows, :] = sq[0, row, h, rows, :] / root
                    pr[1, row, h, rows, :] = sq[1, row, h, rows, :] * root
                    pr[2, row, h, rows, :] = rho4
        acc[...] = jnp.zeros_like(acc)
        if k == 2:
            for copy in moved:
                copy.wait_send()
        pressed = exchange_and_sum(
            2 * k + 1, pr, pin, (Q, C, R), n, force_stage, k, lambda: during(2 * k + 1), last_rows if k == 2 else None
        )
        if k < 2:
            for copy in moved + pressed:
                copy.wait_send()
            for row in range(2):
                move(k, row)
    for copy in arriving["tab"]:
        copy.wait_send()
    for p in (2, 3):
        finish_piece(p)
    for copy in leaving:
        copy.wait()
    arriving["runs"].wait()


TILES = 48


STEPS = 4


def lay_kernel(runs_in, gathered_in, out, runs, gathered, tiles, runs_sem, in_sem, out_sem):
    subs = gathered.shape[0]
    lane = lane_iota()
    beyond = lane + LN
    block = LN // 2 // STEPS
    inputs = [
        pltpu.make_async_copy(
            gathered_in.at[:, pl.ds(i * block, block)], gathered.at[:, pl.ds(i * block, block)], in_sem.at[i]
        )
        for i in range(STEPS)
    ]
    table = pltpu.make_async_copy(runs_in, runs, runs_sem)
    table.start()
    inputs[0].start()
    inputs[1].start()
    tiles[...] = jnp.zeros_like(tiles)
    table.wait()

    def lay(slot, currents):
        for row in range(2):
            for h in range(2):
                at = slot * 4 + h * 2 + row
                later = []
                for src in range(subs):
                    word = runs[src, at]
                    words = jnp.full((8, LN), word)
                    end = (words >> 14) & 255
                    turned = pltpu.roll(gathered[src, slot * 2 + h, row], word & (LN - 1), 1)
                    kept = jnp.where(lane < end, turned, 0.0)
                    merged = jnp.where(lane < ((words >> 7) & (LN - 1)), currents[src], kept)
                    tiles[src, word >> 22] = merged
                    wrapped = jnp.where(beyond < end, turned, 0.0)
                    later.append(jnp.where(end >= LN, wrapped, merged))
                currents = later
        return tuple(currents)

    currents = (jnp.zeros((8, LN), jnp.float32),) * subs
    for i in range(STEPS):
        inputs[i].wait()
        if i + 2 < STEPS:
            inputs[i + 2].start()
        currents = lax.fori_loop(i * (S // STEPS), (i + 1) * (S // STEPS), lay, currents, unroll=2)
    outputs = []
    for src in range(subs):
        word = runs[src, LN - 1]
        tiles[src, (word >> 22) + jnp.where((word >> 14) & 255 >= LN, 1, 0)] = currents[src]
    for src in range(subs):
        copy = pltpu.make_async_copy(
            tiles.at[src, pl.ds(0, TILES)], out.at[pl.ds(src * TILES, TILES)], out_sem.at[src]
        )
        copy.start()
        outputs.append(copy)
    for copy in outputs:
        copy.wait()


def rows_of(a):
    lead = a.shape[:-2]
    a = a.reshape(lead + (2, 2, LN))
    a = jnp.swapaxes(a, -3, -2)
    return a


def shards(tiles, subs, offsets, velocity, mass, entropy, active_counts, targets):
    off = rows_of(offsets).reshape(3, LN, LN)
    vel = rows_of(velocity).reshape(3, LN, LN)
    mas = rows_of(mass).reshape(LN, LN)
    ent = rows_of(entropy).reshape(LN, LN)
    cnt = rows_of(active_counts).reshape(3, 4, LN)
    tgt = rows_of(targets).reshape(LN, LN)
    anywhere = pl.BlockSpec(memory_space=pl.ANY)
    f32 = jnp.float32
    gathered, runs = pl.pallas_call(
        functools.partial(substeps_kernel, tiles, subs),
        out_shape=[
            jax.ShapeDtypeStruct((subs, LN // 2, 2, 8, LN), f32),
            jax.ShapeDtypeStruct((2 * subs, LN), jnp.int32),
        ],
        in_specs=[anywhere] * 6,
        out_specs=[anywhere] * 2,
        scratch_shapes=[
            pltpu.VMEM((subs, LN // 2, 2, 8, LN), f32),
            pltpu.VMEM((3, LN, LN), f32),
            pltpu.VMEM((3, LN, LN), f32),
            pltpu.VMEM((LN, LN), f32),
            pltpu.VMEM((LN, LN), f32),
            pltpu.VMEM((3, 4, LN), jnp.int32),
            pltpu.VMEM((LN, LN), jnp.int32),
            pltpu.VMEM((2 * subs, LN), jnp.int32),
            pltpu.VMEM((5 * NF * 6, S, LN), f32),
            pltpu.VMEM((7, 2, 2, S, LN), f32),
            pltpu.VMEM((3, 2, 2, S, LN), f32),
            pltpu.VMEM((3, 4, S, LN), f32),
            pltpu.VMEM((3, 3, 4, S, LN), f32),
            pltpu.VMEM((2, 2, 2, S, LN), f32),
            pltpu.VMEM((6, 2, S, LN), f32),
            pltpu.VMEM((3, 2, 7, 2, S, LN), f32),
            pltpu.VMEM((3, 2, 3, 2, S, LN), f32),
            pltpu.VMEM((6, 3, 2, S, LN), f32),
            pltpu.VMEM((18 * 2 * S, 4, 8, LN), f32),
            pltpu.VMEM((18 * 2 * S, 4, 8, LN), f32),
            pltpu.VMEM((4, 256, LN), f32),
            pltpu.VMEM((3, 256, LN), f32),
            pltpu.VMEM((LN, LN), jnp.int32),
            pltpu.VMEM((subs, 2 * subs, LN), f32),
            pltpu.SemaphoreType.DMA((2, 8)),
            pltpu.SemaphoreType.DMA((2, 8)),
            pltpu.SemaphoreType.DMA((4,)),
            pltpu.SemaphoreType.DMA((4,)),
            pltpu.SemaphoreType.DMA((4, 6)),
            pltpu.SemaphoreType.DMA((4, 6)),
            pltpu.SemaphoreType.DMA((4, 3)),
            pltpu.SemaphoreType.DMA((6,)),
            pltpu.SemaphoreType.DMA,
        ],
        compiler_params=pltpu.CompilerParams(collective_id=0, has_side_effects=True, vmem_limit_bytes=62 * 1024 * 1024),
        name="substeps",
    )(off, vel, mas, ent, cnt, tgt)
    arrived = pl.pallas_call(
        lay_kernel,
        out_shape=jax.ShapeDtypeStruct((subs * TILES, 8, LN), f32),
        in_specs=[anywhere] * 2,
        out_specs=anywhere,
        scratch_shapes=[
            pltpu.SMEM((2 * subs, LN), jnp.int32),
            pltpu.VMEM((subs, LN // 2, 2, 8, LN), f32),
            pltpu.VMEM((subs, TILES + 2, 8, LN), f32),
            pltpu.SemaphoreType.DMA,
            pltpu.SemaphoreType.DMA((STEPS,)),
            pltpu.SemaphoreType.DMA((subs,)),
        ],
        name="lay",
    )(runs, gathered)
    return jnp.transpose(arrived, (1, 0, 2)).reshape(8, subs * TILES * LN)


def solution(mesh):
    tiles, subs = mesh.shape["tile"], mesh.shape["sub"]
    placed = (
        P(None, None, "tile", "sub"),
        P(None, None, "tile", "sub"),
        P(None, "tile", "sub"),
        P(None, "tile", "sub"),
        P(None, "tile", "sub"),
        P(None, "tile", "sub"),
    )
    return jax.shard_map(
        functools.partial(shards, tiles, subs),
        mesh=mesh,
        in_specs=placed,
        out_specs=P(None, ("tile", "sub")),
        check_vma=False,
    )
```
